32 devices in a mesh: gx: 4 (over y, x), gy: 8 (over z, core).
Axes of the slice: x: 2, y: 2, z: 4, core: 2. Of those that a mesh axis runs over, the one named last changes fastest.
Arguments:
- volume: float32 [128, 512, 256], P('gx', 'gy'), may hold values from -18 to 18, as said below
Outputs:
- denoised: float32 [128, 512, 256], P('gx', 'gy')
The draws below stay inside these ranges and needn't reach their ends.
Inputs may be any that keep to these rules, and one draw needn't show every extreme that they name: `volume`: real values.
All inputs are finite; a program needn't handle non-finite values.
Results may differ from the reference program's by a relative error of at most 0.00002.
Values sent between devices are 32-bit elements; how exact they have to be, the bound alone decides.
A program may use at most 128 MiB of HBM per device.

```python
import math
import jax
import jax.numpy as jnp

NZ = 256
LEVELS = 3
NX = 128
NY = 512


def draw_volume(key, part):
    ramp_x = 1.0 + 2.0 * jnp.arange(NX, dtype=jnp.float32)[:, None, None] / NX
    noise = jnp.clip(jax.random.normal(key, (NX, NY, NZ), jnp.float32), -6.0, 6.0)
    return (ramp_x * noise).astype(jnp.float32)


def setup_inputs(seed: int = 0) -> dict:
    seeds = jax.random.split(jax.random.key(seed), 2)
    return {
        "volume": draw_volume(jax.random.fold_in(seeds[1], 71), 0),
    }


root_three = math.sqrt(3.0)
lift_near = math.sqrt(3.0) / 4.0
lift_far = (math.sqrt(3.0) - 2.0) / 4.0
scale_low = (math.sqrt(3.0) - 1.0) / math.sqrt(2.0)
scale_high = (math.sqrt(3.0) + 1.0) / math.sqrt(2.0)

def take_every(values, start, along):
    index = [slice(None)] * values.ndim
    index[along] = slice(start, None, 2)
    return values[tuple(index)]

def weave(first, second, along):
    stacked = jnp.stack([first, second], axis=along + 1)
    shape = list(first.shape)
    shape[along] = shape[along] * 2
    return stacked.reshape(shape)

def forward_lines(values, along):
    even_cells = take_every(values, 0, along)
    odd_cells = take_every(values, 1, along)
    smooth = even_cells + root_three * odd_cells
    detail = odd_cells - lift_near * smooth - lift_far * jnp.roll(smooth, 1, axis=along)
    smooth = smooth - jnp.roll(detail, -1, axis=along)
    return (scale_high * detail, scale_low * smooth)

def inverse_lines(detail, smooth, along):
    detail = detail / scale_high
    smooth = smooth / scale_low
    first = smooth + jnp.roll(detail, -1, axis=along)
    odd_cells = detail + lift_near * first + lift_far * jnp.roll(first, 1, axis=along)
    even_cells = first - root_three * odd_cells
    return weave(even_cells, odd_cells, along)

def forward_level(coarse):
    detail, smooth = forward_lines(coarse, 0)
    coeffs = weave(detail, smooth, 0)
    detail, smooth = forward_lines(coeffs, 1)
    coeffs = weave(detail, smooth, 1)
    detail, smooth = forward_lines(coeffs, 2)
    return jnp.concatenate([smooth, detail], axis=2)

def inverse_level(coeffs):
    half = coeffs.shape[2] // 2
    rebuilt = inverse_lines(coeffs[:, :, half:], coeffs[:, :, :half], 2)
    rebuilt = inverse_lines(take_every(rebuilt, 0, 1), take_every(rebuilt, 1, 1), 1)
    return inverse_lines(take_every(rebuilt, 0, 0), take_every(rebuilt, 1, 0), 0)

def split_view(coeffs):
    sizes = coeffs.shape
    return coeffs.reshape(sizes[0] // 2, 2, sizes[1] // 2, 2, sizes[2])

def shrink_insert(coeffs, coarse, limit):
    shrunk = coeffs - jnp.clip(coeffs, -limit, limit)
    half = coeffs.shape[2] // 2
    view = split_view(shrunk).at[:, 1, :, 1, :half].set(coarse)
    return view.reshape(coeffs.shape)

def reference(volume):
    levels = []
    coarse = volume
    for level in range(LEVELS):
        coeffs = forward_level(coarse)
        levels.append(coeffs)
        half = coeffs.shape[2] // 2
        coarse = split_view(coeffs)[:, 1, :, 1, :half]
    finest = levels[0]
    half = finest.shape[2] // 2
    diagonal = split_view(finest)[:, 0, :, 0, half:]
    count = NX * NY * NZ // 8
    noise = jnp.sum(jnp.abs(diagonal)) * (math.sqrt(math.pi / 2.0) / count)
    rebuilt = coarse
    for level in range(LEVELS - 1, -1, -1):
        coeffs = shrink_insert(levels[level], rebuilt, noise)
        rebuilt = inverse_level(coeffs)
    return rebuilt
```

```python
import functools
import math

import jax
import jax.numpy as jnp
import numpy as np
from jax import lax
from jax.experimental import pallas as pl
from jax.experimental.pallas import tpu as pltpu
from jax.sharding import PartitionSpec as P

ROOT3 = math.sqrt(3.0)
NEAR = math.sqrt(3.0) / 4.0
FAR = (math.sqrt(3.0) - 2.0) / 4.0
LOW = (math.sqrt(3.0) - 1.0) / math.sqrt(2.0)
HIGH = (math.sqrt(3.0) + 1.0) / math.sqrt(2.0)
LANES = 128
PAD = 8


def forward_matrix(size):
    lines = np.eye(size)
    even, odd = lines[:, 0::2], lines[:, 1::2]
    smooth = even + ROOT3 * odd
    detail = odd - NEAR * smooth - FAR * np.roll(smooth, 1, 1)
    smooth = smooth - np.roll(detail, -1, 1)
    return np.concatenate([LOW * smooth, HIGH * detail], 1)


def inverse_matrix(size):
    lines = np.eye(size)
    smooth, detail = lines[:, : size // 2] / LOW, lines[:, size // 2 :] / HIGH
    first = smooth + np.roll(detail, -1, 1)
    odd = detail + NEAR * first + FAR * np.roll(first, 1, 1)
    even = first - ROOT3 * odd
    return np.stack([even, odd], 2).reshape(size, size)


def halves(matrix, size):
    full = np.zeros((size, size))
    full[: matrix.shape[0], : matrix.shape[1]] = matrix
    high = full.astype(jnp.bfloat16)
    low = (full - high.astype(np.float64)).astype(jnp.bfloat16)
    return np.stack([high, low])


def times(values, w_ref):
    high = values.astype(jnp.bfloat16)
    low = (values - high.astype(jnp.float32)).astype(jnp.bfloat16)
    dot = functools.partial(jnp.dot, preferred_element_type=jnp.float32)
    return dot(high, w_ref[0]) + (dot(low, w_ref[0]) + dot(high, w_ref[1]))


def shrink(values, noise):
    return values - jnp.clip(values, -noise, noise)


def sums(even, odd):
    smooth = even + ROOT3 * odd
    return smooth, odd - NEAR * smooth


def undo(detail, first, before):
    odd = detail + NEAR * first + FAR * before
    return first - ROOT3 * odd, odd


def weave(even, odd):
    both = jnp.stack([even, odd], axis=1)
    return both.reshape((2 * even.shape[0],) + even.shape[1:])


def forward_rows(even, odd):
    axis = even.ndim - 2
    smooth, part = sums(even, odd)
    detail = part - FAR * pltpu.roll(smooth, 1, axis)
    return detail, smooth - pltpu.roll(detail, even.shape[axis] - 1, axis)


def limits(noise, level):
    base = noise * (1.0 / LOW ** (2 * (level - 1)))
    return base * (1.0 / (HIGH * HIGH)), base * (1.0 / (HIGH * LOW)), base * (1.0 / (LOW * LOW))


def kernel(shape, nx, ny, vol, g1, gu, g3, g4, g5, g6,
           d1d, d1s, s1d, s1s, dd, ds, sd, ep3, b3, noise, v1, v2, v3,
           w1, wu, w3,
           e1, hx1, sx1, hy1, sy1, hc1, sc1, xd1, xs1,
           e2, xl, xh, xlow, xhigh, xd2, xs2, t3d, t3s,
           mine, rows_in, dummy, send, recv, lsem, wsem):
    cx, cy, cz = shape
    hx, hy, qx, qy = cx // 2, cy // 2, cx // 4, cy // 4
    ix, iy = lax.axis_index("gx"), lax.axis_index("gy")

    def device(dx, dy):
        return (lax.rem(ix + dx + nx, nx), lax.rem(iy + dy + ny, ny))

    near = [(dx, dy) for dx in (-1, 0, 1) for dy in (-1, 0, 1) if dx or dy]
    peers = [(dx, dy) for dx in range(nx) for dy in range(ny) if dx or dy]
    taken = {(dx % nx, dy % ny) for dx, dy in near}
    barrier = pltpu.get_barrier_semaphore()

    def greet(dx, dy):
        pl.semaphore_signal(barrier, inc=1, device_id=device(dx, dy),
                            device_id_type=pl.DeviceIdType.MESH)

    for d in sorted(taken):
        greet(*d)
    loads = [
        pltpu.make_async_copy(
            vol.at[:, :, pl.ds(h * LANES, LANES)],
            e1.at[:, h, pl.ds(PAD, cy), :], lsem.at[h])
        for h in range(2)
    ]
    for c in loads:
        c.start()
    for d in peers:
        if d not in taken:
            greet(*d)
    weights = [
        pltpu.make_async_copy(src, dst, wsem.at[i])
        for i, (src, dst) in enumerate(
            zip((g1, gu, g3, g4, g5, g6), (w1, wu, w3, v1, v2, v3)))
    ]
    for c in weights:
        c.start()

    sent = [0]

    def post(src, dst, dx, dy, group):
        sent[0] += math.prod(src.shape) // LANES
        pltpu.make_async_remote_copy(
            src_ref=src, dst_ref=dst, send_sem=send.at[0], recv_sem=recv.at[group],
            device_id=device(dx, dy), device_id_type=pl.DeviceIdType.MESH).start()
        return math.prod(src.shape) // LANES

    def land(sem, rows):
        part = dummy.at[pl.ds(0, rows)]
        pltpu.make_async_copy(part, part, sem).wait()

    ep3[:, 0 : PAD // 2] = jnp.zeros((qx + 4, PAD // 2, LANES), jnp.float32)
    ep3[:, PAD // 2 + hy // 2 + PAD :] = jnp.zeros((qx + 4, PAD // 2, LANES), jnp.float32)
    for ref in (dd, ds, sd):
        ref[:, 0 : PAD // 2] = jnp.zeros((qx + 2, PAD // 2, LANES), jnp.float32)
        ref[:, PAD // 2 + hy // 2 + PAD :] = jnp.zeros((qx + 2, PAD // 2, LANES), jnp.float32)

    for c in loads:
        c.wait()

    top = PAD + cy
    sx1[1] = sums(e1[0, :, PAD:top], e1[1, :, PAD:top])[1]
    sy1[1] = sums(e1[:, :, PAD : PAD + 1], e1[:, :, PAD + 1 : PAD + 2])[1]
    sx1[0] = sums(e1[cx - 2, :, PAD:top], e1[cx - 1, :, PAD:top])[0]
    sy1[0] = sums(e1[:, :, top - 2 : top - 1], e1[:, :, top - 1 : top])[0]
    for x in range(2):
        sc1[x, 1] = sums(sx1[x, :, 0:1], sx1[x, :, 1:2])[1]
        sc1[x, 0] = sums(sx1[x, :, cy - 2 : cy - 1], sx1[x, :, cy - 1 : cy])[0]
    pl.semaphore_wait(barrier, len(peers))
    step = (1, -1)
    post_x = lambda x, g: post(sx1.at[x], hx1.at[x, :, pl.ds(PAD, cy), :], step[x], 0, g)
    post_y = lambda y, g: post(sy1.at[y], hy1.at[y], 0, step[y], g)
    post_c = lambda x, y, g: post(sc1.at[x, y], hc1.at[x, y], step[x], step[y], g)
    now1 = post_c(1, 1, 0) + post_x(1, 0) + post_y(1, 0)
    later1 = (post_c(0, 1, 1) + post_c(1, 0, 1) + post_c(0, 0, 1)
              + post_x(0, 1) + post_y(0, 1))

    def place(ref, rows, side):
        if side == 0:
            ref[..., PAD - 2 : PAD - 1, :] = rows
            ref[..., PAD - 1 : PAD, :] = jnp.zeros_like(rows)
        else:
            ref[..., top : top + 1, :] = -ROOT3 * rows
            ref[..., top + 1 : top + 2, :] = rows

    def pair1(n, rows=slice(None)):
        return sums(e1[2 * n, :, rows], e1[2 * n + 1, :, rows])

    def lift1(rows):
        def step(n, carry):
            _, part_n = pair1(n, rows)
            before, _ = pair1(n - 1, rows)
            detail = part_n - FAR * before
            xd1[n, :, rows] = detail
            xs1[n, :, rows] = before - detail
            return carry

        lax.fori_loop(1, hx, step, 0)

    def coarse1(n, first, count):
        for h in range(2):
            load = lambda start: xs1[n, h, pl.ds(start + 2 * first, count, stride=2), :]
            s0, _ = sums(load(PAD), load(PAD + 1))
            _, tp = sums(load(PAD + 2), load(PAD + 3))
            s1s[n, h, PAD + first : PAD + first + count] = s0 - (tp - FAR * s0)

    def coarse1_inner(n, carry):
        coarse1(n, 0, hy)
        return carry

    def coarse1_top(n, carry):
        coarse1(n, hy - 1, 1)
        return carry

    lift1(slice(PAD, top))
    lax.fori_loop(1, hx, coarse1_inner, 0)
    for c in weights:
        c.wait()
    land(recv.at[0], now1)
    place(e1, hy1[1], 1)
    place(hx1.at[1], hc1[1, 1], 1)
    lift1(slice(top, top + 2))
    edge, _ = pair1(hx - 1)
    edge_d = hx1[1] - FAR * edge
    xd1[hx] = edge_d
    xs1[hx] = edge - edge_d
    lax.fori_loop(1, hx, coarse1_top, 0)
    coarse1(hx, 0, hy)

    def lines(ref, xs, ys):
        n = (xs.stop - xs.start) * (ys.stop - ys.start)
        return jnp.concatenate([ref[xs, h, ys].reshape(n, LANES) for h in range(2)], axis=1)

    chunk = hx // 2
    own = slice(PAD, PAD + hy)
    for i in range(2):
        rows = lines(s1s, slice(1 + i * chunk, 1 + (i + 1) * chunk), own)
        e2[i * chunk : (i + 1) * chunk, own] = times(rows, wu).reshape(chunk, hy, LANES)

    def pair2(m, rows):
        return sums(e2[2 * m, rows], e2[2 * m + 1, rows])

    def coarse2(m, rows):
        return pair2(m, rows)[0] * (1.0 + FAR) - pair2(m + 1, rows)[1]

    xl[0] = pair2(qx - 2, own)[0]
    xl[1] = e2[hx - 2, own]
    xl[2] = e2[hx - 1, own]
    xl[3] = sums(coarse2(qx - 4, own), coarse2(qx - 3, own))[0]
    xh[0] = pair2(0, own)[1]
    xh[1] = sums(coarse2(0, own), coarse2(1, own))[1]
    y_own, y_low, y_high = pl.ds(PAD, hy), pl.ds(0, PAD), pl.ds(PAD + hy, PAD)
    s_own, s_first, s_last = pl.ds(0, hy), pl.ds(0, PAD), pl.ds(hy - PAD, PAD)
    round2 = 0
    for rows_s, rows_d, dy in ((s_last, y_low, 1), (s_first, y_high, -1), (s_own, y_own, 0)):
        round2 += post(xl.at[:, rows_s, :], xlow.at[:, rows_d, :], 1, dy, 2)
        round2 += post(xh.at[:, rows_s, :], xhigh.at[:, rows_d, :], -1, dy, 2)
    round2 += post(e2.at[:, pl.ds(PAD, PAD), :], e2.at[:, y_high, :], 0, -1, 2)
    round2 += post(e2.at[:, pl.ds(hy, PAD), :], e2.at[:, y_low, :], 0, 1, 2)

    land(recv.at[1], later1)
    place(e1, hy1[0], 0)
    place(hx1.at[1], hc1[1, 0], 0)
    place(hx1.at[0], hc1[0, 0], 0)
    place(hx1.at[0], hc1[0, 1], 1)
    first_s, first_t = pair1(0)
    first_d = first_t - FAR * hx1[0]
    xd1[0] = first_d
    xs1[0] = hx1[0] - first_d
    low = slice(PAD - 2, PAD)

    lift1(low)
    edge, _ = sums(e1[cx - 2, :, low], e1[cx - 1, :, low])
    edge_d = hx1[1, :, low] - FAR * edge
    xd1[hx, :, low] = edge_d
    xs1[hx, :, low] = edge - edge_d

    def cols1(src, det, smo):
        def step(n, carry):
            for h in range(2):
                load = lambda start: src[n, h, pl.ds(start, hy + 1, stride=2), :]
                s0, t0 = sums(load(PAD), load(PAD + 1))
                sm, _ = sums(load(PAD - 2), load(PAD - 1))
                d = t0 - FAR * sm
                det[n, h, 0 : hy + 1] = d
                smo[n, h, PAD - 1 : PAD + hy] = sm - d
            return carry

        lax.fori_loop(0, hx + 1, step, 0)

    rows1 = hy + PAD
    parts1 = ((0, chunk), (chunk, hx + 1))

    def depth1(ref):
        magnitude = jnp.zeros((PAD, LANES), jnp.float32)
        for lo, hi in parts1:
            rows = lines(ref, slice(lo, hi), slice(0, rows1))
            if ref is s1s:
                ref[lo:hi, 1] = times(rows, w1.at[:, :, LANES : 2 * LANES]).reshape(
                    hi - lo, rows1, LANES)
                continue
            got = times(rows, w1)
            for h in range(2):
                ref[lo:hi, h] = got[:, h * LANES : (h + 1) * LANES].reshape(hi - lo, rows1, LANES)
            if ref is d1d:
                inside = got[:, LANES:].reshape(hi - lo, rows1, LANES)[:chunk, :hy]
                magnitude = magnitude + jnp.sum(
                    jnp.abs(inside).reshape(chunk * hy // PAD, PAD, LANES), axis=0)
        return magnitude

    cols1(xd1, d1d, d1s)
    mine[...] = jnp.sum(depth1(d1d), axis=0, keepdims=True)
    landed = 0
    for k, d in enumerate(peers):
        landed += post(mine, rows_in.at[k], d[0], d[1], 3)

    cols1(xs1, s1d, s1s)
    depth1(d1s)
    depth1(s1d)
    depth1(s1s)

    land(recv.at[2], round2)
    every = slice(0, hy + 2 * PAD)
    before = xlow[0]
    xs2[0] = xlow[3]
    for m in range(-1, qx + 1):
        if m == qx:
            smooth, part = None, xhigh[0]
        elif m == -1:
            smooth, part = sums(xlow[1], xlow[2])
        else:
            smooth, part = pair2(m, every)
        detail = part - FAR * before
        xd2[m + 1] = detail
        xs2[m + 2] = before - detail
        before = smooth
    xs2[qx + 3] = xhigh[1]
    pairs = hy // 2 + PAD

    def rows2(src):
        return forward_rows(src[:, pl.ds(0, pairs, stride=2), :],
                            src[:, pl.ds(1, pairs, stride=2), :])

    mid = slice(PAD // 2, PAD // 2 + pairs)
    dd[:, mid], ds[:, mid] = rows2(xd2)
    det, smo = rows2(xs2)
    sd[:, mid] = det[1 : qx + 3]
    ep3[:, mid] = smo

    n_own, n3, h3 = qx // 2, qx // 2 + 2, qy // 2 + PAD
    low_s, low_t = [ep3[0]], [None]
    for n in range(n_own + 1):
        s, t = sums(ep3[1 + 2 * n], ep3[2 + 2 * n])
        low_s.append(s)
        low_t.append(t)
    low_t.append(ep3[qx + 3])
    for n in range(n3):
        detail = low_t[n + 1] - FAR * low_s[n]
        t3d[n] = detail
        t3s[n] = low_s[n] - detail
    bands = []
    for src in (t3d, t3s):
        bands += forward_rows(src[:, pl.ds(0, h3, stride=2), :], src[:, pl.ds(1, h3, stride=2), :])
    for i, band in enumerate(bands):
        b3[i] = times(band.reshape(n3 * h3, LANES), w3).reshape(n3, h3, LANES)

    land(recv.at[3], landed)
    acc = mine[...]
    for k in range(len(peers)):
        acc = acc + rows_in[k]
    noise[...] = acc
    land(send.at[0], sent[0])


def finish(shape, count_all, d1d, d1s, s1d, s1s, dd, ds, sd, ep3, b3, total, v1, v2, v3, out,
           ss, r2, r1, s0, p1d, p1s, o1, ob, osem):
    cx, cy, cz = shape
    hx, hy, qx, qy = cx // 2, cy // 2, cx // 4, cy // 4
    n3, h3, x2, yrows = qx // 2 + 2, qy // 2 + PAD, qx + 2, qy + 2 * PAD
    noise = jnp.sum(total[...], axis=(0, 1), keepdims=True) * (
        HIGH * HIGH * math.sqrt(math.pi / 2.0) / count_all)

    far1, mid1, near1 = limits(noise, 1)

    def inv1(det, smo, h, dst, limit_d, limit_s):
        def one_x(n):
            d = shrink(det[n, h], limit_d)
            s = s0[n] if limit_s is None else shrink(smo[n, h], limit_s)
            return d, s + d

        def step(n, carry):
            d, before = carry
            after, one = one_x(n + 1)
            even, odd = undo(d, one, before)
            dst[2 * n, h] = even
            dst[2 * n + 1, h] = odd
            return after, one

        lax.fori_loop(0, hx, step, one_x(0), unroll=4)

    for h in range(2):
        inv1(d1d, s1d, h, p1d, far1, mid1)
    inv1(d1s, s1s, 1, p1s, mid1, near1)

    far3, mid3, near3 = (v.reshape(1, 1, 1) for v in limits(noise, 3))
    lane3 = lax.broadcasted_iota(jnp.int32, (n3, h3, LANES), 2)
    b_dd, b_ds, b_sd = shrink(b3[0], far3), shrink(b3[1], mid3), shrink(b3[2], mid3)
    b_ss = jnp.where(lane3 < cz // 8, b3[3], shrink(b3[3], near3))

    def inverse_x(det, smo):
        one = smo + det
        even, odd = undo(det[:-1], one[1:], one[:-1])
        return weave(even, odd)

    y_d = inverse_x(b_dd, b_sd)
    y_s = inverse_x(b_ds, b_ss)
    one = y_s + pltpu.roll(y_d, h3 - 1, 1)
    even, odd = undo(y_d, one, pltpu.roll(one, 1, 1))
    r2[:, pl.ds(0, h3, stride=2), :] = even
    r2[:, pl.ds(1, h3, stride=2), :] = odd
    back = times(r2[...].reshape(x2 * yrows, LANES), v3).reshape(x2, yrows, LANES)

    far2, mid2, near2 = limits(noise, 2)
    lane2 = lax.broadcasted_iota(jnp.int32, (x2, yrows, LANES), 2)
    ss[...] = jnp.where(lane2 < cz // 4, back, shrink(ep3[1 : qx + 3], near2.reshape(1, 1, 1)))

    def one_x(n):
        d_d = shrink(dd[n], far2)
        d_s = shrink(ds[n], mid2)
        s_d = shrink(sd[n], mid2)
        return d_d, d_s, s_d + d_d, ss[n] + d_s

    def inv2(n, carry):
        d_d, d_s, b_d, b_s = carry
        after = one_x(n + 1)
        pair_d = undo(d_d, after[2], b_d)
        pair_s = undo(d_s, after[3], b_s)
        for i in range(2):
            y_d, y_s = pair_d[i], pair_s[i]
            one = y_s + pltpu.roll(y_d, yrows - 1, 0)
            even, odd = undo(y_d, one, pltpu.roll(one, 1, 0))
            r1[2 * n + i, pl.ds(0, yrows, stride=2), :] = even
            r1[2 * n + i, pl.ds(1, yrows, stride=2), :] = odd
        return after

    lax.fori_loop(0, qx + 1, inv2, one_x(0), unroll=3)
    x1, y1 = hx + 2, hy + PAD
    back = times(r1[:, PAD : PAD + y1].reshape(x1 * y1, LANES), v2).reshape(x1, y1, LANES)
    s0[...] = back[1:]
    inv1(d1s, s1s, 0, p1s, mid1, None)

    def inv1_y(n):
        for h in range(2):
            y_d = p1d[n, h, 0:hy]
            y_n = p1d[n, h, 1 : hy + 1]
            s = p1s[n, h, PAD : PAD + hy]
            s_b = p1s[n, h, PAD - 1 : PAD - 1 + hy]
            even, odd = undo(y_d, s + y_n, s_b + y_d)
            o1[n, h, pl.ds(0, hy, stride=2), :] = even
            o1[n, h, pl.ds(1, hy, stride=2), :] = odd

    layers = 8
    outs = []
    for n in range(layers):
        inv1_y(n)
    for i in range(cx // layers):
        for n in range((i + 1) * layers, min((i + 2) * layers, cx)):
            inv1_y(n)
        xs = slice(i * layers, (i + 1) * layers)
        rows = jnp.concatenate(
            [o1[xs, h].reshape(layers * cy, LANES) for h in range(2)], axis=1)
        ob[xs] = times(rows, v1).reshape(layers, cy, cz)
        c = pltpu.make_async_copy(ob.at[xs], out.at[xs], osem.at[i])
        c.start()
        outs.append(c)
    for c in outs:
        c.wait()


def on_device(nx, ny, volume):
    cx, cy, cz = volume.shape
    hx, hy, qx, qy = cx // 2, cy // 2, cx // 4, cy // 4
    n3, h3 = qx // 2 + 2, qy // 2 + PAD
    f32 = jnp.float32
    count = cx * nx * cy * ny * cz // 8
    w1 = forward_matrix(cz)
    weights = [
        halves(w1, cz), halves(w1[:, : cz // 2] @ forward_matrix(cz // 2), cz)[:, :, : cz // 2],
        halves(forward_matrix(cz // 4), LANES), halves(inverse_matrix(cz), cz),
        halves(inverse_matrix(cz // 2), LANES), halves(inverse_matrix(cz // 4), LANES),
    ]
    vmem = lambda *s: pltpu.VMEM(s, f32)
    ey, ey2, ey3 = cy + 2 * PAD, hy + 2 * PAD, qy + 2 * PAD
    wide = lambda *s: pltpu.VMEM((2,) + s, jnp.bfloat16)
    made = (
        *[vmem(hx + 1, 2, hy + PAD, LANES) for _ in range(4)],
        *[vmem(qx + 2, ey3, LANES) for _ in range(3)],
        vmem(qx + 4, ey3, LANES), vmem(4, n3, h3, LANES), vmem(1, LANES),
        wide(cz, cz), wide(LANES, LANES), wide(LANES, LANES),
    )
    rows = 4 * cy + 4 * cx + 8 + 6 * (hy + 2 * PAD) + 2 * hx * PAD + nx * ny
    scratch = [
        wide(cz, cz), wide(cz, LANES), wide(LANES, LANES),
        vmem(cx, 2, ey, LANES), vmem(2, 2, ey, LANES), vmem(2, 2, cy, LANES),
        vmem(2, cx, 2, 1, LANES), vmem(2, cx, 2, 1, LANES),
        vmem(2, 2, 2, 1, LANES), vmem(2, 2, 2, 1, LANES),
        vmem(hx + 1, 2, ey, LANES), vmem(hx + 1, 2, ey, LANES),
        vmem(hx, ey2, LANES), vmem(4, hy, LANES), vmem(2, hy, LANES),
        vmem(4, ey2, LANES), vmem(2, ey2, LANES),
        vmem(qx + 2, ey2, LANES), vmem(qx + 4, ey2, LANES),
        vmem(n3, ey3, LANES), vmem(n3, ey3, LANES),
        vmem(1, LANES), vmem(nx * ny - 1, 1, LANES), vmem(rows, 1, LANES),
        pltpu.SemaphoreType.DMA((1,)), pltpu.SemaphoreType.DMA((4,)),
        pltpu.SemaphoreType.DMA((2,)), pltpu.SemaphoreType.DMA((6,)),
    ]
    near = pl.BlockSpec(memory_space=pltpu.VMEM)
    passed = pl.pallas_call(
        functools.partial(kernel, (cx, cy, cz), nx, ny),
        out_shape=made,
        in_specs=[pl.BlockSpec(memory_space=pltpu.HBM)] * 7,
        out_specs=(near,) * len(made),
        scratch_shapes=scratch,
        compiler_params=pltpu.CompilerParams(
            collective_id=0, has_side_effects=True, vmem_limit_bytes=40 * 1024 * 1024),
    )(volume, *[jnp.asarray(w) for w in weights])
    return pl.pallas_call(
        functools.partial(finish, (cx, cy, cz), count),
        out_shape=jax.ShapeDtypeStruct(volume.shape, f32),
        in_specs=[near] * len(made),
        out_specs=pl.BlockSpec(memory_space=pltpu.HBM),
        scratch_shapes=[
            vmem(qx + 2, ey3, LANES), vmem(qx + 2, ey3, LANES), vmem(hx + 2, 2 * ey3, LANES),
            vmem(hx + 1, hy + PAD, LANES),
            vmem(cx, 2, hy + PAD, LANES), vmem(cx, 2, hy + PAD, LANES),
            vmem(cx, 2, cy, LANES), vmem(cx, cy, cz), pltpu.SemaphoreType.DMA((cx // 8,)),
        ],
        compiler_params=pltpu.CompilerParams(vmem_limit_bytes=24 * 1024 * 1024),
    )(*passed)


def solution(mesh):
    spec = P("gx", "gy", None)
    body = functools.partial(on_device, mesh.shape["gx"], mesh.shape["gy"])
    return jax.shard_map(body, mesh=mesh, in_specs=(spec,), out_specs=spec, check_vma=False)
```

```python
import functools
import math

import jax
import jax.numpy as jnp
import numpy as np
from jax import lax
from jax.experimental import pallas as pl
from jax.experimental.pallas import tpu as pltpu
from jax.sharding import PartitionSpec as P

ROOT3 = math.sqrt(3.0)
NEAR = math.sqrt(3.0) / 4.0
FAR = (math.sqrt(3.0) - 2.0) / 4.0
LOW = (math.sqrt(3.0) - 1.0) / math.sqrt(2.0)
HIGH = (math.sqrt(3.0) + 1.0) / math.sqrt(2.0)
LANES = 128
PAD = 8


def forward_matrix(size):
    lines = np.eye(size)
    even, odd = lines[:, 0::2], lines[:, 1::2]
    smooth = even + ROOT3 * odd
    detail = odd - NEAR * smooth - FAR * np.roll(smooth, 1, 1)
    smooth = smooth - np.roll(detail, -1, 1)
    return np.concatenate([LOW * smooth, HIGH * detail], 1)


def inverse_matrix(size):
    lines = np.eye(size)
    smooth, detail = lines[:, : size // 2] / LOW, lines[:, size // 2 :] / HIGH
    first = smooth + np.roll(detail, -1, 1)
    odd = detail + NEAR * first + FAR * np.roll(first, 1, 1)
    even = first - ROOT3 * odd
    return np.stack([even, odd], 2).reshape(size, size)


def halves(matrix, size):
    full = np.zeros((size, size))
    full[: matrix.shape[0], : matrix.shape[1]] = matrix
    high = full.astype(jnp.bfloat16)
    low = (full - high.astype(np.float64)).astype(jnp.bfloat16)
    return np.stack([high, low])


def times(values, w_ref):
    high = values.astype(jnp.bfloat16)
    low = (values - high.astype(jnp.float32)).astype(jnp.bfloat16)
    dot = functools.partial(jnp.dot, preferred_element_type=jnp.float32)
    return dot(high, w_ref[0]) + (dot(low, w_ref[0]) + dot(high, w_ref[1]))


def shrink(values, noise):
    return values - jnp.clip(values, -noise, noise)


def sums(even, odd):
    smooth = even + ROOT3 * odd
    return smooth, odd - NEAR * smooth


def undo(detail, first, before):
    odd = detail + NEAR * first + FAR * before
    return first - ROOT3 * odd, odd


def weave(even, odd):
    both = jnp.stack([even, odd], axis=1)
    return both.reshape((2 * even.shape[0],) + even.shape[1:])


def forward_rows(even, odd):
    axis = even.ndim - 2
    smooth, part = sums(even, odd)
    detail = part - FAR * pltpu.roll(smooth, 1, axis)
    return detail, smooth - pltpu.roll(detail, even.shape[axis] - 1, axis)


def limits(noise, level):
    base = noise * (1.0 / LOW ** (2 * (level - 1)))
    return base * (1.0 / (HIGH * HIGH)), base * (1.0 / (HIGH * LOW)), base * (1.0 / (LOW * LOW))


def kernel(shape, nx, ny, vol, g1, gu, g3, g4, g5, g6,
           d1d, d1s, s1d, s1s, dd, ds, sd, ep3, b3, noise, v1, v2, v3,
           w1, wu, w3,
           e1, hx1, sx1, hy1, sy1, hc1, sc1, xd1, xs1,
           e2, xl, xh, xlow, xhigh, xd2, xs2, t3d, t3s,
           mine, rows_in, dummy, send, recv, lsem, wsem):
    cx, cy, cz = shape
    hx, hy, qx, qy = cx // 2, cy // 2, cx // 4, cy // 4
    ix, iy = lax.axis_index("gx"), lax.axis_index("gy")

    def device(dx, dy):
        return (lax.rem(ix + dx + nx, nx), lax.rem(iy + dy + ny, ny))

    near = [(dx, dy) for dx in (-1, 0, 1) for dy in (-1, 0, 1) if dx or dy]
    peers = [(dx, dy) for dx in range(nx) for dy in range(ny) if dx or dy]
    taken = {(dx % nx, dy % ny) for dx, dy in near}
    barrier = pltpu.get_barrier_semaphore()

    def greet(dx, dy):
        pl.semaphore_signal(barrier, inc=1, device_id=device(dx, dy),
                            device_id_type=pl.DeviceIdType.MESH)

    for d in sorted(taken):
        greet(*d)
    loads = [
        pltpu.make_async_copy(
            vol.at[:, :, pl.ds(h * LANES, LANES)],
            e1.at[:, h, pl.ds(PAD, cy), :], lsem.at[h])
        for h in range(2)
    ]
    for c in loads:
        c.start()
    for d in peers:
        if d not in taken:
            greet(*d)
    weights = [
        pltpu.make_async_copy(src, dst, wsem.at[i])
        for i, (src, dst) in enumerate(
            zip((g1, gu, g3, g4, g5, g6), (w1, wu, w3, v1, v2, v3)))
    ]
    for c in weights:
        c.start()

    sent = [0]

    def post(src, dst, dx, dy, group):
        sent[0] += math.prod(src.shape) // LANES
        pltpu.make_async_remote_copy(
            src_ref=src, dst_ref=dst, send_sem=send.at[0], recv_sem=recv.at[group],
            device_id=device(dx, dy), device_id_type=pl.DeviceIdType.MESH).start()
        return math.prod(src.shape) // LANES

    def land(sem, rows):
        part = dummy.at[pl.ds(0, rows)]
        pltpu.make_async_copy(part, part, sem).wait()

    ep3[:, 0 : PAD // 2] = jnp.zeros((qx + 4, PAD // 2, LANES), jnp.float32)
    ep3[:, PAD // 2 + hy // 2 + PAD :] = jnp.zeros((qx + 4, PAD // 2, LANES), jnp.float32)
    for ref in (dd, ds, sd):
        ref[:, 0 : PAD // 2] = jnp.zeros((qx + 2, PAD // 2, LANES), jnp.float32)
        ref[:, PAD // 2 + hy // 2 + PAD :] = jnp.zeros((qx + 2, PAD // 2, LANES), jnp.float32)

    for c in loads:
        c.wait()

    top = PAD + cy
    sx1[1] = sums(e1[0, :, PAD:top], e1[1, :, PAD:top])[1]
    sy1[1] = sums(e1[:, :, PAD : PAD + 1], e1[:, :, PAD + 1 : PAD + 2])[1]
    sx1[0] = sums(e1[cx - 2, :, PAD:top], e1[cx - 1, :, PAD:top])[0]
    sy1[0] = sums(e1[:, :, top - 2 : top - 1], e1[:, :, top - 1 : top])[0]
    for x in range(2):
        sc1[x, 1] = sums(sx1[x, :, 0:1], sx1[x, :, 1:2])[1]
        sc1[x, 0] = sums(sx1[x, :, cy - 2 : cy - 1], sx1[x, :, cy - 1 : cy])[0]
    pl.semaphore_wait(barrier, len(peers))
    step = (1, -1)
    post_x = lambda x, g: post(sx1.at[x], hx1.at[x, :, pl.ds(PAD, cy), :], step[x], 0, g)
    post_y = lambda y, g: post(sy1.at[y], hy1.at[y], 0, step[y], g)
    post_c = lambda x, y, g: post(sc1.at[x, y], hc1.at[x, y], step[x], step[y], g)
    now1 = post_c(1, 1, 0) + post_x(1, 0) + post_y(1, 0)
    later1 = (post_c(0, 1, 1) + post_c(1, 0, 1) + post_c(0, 0, 1)
              + post_x(0, 1) + post_y(0, 1))

    def place(ref, rows, side):
        if side == 0:
            ref[..., PAD - 2 : PAD - 1, :] = rows
            ref[..., PAD - 1 : PAD, :] = jnp.zeros_like(rows)
        else:
            ref[..., top : top + 1, :] = -ROOT3 * rows
            ref[..., top + 1 : top + 2, :] = rows

    def pair1(n, rows=slice(None)):
        return sums(e1[2 * n, :, rows], e1[2 * n + 1, :, rows])

    def lift1(rows):
        def step(n, carry):
            _, part_n = pair1(n, rows)
            before, _ = pair1(n - 1, rows)
            detail = part_n - FAR * before
            xd1[n, :, rows] = detail
            xs1[n, :, rows] = before - detail
            return carry

        lax.fori_loop(1, hx, step, 0)

    def coarse1(n, first, count):
        for h in range(2):
            load = lambda start: xs1[n, h, pl.ds(start + 2 * first, count, stride=2), :]
            s0, _ = sums(load(PAD), load(PAD + 1))
            _, tp = sums(load(PAD + 2), load(PAD + 3))
            s1s[n, h, PAD + first : PAD + first + count] = s0 - (tp - FAR * s0)

    def coarse1_inner(n, carry):
        coarse1(n, 0, hy)
        return carry

    def coarse1_top(n, carry):
        coarse1(n, hy - 1, 1)
        return carry

    lift1(slice(PAD, top))
    lax.fori_loop(1, hx, coarse1_inner, 0)
    for c in weights:
        c.wait()
    land(recv.at[0], now1)
    place(e1, hy1[1], 1)
    place(hx1.at[1], hc1[1, 1], 1)
    lift1(slice(top, top + 2))
    edge, _ = pair1(hx - 1)
    edge_d = hx1[1] - FAR * edge
    xd1[hx] = edge_d
    xs1[hx] = edge - edge_d
    lax.fori_loop(1, hx, coarse1_top, 0)
    coarse1(hx, 0, hy)

    def lines(ref, xs, ys):
        n = (xs.stop - xs.start) * (ys.stop - ys.start)
        return jnp.concatenate([ref[xs, h, ys].reshape(n, LANES) for h in range(2)], axis=1)

    chunk = hx // 2
    own = slice(PAD, PAD + hy)
    for i in range(2):
        rows = lines(s1s, slice(1 + i * chunk, 1 + (i + 1) * chunk), own)
        e2[i * chunk : (i + 1) * chunk, own] = times(rows, wu).reshape(chunk, hy, LANES)

    def pair2(m, rows):
        return sums(e2[2 * m, rows], e2[2 * m + 1, rows])

    def coarse2(m, rows):
        return pair2(m, rows)[0] * (1.0 + FAR) - pair2(m + 1, rows)[1]

    xl[0] = pair2(qx - 2, own)[0]
    xl[1] = e2[hx - 2, own]
    xl[2] = e2[hx - 1, own]
    xl[3] = sums(coarse2(qx - 4, own), coarse2(qx - 3, own))[0]
    xh[0] = pair2(0, own)[1]
    xh[1] = sums(coarse2(0, own), coarse2(1, own))[1]
    y_own, y_low, y_high = pl.ds(PAD, hy), pl.ds(0, PAD), pl.ds(PAD + hy, PAD)
    s_own, s_first, s_last = pl.ds(0, hy), pl.ds(0, PAD), pl.ds(hy - PAD, PAD)
    round2 = 0
    for rows_s, rows_d, dy in ((s_last, y_low, 1), (s_first, y_high, -1), (s_own, y_own, 0)):
        round2 += post(xl.at[:, rows_s, :], xlow.at[:, rows_d, :], 1, dy, 2)
        round2 += post(xh.at[:, rows_s, :], xhigh.at[:, rows_d, :], -1, dy, 2)
    round2 += post(e2.at[:, pl.ds(PAD, PAD), :], e2.at[:, y_high, :], 0, -1, 2)
    round2 += post(e2.at[:, pl.ds(hy, PAD), :], e2.at[:, y_low, :], 0, 1, 2)

    land(recv.at[1], later1)
    place(e1, hy1[0], 0)
    place(hx1.at[1], hc1[1, 0], 0)
    place(hx1.at[0], hc1[0, 0], 0)
    place(hx1.at[0], hc1[0, 1], 1)
    first_s, first_t = pair1(0)
    first_d = first_t - FAR * hx1[0]
    xd1[0] = first_d
    xs1[0] = hx1[0] - first_d
    low = slice(PAD - 2, PAD)

    lift1(low)
    edge, _ = sums(e1[cx - 2, :, low], e1[cx - 1, :, low])
    edge_d = hx1[1, :, low] - FAR * edge
    xd1[hx, :, low] = edge_d
    xs1[hx, :, low] = edge - edge_d

    def cols1(src, det, smo):
        def step(n, carry):
            for h in range(2):
                load = lambda start: src[n, h, pl.ds(start, hy + 1, stride=2), :]
                s0, t0 = sums(load(PAD), load(PAD + 1))
                sm, _ = sums(load(PAD - 2), load(PAD - 1))
                d = t0 - FAR * sm
                det[n, h, 0 : hy + 1] = d
                smo[n, h, PAD - 1 : PAD + hy] = sm - d
            return carry

        lax.fori_loop(0, hx + 1, step, 0)

    rows1 = hy + PAD
    parts1 = ((0, chunk), (chunk, hx + 1))

    def depth1(ref):
        magnitude = jnp.zeros((PAD, LANES), jnp.float32)
        for lo, hi in parts1:
            rows = lines(ref, slice(lo, hi), slice(0, rows1))
            if ref is s1s:
                ref[lo:hi, 1] = times(rows, w1.at[:, :, LANES : 2 * LANES]).reshape(
                    hi - lo, rows1, LANES)
                continue
            got = times(rows, w1)
            for h in range(2):
                ref[lo:hi, h] = got[:, h * LANES : (h + 1) * LANES].reshape(hi - lo, rows1, LANES)
            if ref is d1d:
                inside = got[:, LANES:].reshape(hi - lo, rows1, LANES)[:chunk, :hy]
                magnitude = magnitude + jnp.sum(
                    jnp.abs(inside).reshape(chunk * hy // PAD, PAD, LANES), axis=0)
        return magnitude

    cols1(xd1, d1d, d1s)
    mine[...] = jnp.sum(depth1(d1d), axis=0, keepdims=True)
    landed = 0
    for k, d in enumerate(peers):
        landed += post(mine, rows_in.at[k], d[0], d[1], 3)

    cols1(xs1, s1d, s1s)
    depth1(d1s)
    depth1(s1d)
    depth1(s1s)

    land(recv.at[2], round2)
    every = slice(0, hy + 2 * PAD)
    before = xlow[0]
    xs2[0] = xlow[3]
    for m in range(-1, qx + 1):
        if m == qx:
            smooth, part = None, xhigh[0]
        elif m == -1:
            smooth, part = sums(xlow[1], xlow[2])
        else:
            smooth, part = pair2(m, every)
        detail = part - FAR * before
        xd2[m + 1] = detail
        xs2[m + 2] = before - detail
        before = smooth
    xs2[qx + 3] = xhigh[1]
    pairs = hy // 2 + PAD

    def rows2(src):
        return forward_rows(src[:, pl.ds(0, pairs, stride=2), :],
                            src[:, pl.ds(1, pairs, stride=2), :])

    mid = slice(PAD // 2, PAD // 2 + pairs)
    dd[:, mid], ds[:, mid] = rows2(xd2)
    det, smo = rows2(xs2)
    sd[:, mid] = det[1 : qx + 3]
    ep3[:, mid] = smo

    n_own, n3, h3 = qx // 2, qx // 2 + 2, qy // 2 + PAD
    low_s, low_t = [ep3[0]], [None]
    for n in range(n_own + 1):
        s, t = sums(ep3[1 + 2 * n], ep3[2 + 2 * n])
        low_s.append(s)
        low_t.append(t)
    low_t.append(ep3[qx + 3])
    for n in range(n3):
        detail = low_t[n + 1] - FAR * low_s[n]
        t3d[n] = detail
        t3s[n] = low_s[n] - detail
    bands = []
    for src in (t3d, t3s):
        bands += forward_rows(src[:, pl.ds(0, h3, stride=2), :], src[:, pl.ds(1, h3, stride=2), :])
    for i, band in enumerate(bands):
        b3[i] = times(band.reshape(n3 * h3, LANES), w3).reshape(n3, h3, LANES)

    land(recv.at[3], landed)
    acc = mine[...]
    for k in range(len(peers)):
        acc = acc + rows_in[k]
    noise[...] = acc
    land(send.at[0], sent[0])


def finish(shape, count_all, d1d, d1s, s1d, s1s, dd, ds, sd, ep3, b3, total, v1, v2, v3, out,
           ss, r2, r1, s0, p1d, p1s, o1, ob, osem):
    cx, cy, cz = shape
    hx, hy, qx, qy = cx // 2, cy // 2, cx // 4, cy // 4
    n3, h3, x2, yrows = qx // 2 + 2, qy // 2 + PAD, qx + 2, qy + 2 * PAD
    noise = jnp.sum(total[...], axis=(0, 1), keepdims=True) * (
        HIGH * HIGH * math.sqrt(math.pi / 2.0) / count_all)

    far1, mid1, near1 = limits(noise, 1)

    def inv1(det, smo, h, dst, limit_d, limit_s):
        def one_x(n):
            d = shrink(det[n, h], limit_d)
            s = s0[n] if limit_s is None else shrink(smo[n, h], limit_s)
            return d, s + d

        def step(n, carry):
            d, before = carry
            after, one = one_x(n + 1)
            even, odd = undo(d, one, before)
            dst[2 * n, h] = even
            dst[2 * n + 1, h] = odd
            return after, one

        lax.fori_loop(0, hx, step, one_x(0), unroll=4)

    for h in range(2):
        inv1(d1d, s1d, h, p1d, far1, mid1)
    inv1(d1s, s1s, 1, p1s, mid1, near1)

    far3, mid3, near3 = (v.reshape(1, 1, 1) for v in limits(noise, 3))
    lane3 = lax.broadcasted_iota(jnp.int32, (n3, h3, LANES), 2)
    b_dd, b_ds, b_sd = shrink(b3[0], far3), shrink(b3[1], mid3), shrink(b3[2], mid3)
    b_ss = jnp.where(lane3 < cz // 8, b3[3], shrink(b3[3], near3))

    def inverse_x(det, smo):
        one = smo + det
        even, odd = undo(det[:-1], one[1:], one[:-1])
        return weave(even, odd)

    y_d = inverse_x(b_dd, b_sd)
    y_s = inverse_x(b_ds, b_ss)
    one = y_s + pltpu.roll(y_d, h3 - 1, 1)
    even, odd = undo(y_d, one, pltpu.roll(one, 1, 1))
    r2[:, pl.ds(0, h3, stride=2), :] = even
    r2[:, pl.ds(1, h3, stride=2), :] = odd
    back = times(r2[...].reshape(x2 * yrows, LANES), v3).reshape(x2, yrows, LANES)

    far2, mid2, near2 = limits(noise, 2)
    lane2 = lax.broadcasted_iota(jnp.int32, (x2, yrows, LANES), 2)
    ss[...] = jnp.where(lane2 < cz // 4, back, shrink(ep3[1 : qx + 3], near2.reshape(1, 1, 1)))

    def one_x(n):
        d_d = shrink(dd[n], far2)
        d_s = shrink(ds[n], mid2)
        s_d = shrink(sd[n], mid2)
        return d_d, d_s, s_d + d_d, ss[n] + d_s

    def inv2(n, carry):
        d_d, d_s, b_d, b_s = carry
        after = one_x(n + 1)
        pair_d = undo(d_d, after[2], b_d)
        pair_s = undo(d_s, after[3], b_s)
        for i in range(2):
            y_d, y_s = pair_d[i], pair_s[i]
            one = y_s + pltpu.roll(y_d, yrows - 1, 0)
            even, odd = undo(y_d, one, pltpu.roll(one, 1, 0))
            r1[2 * n + i, pl.ds(0, yrows, stride=2), :] = even
            r1[2 * n + i, pl.ds(1, yrows, stride=2), :] = odd
        return after

    lax.fori_loop(0, qx + 1, inv2, one_x(0), unroll=3)
    x1, y1 = hx + 2, hy + PAD
    back = times(r1[:, PAD : PAD + y1].reshape(x1 * y1, LANES), v2).reshape(x1, y1, LANES)
    s0[...] = back[1:]
    inv1(d1s, s1s, 0, p1s, mid1, None)

    def inv1_y(n):
        for h in range(2):
            y_d = p1d[n, h, 0:hy]
            y_n = p1d[n, h, 1 : hy + 1]
            s = p1s[n, h, PAD : PAD + hy]
            s_b = p1s[n, h, PAD - 1 : PAD - 1 + hy]
            even, odd = undo(y_d, s + y_n, s_b + y_d)
            o1[n, h, pl.ds(0, hy, stride=2), :] = even
            o1[n, h, pl.ds(1, hy, stride=2), :] = odd

    layers = 8
    outs = []
    for n in range(layers):
        inv1_y(n)
    for i in range(cx // layers):
        for n in range((i + 1) * layers, min((i + 2) * layers, cx)):
            inv1_y(n)
        xs = slice(i * layers, (i + 1) * layers)
        rows = jnp.concatenate(
            [o1[xs, h].reshape(layers * cy, LANES) for h in range(2)], axis=1)
        ob[xs] = times(rows, v1).reshape(layers, cy, cz)
        c = pltpu.make_async_copy(ob.at[xs], out.at[xs], osem.at[i])
        c.start()
        outs.append(c)
    for c in outs:
        c.wait()


def on_device(nx, ny, volume):
    cx, cy, cz = volume.shape
    hx, hy, qx, qy = cx // 2, cy // 2, cx // 4, cy // 4
    n3, h3 = qx // 2 + 2, qy // 2 + PAD
    f32 = jnp.float32
    count = cx * nx * cy * ny * cz // 8
    w1 = forward_matrix(cz)
    weights = [
        halves(w1, cz), halves(w1[:, : cz // 2] @ forward_matrix(cz // 2), cz)[:, :, : cz // 2],
        halves(forward_matrix(cz // 4), LANES), halves(inverse_matrix(cz), cz),
        halves(inverse_matrix(cz // 2), LANES), halves(inverse_matrix(cz // 4), LANES),
    ]
    vmem = lambda *s: pltpu.VMEM(s, f32)
    ey, ey2, ey3 = cy + 2 * PAD, hy + 2 * PAD, qy + 2 * PAD
    wide = lambda *s: pltpu.VMEM((2,) + s, jnp.bfloat16)
    made = (
        *[vmem(hx + 1, 2, hy + PAD, LANES) for _ in range(4)],
        *[vmem(qx + 2, ey3, LANES) for _ in range(3)],
        vmem(qx + 4, ey3, LANES), vmem(4, n3, h3, LANES), vmem(1, LANES),
        wide(cz, cz), wide(LANES, LANES), wide(LANES, LANES),
    )
    rows = 4 * cy + 4 * cx + 8 + 6 * (hy + 2 * PAD) + 2 * hx * PAD + nx * ny
    scratch = [
        wide(cz, cz), wide(cz, LANES), wide(LANES, LANES),
        vmem(cx, 2, ey, LANES), vmem(2, 2, ey, LANES), vmem(2, 2, cy, LANES),
        vmem(2, cx, 2, 1, LANES), vmem(2, cx, 2, 1, LANES),
        vmem(2, 2, 2, 1, LANES), vmem(2, 2, 2, 1, LANES),
        vmem(hx + 1, 2, ey, LANES), vmem(hx + 1, 2, ey, LANES),
        vmem(hx, ey2, LANES), vmem(4, hy, LANES), vmem(2, hy, LANES),
        vmem(4, ey2, LANES), vmem(2, ey2, LANES),
        vmem(qx + 2, ey2, LANES), vmem(qx + 4, ey2, LANES),
        vmem(n3, ey3, LANES), vmem(n3, ey3, LANES),
        vmem(1, LANES), vmem(nx * ny - 1, 1, LANES), vmem(rows, 1, LANES),
        pltpu.SemaphoreType.DMA((1,)), pltpu.SemaphoreType.DMA((4,)),
        pltpu.SemaphoreType.DMA((2,)), pltpu.SemaphoreType.DMA((6,)),
    ]
    near = pl.BlockSpec(memory_space=pltpu.VMEM)
    passed = pl.pallas_call(
        functools.partial(kernel, (cx, cy, cz), nx, ny),
        out_shape=made,
        in_specs=[pl.BlockSpec(memory_space=pltpu.HBM)] * 7,
        out_specs=(near,) * len(made),
        scratch_shapes=scratch,
        compiler_params=pltpu.CompilerParams(
            collective_id=0, has_side_effects=True, vmem_limit_bytes=56 * 1024 * 1024),
    )(volume, *[jnp.asarray(w) for w in weights])
    return pl.pallas_call(
        functools.partial(finish, (cx, cy, cz), count),
        out_shape=jax.ShapeDtypeStruct(volume.shape, f32),
        in_specs=[near] * len(made),
        out_specs=pl.BlockSpec(memory_space=pltpu.HBM),
        scratch_shapes=[
            vmem(qx + 2, ey3, LANES), vmem(qx + 2, ey3, LANES), vmem(hx + 2, 2 * ey3, LANES),
            vmem(hx + 1, hy + PAD, LANES),
            vmem(cx, 2, hy + PAD, LANES), vmem(cx, 2, hy + PAD, LANES),
            vmem(cx, 2, cy, LANES), vmem(cx, cy, cz), pltpu.SemaphoreType.DMA((cx // 8,)),
        ],
        compiler_params=pltpu.CompilerParams(vmem_limit_bytes=24 * 1024 * 1024),
    )(*passed)


def solution(mesh):
    spec = P("gx", "gy", None)
    body = functools.partial(on_device, mesh.shape["gx"], mesh.shape["gy"])
    return jax.shard_map(body, mesh=mesh, in_specs=(spec,), out_specs=spec, check_vma=False)
```

```python
import functools
import math

import jax
import jax.numpy as jnp
import numpy as np
from jax import lax
from jax.experimental import pallas as pl
from jax.experimental.pallas import tpu as pltpu
from jax.sharding import PartitionSpec as P

ROOT3 = math.sqrt(3.0)
NEAR = math.sqrt(3.0) / 4.0
FAR = (math.sqrt(3.0) - 2.0) / 4.0
LOW = (math.sqrt(3.0) - 1.0) / math.sqrt(2.0)
HIGH = (math.sqrt(3.0) + 1.0) / math.sqrt(2.0)
LANES = 128
PAD = 8


def forward_matrix(size):
    lines = np.eye(size)
    even, odd = lines[:, 0::2], lines[:, 1::2]
    smooth = even + ROOT3 * odd
    detail = odd - NEAR * smooth - FAR * np.roll(smooth, 1, 1)
    smooth = smooth - np.roll(detail, -1, 1)
    return np.concatenate([LOW * smooth, HIGH * detail], 1)


def inverse_matrix(size):
    lines = np.eye(size)
    smooth, detail = lines[:, : size // 2] / LOW, lines[:, size // 2 :] / HIGH
    first = smooth + np.roll(detail, -1, 1)
    odd = detail + NEAR * first + FAR * np.roll(first, 1, 1)
    even = first - ROOT3 * odd
    return np.stack([even, odd], 2).reshape(size, size)


def halves(matrix, size):
    full = np.zeros((size, size))
    full[: matrix.shape[0], : matrix.shape[1]] = matrix
    high = full.astype(jnp.bfloat16)
    low = (full - high.astype(np.float64)).astype(jnp.bfloat16)
    return np.stack([high, low])


def times(values, w_ref):
    high = values.astype(jnp.bfloat16)
    low = (values - high.astype(jnp.float32)).astype(jnp.bfloat16)
    dot = functools.partial(jnp.dot, preferred_element_type=jnp.float32)
    return dot(high, w_ref[0]) + (dot(low, w_ref[0]) + dot(high, w_ref[1]))


def shrink(values, noise):
    return values - jnp.clip(values, -noise, noise)


def sums(even, odd):
    smooth = even + ROOT3 * odd
    return smooth, odd - NEAR * smooth


def undo(detail, first, before):
    odd = detail + NEAR * first + FAR * before
    return first - ROOT3 * odd, odd


def weave(even, odd):
    both = jnp.stack([even, odd], axis=1)
    return both.reshape((2 * even.shape[0],) + even.shape[1:])


def forward_rows(even, odd):
    axis = even.ndim - 2
    smooth, part = sums(even, odd)
    detail = part - FAR * pltpu.roll(smooth, 1, axis)
    return detail, smooth - pltpu.roll(detail, even.shape[axis] - 1, axis)


def limits(noise, level):
    base = noise * (1.0 / LOW ** (2 * (level - 1)))
    return base * (1.0 / (HIGH * HIGH)), base * (1.0 / (HIGH * LOW)), base * (1.0 / (LOW * LOW))


def kernel(shape, nx, ny, vol, g1, g2, g3, g4, g5, g6,
           d1d, d1s, s1d, s1s, dd, ds, sd, ep3, b3, noise, v1, v2, v3,
           w1, w2, w3,
           e1, hx1, sx1, hy1, sy1, hc1, sc1, xd1, xs1,
           e2, xl, xh, xlow, xhigh, xd2, xs2, t3d, t3s,
           mine, rows_in, dummy, send, recv, lsem, wsem):
    cx, cy, cz = shape
    hx, hy, qx, qy = cx // 2, cy // 2, cx // 4, cy // 4
    ix, iy = lax.axis_index("gx"), lax.axis_index("gy")

    def device(dx, dy):
        return (lax.rem(ix + dx + nx, nx), lax.rem(iy + dy + ny, ny))

    near = [(dx, dy) for dx in (-1, 0, 1) for dy in (-1, 0, 1) if dx or dy]
    peers = [(dx, dy) for dx in range(nx) for dy in range(ny) if dx or dy]
    taken = {(dx % nx, dy % ny) for dx, dy in near}
    barrier = pltpu.get_barrier_semaphore()

    def greet(dx, dy):
        pl.semaphore_signal(barrier, inc=1, device_id=device(dx, dy),
                            device_id_type=pl.DeviceIdType.MESH)

    for d in sorted(taken):
        greet(*d)
    loads = [
        pltpu.make_async_copy(
            vol.at[:, :, pl.ds(h * LANES, LANES)],
            e1.at[:, h, pl.ds(PAD, cy), :], lsem.at[h])
        for h in range(2)
    ]
    for c in loads:
        c.start()
    for d in peers:
        if d not in taken:
            greet(*d)
    first_weight = pltpu.make_async_copy(g1, w1, wsem.at[0])
    first_weight.start()
    more = list(zip((g2, g3, g4, g5, g6), (w2, w3, v1, v2, v3)))
    for src, dst in more:
        pltpu.make_async_copy(src, dst, wsem.at[1]).start()

    sent = [0]

    def post(src, dst, dx, dy, group):
        sent[0] += math.prod(src.shape) // LANES
        pltpu.make_async_remote_copy(
            src_ref=src, dst_ref=dst, send_sem=send.at[0], recv_sem=recv.at[group],
            device_id=device(dx, dy), device_id_type=pl.DeviceIdType.MESH).start()
        return math.prod(src.shape) // LANES

    def land(sem, rows):
        part = dummy.at[pl.ds(0, rows)]
        pltpu.make_async_copy(part, part, sem).wait()

    ep3[:, 0 : PAD // 2] = jnp.zeros((qx + 4, PAD // 2, LANES), jnp.float32)
    ep3[:, PAD // 2 + hy // 2 + PAD :] = jnp.zeros((qx + 4, PAD // 2, LANES), jnp.float32)
    for ref in (dd, ds, sd):
        ref[:, 0 : PAD // 2] = jnp.zeros((qx + 2, PAD // 2, LANES), jnp.float32)
        ref[:, PAD // 2 + hy // 2 + PAD :] = jnp.zeros((qx + 2, PAD // 2, LANES), jnp.float32)

    top = PAD + cy
    own1, own = slice(PAD, top), slice(PAD, PAD + hy)
    for c in loads:
        c.wait()
    first_weight.wait()

    def depth(xs, ys):
        shape = (xs.stop - xs.start, ys.stop - ys.start, LANES)
        rows = jnp.concatenate(
            [e1[xs, h, ys].reshape(shape[0] * shape[1], LANES) for h in range(2)], axis=1)
        got = times(rows, w1)
        for h in range(2):
            e1[xs, h, ys] = got[:, h * LANES : (h + 1) * LANES].reshape(shape)

    inner = slice(2 * PAD, top - PAD)
    depth(slice(0, cx), slice(PAD, 2 * PAD))
    depth(slice(0, cx), slice(top - PAD, top))
    depth(slice(0, 2), inner)
    depth(slice(cx - 2, cx), inner)
    sx1[1] = sums(e1[0, :, own1], e1[1, :, own1])[1]
    sx1[0] = sums(e1[cx - 2, :, own1], e1[cx - 1, :, own1])[0]
    sy1[1] = sums(e1[:, :, PAD : PAD + 1], e1[:, :, PAD + 1 : PAD + 2])[1]
    sy1[0] = sums(e1[:, :, top - 2 : top - 1], e1[:, :, top - 1 : top])[0]
    for x in range(2):
        sc1[x, 1] = sums(sx1[x, :, 0:1], sx1[x, :, 1:2])[1]
        sc1[x, 0] = sums(sx1[x, :, cy - 2 : cy - 1], sx1[x, :, cy - 1 : cy])[0]
    pl.semaphore_wait(barrier, len(peers))
    step = (1, -1)
    post_x = lambda x, h, g: post(
        sx1.at[x, h], hx1.at[x, h, pl.ds(PAD, cy), :], step[x], 0, g)
    post_y = lambda y, h, g: post(sy1.at[y, :, h], hy1.at[y, :, h], 0, step[y], g)
    post_c = lambda x, y, h, g: post(
        sc1.at[x, y, h], hc1.at[x, y, h], step[x], step[y], g)
    noise1 = post_c(0, 0, 1, 0) + post_x(0, 1, 0) + post_y(0, 1, 0)
    coarse1 = post_c(1, 1, 0, 1) + post_x(1, 0, 1) + post_y(1, 0, 1)
    later1 = (post_c(0, 0, 0, 2) + post_c(1, 1, 1, 2) + post_x(0, 0, 2) + post_x(1, 1, 2)
              + post_y(0, 0, 2) + post_y(1, 1, 2))
    for h in range(2):
        later1 += post_c(0, 1, h, 2) + post_c(1, 0, h, 2)

    slab = 4
    for lo in range(2, cx - 2, slab):
        depth(slice(lo, min(lo + slab, cx - 2)), inner)

    def pair1(n, rows=slice(None)):
        return sums(e1[2 * n, :, rows], e1[2 * n + 1, :, rows])

    def lift1(rows):
        def step(n, carry):
            _, part_n = pair1(n, rows)
            before, _ = pair1(n - 1, rows)
            detail = part_n - FAR * before
            xd1[n, :, rows] = detail
            xs1[n, :, rows] = before - detail
            return carry

        lax.fori_loop(1, hx, step, 0)

    def shrunk(n):
        load = lambda start: xs1[n, 0, pl.ds(start, hy, stride=2), :]
        s0, _ = sums(load(PAD), load(PAD + 1))
        _, tp = sums(load(PAD + 2), load(PAD + 3))
        s1s[n, 0, own] = s0 - (tp - FAR * s0)

    def finest(n):
        load = lambda start: xd1[n, 1, pl.ds(start, hy, stride=2), :]
        _, t0 = sums(load(PAD), load(PAD + 1))
        sm, _ = sums(load(PAD - 2), load(PAD - 1))
        return jnp.abs(t0 - FAR * sm)

    def fold(values):
        return jnp.sum(values.reshape(hy // PAD, PAD, LANES), axis=0)

    known = lax.broadcasted_iota(jnp.int32, (hy, LANES), 0) > 0

    def inside(n, magnitude):
        shrunk(n)
        return magnitude + fold(jnp.where(known, finest(n), 0.0))

    lift1(own1)
    magnitude = lax.fori_loop(1, hx, inside, jnp.zeros((PAD, LANES), jnp.float32))
    land(wsem.at[1], sum(2 * math.prod(dst.shape) // (4 * LANES) for _, dst in more))
    done = hy - PAD
    rows = s1s[1:hx, 0, PAD : PAD + done].reshape((hx - 1) * done, LANES)
    e2[0 : hx - 1, PAD : PAD + done] = times(rows, w2).reshape(hx - 1, done, LANES)

    land(recv.at[0], noise1)
    edge = hy1[0, :, 1].reshape(hx, 2, 1, LANES)
    edge_s, edge_t = sums(edge[:, 0], edge[:, 1])
    edge_d = edge_t - FAR * jnp.concatenate([hc1[0, 0, 1][None], edge_s[:-1]], axis=0)
    xd1[0, 1, own1] = sums(e1[0, 1, own1], e1[1, 1, own1])[1] - FAR * hx1[0, 1, own1]
    xd1[0, 1, PAD - 2 : PAD - 1] = edge_d[0]
    xd1[0, 1, PAD - 1 : PAD] = jnp.zeros((1, LANES), jnp.float32)
    _, edge_t = sums(xd1[1:hx, 1, PAD : PAD + 1], xd1[1:hx, 1, PAD + 1 : PAD + 2])
    row = jnp.sum(jnp.abs(edge_t - FAR * edge_d[1:]), axis=0)
    mine[...] = row + jnp.sum(magnitude + fold(finest(0)), axis=0, keepdims=True)
    landed = 0
    for k, d in enumerate(peers):
        landed += post(mine, rows_in.at[k], d[0], d[1], 4)

    land(recv.at[1], coarse1)
    edge, _ = sums(e1[cx - 2, 0, own1], e1[cx - 1, 0, own1])
    xs1[hx, 0, own1] = edge - (hx1[1, 0, own1] - FAR * edge)
    shrunk(hx)
    edge = hy1[1, :, 0].reshape(hx, 2, 1, LANES)
    edge_s, edge_t = sums(edge[:, 0], edge[:, 1])
    after = jnp.concatenate([edge_t[1:], hc1[1, 1, 0][None]], axis=0)
    last_t = edge_s - (after - FAR * edge_s)
    last_s, _ = sums(xs1[1 : hx + 1, 0, top - 2 : top - 1], xs1[1 : hx + 1, 0, top - 1 : top])
    s1s[1 : hx + 1, 0, PAD + hy - 1 : PAD + hy] = last_s - (last_t - FAR * last_s)
    rows = jnp.concatenate(
        [s1s[1:hx, 0, PAD + done : PAD + hy].reshape((hx - 1) * PAD, LANES), s1s[hx, 0, own]],
        axis=0)
    got = times(rows, w2)
    e2[0 : hx - 1, PAD + done : PAD + hy] = got[: (hx - 1) * PAD].reshape(hx - 1, PAD, LANES)
    e2[hx - 1, own] = got[(hx - 1) * PAD :]

    def pair2(m, rows):
        return sums(e2[2 * m, rows], e2[2 * m + 1, rows])

    def coarse2(m, rows):
        return pair2(m, rows)[0] * (1.0 + FAR) - pair2(m + 1, rows)[1]

    xl[0] = pair2(qx - 2, own)[0]
    xl[1] = e2[hx - 2, own]
    xl[2] = e2[hx - 1, own]
    xl[3] = sums(coarse2(qx - 4, own), coarse2(qx - 3, own))[0]
    xh[0] = pair2(0, own)[1]
    xh[1] = sums(coarse2(0, own), coarse2(1, own))[1]
    y_own, y_low, y_high = pl.ds(PAD, hy), pl.ds(0, PAD), pl.ds(PAD + hy, PAD)
    s_own, s_first, s_last = pl.ds(0, hy), pl.ds(0, PAD), pl.ds(hy - PAD, PAD)
    round2 = 0
    for rows_s, rows_d, dy in ((s_last, y_low, 1), (s_first, y_high, -1), (s_own, y_own, 0)):
        round2 += post(xl.at[:, rows_s, :], xlow.at[:, rows_d, :], 1, dy, 3)
        round2 += post(xh.at[:, rows_s, :], xhigh.at[:, rows_d, :], -1, dy, 3)
    round2 += post(e2.at[:, pl.ds(PAD, PAD), :], e2.at[:, y_high, :], 0, -1, 3)
    round2 += post(e2.at[:, pl.ds(hy, PAD), :], e2.at[:, y_low, :], 0, 1, 3)

    land(recv.at[2], later1)

    def place(ref, rows, side):
        if side == 0:
            ref[..., PAD - 2 : PAD - 1, :] = rows
            ref[..., PAD - 1 : PAD, :] = jnp.zeros_like(rows)
        else:
            ref[..., top : top + 1, :] = -ROOT3 * rows
            ref[..., top + 1 : top + 2, :] = rows

    for side in range(2):
        place(e1, hy1[side], side)
        for x in range(2):
            place(hx1.at[x], hc1[x, side], side)
    lift1(slice(PAD - 2, PAD))
    lift1(slice(top, top + 2))
    wide = slice(PAD - 2, top + 2)
    _, edge = pair1(0, wide)
    detail = edge - FAR * hx1[0, :, wide]
    xd1[0, :, wide] = detail
    xs1[0, :, wide] = hx1[0, :, wide] - detail
    edge, _ = pair1(hx - 1, wide)
    detail = hx1[1, :, wide] - FAR * edge
    xd1[hx, :, wide] = detail
    xs1[hx, :, wide] = edge - detail

    def cols1(src, det, smo):
        def step(n, carry):
            for h in range(2):
                load = lambda start: src[n, h, pl.ds(start, hy + 1, stride=2), :]
                s0, t0 = sums(load(PAD), load(PAD + 1))
                sm, _ = sums(load(PAD - 2), load(PAD - 1))
                d = t0 - FAR * sm
                det[n, h, 0 : hy + 1] = d
                smo[n, h, PAD - 1 : PAD + hy] = sm - d
            return carry

        lax.fori_loop(0, hx + 1, step, 0)

    cols1(xd1, d1d, d1s)
    cols1(xs1, s1d, s1s)

    land(recv.at[3], round2)
    every = slice(0, hy + 2 * PAD)
    before = xlow[0]
    xs2[0] = xlow[3]
    for m in range(-1, qx + 1):
        if m == qx:
            smooth, part = None, xhigh[0]
        elif m == -1:
            smooth, part = sums(xlow[1], xlow[2])
        else:
            smooth, part = pair2(m, every)
        detail = part - FAR * before
        xd2[m + 1] = detail
        xs2[m + 2] = before - detail
        before = smooth
    xs2[qx + 3] = xhigh[1]
    pairs = hy // 2 + PAD

    def rows2(src):
        return forward_rows(src[:, pl.ds(0, pairs, stride=2), :],
                            src[:, pl.ds(1, pairs, stride=2), :])

    mid = slice(PAD // 2, PAD // 2 + pairs)
    dd[:, mid], ds[:, mid] = rows2(xd2)
    det, smo = rows2(xs2)
    sd[:, mid] = det[1 : qx + 3]
    ep3[:, mid] = smo

    n_own, n3, h3 = qx // 2, qx // 2 + 2, qy // 2 + PAD
    low_s, low_t = [ep3[0]], [None]
    for n in range(n_own + 1):
        s, t = sums(ep3[1 + 2 * n], ep3[2 + 2 * n])
        low_s.append(s)
        low_t.append(t)
    low_t.append(ep3[qx + 3])
    for n in range(n3):
        detail = low_t[n + 1] - FAR * low_s[n]
        t3d[n] = detail
        t3s[n] = low_s[n] - detail
    bands = []
    for src in (t3d, t3s):
        bands += forward_rows(src[:, pl.ds(0, h3, stride=2), :], src[:, pl.ds(1, h3, stride=2), :])
    for i, band in enumerate(bands):
        b3[i] = times(band.reshape(n3 * h3, LANES), w3).reshape(n3, h3, LANES)

    land(recv.at[4], landed)
    acc = mine[...]
    for k in range(len(peers)):
        acc = acc + rows_in[k]
    noise[...] = acc
    land(send.at[0], sent[0])


def finish(shape, count_all, d1d, d1s, s1d, s1s, dd, ds, sd, ep3, b3, total, v1, v2, v3, out,
           ss, r2, r1, s0, p1d, p1s, o1, ob, osem):
    cx, cy, cz = shape
    hx, hy, qx, qy = cx // 2, cy // 2, cx // 4, cy // 4
    n3, h3, x2, yrows = qx // 2 + 2, qy // 2 + PAD, qx + 2, qy + 2 * PAD
    noise = jnp.sum(total[...], axis=(0, 1), keepdims=True) * (
        HIGH * HIGH * math.sqrt(math.pi / 2.0) / count_all)

    far1, mid1, near1 = limits(noise, 1)

    def inv1(det, smo, h, dst, limit_d, limit_s):
        def one_x(n):
            d = shrink(det[n, h], limit_d)
            s = s0[n] if limit_s is None else shrink(smo[n, h], limit_s)
            return d, s + d

        def step(n, carry):
            d, before = carry
            after, one = one_x(n + 1)
            even, odd = undo(d, one, before)
            dst[2 * n, h] = even
            dst[2 * n + 1, h] = odd
            return after, one

        lax.fori_loop(0, hx, step, one_x(0), unroll=4)

    for h in range(2):
        inv1(d1d, s1d, h, p1d, far1, mid1)
    inv1(d1s, s1s, 1, p1s, mid1, near1)

    far3, mid3, near3 = (v.reshape(1, 1, 1) for v in limits(noise, 3))
    lane3 = lax.broadcasted_iota(jnp.int32, (n3, h3, LANES), 2)
    b_dd, b_ds, b_sd = shrink(b3[0], far3), shrink(b3[1], mid3), shrink(b3[2], mid3)
    b_ss = jnp.where(lane3 < cz // 8, b3[3], shrink(b3[3], near3))

    def inverse_x(det, smo):
        one = smo + det
        even, odd = undo(det[:-1], one[1:], one[:-1])
        return weave(even, odd)

    y_d = inverse_x(b_dd, b_sd)
    y_s = inverse_x(b_ds, b_ss)
    one = y_s + pltpu.roll(y_d, h3 - 1, 1)
    even, odd = undo(y_d, one, pltpu.roll(one, 1, 1))
    r2[:, pl.ds(0, h3, stride=2), :] = even
    r2[:, pl.ds(1, h3, stride=2), :] = odd
    back = times(r2[...].reshape(x2 * yrows, LANES), v3).reshape(x2, yrows, LANES)

    far2, mid2, near2 = limits(noise, 2)
    lane2 = lax.broadcasted_iota(jnp.int32, (x2, yrows, LANES), 2)
    ss[...] = jnp.where(lane2 < cz // 4, back, shrink(ep3[1 : qx + 3], near2.reshape(1, 1, 1)))

    def one_x(n):
        d_d = shrink(dd[n], far2)
        d_s = shrink(ds[n], mid2)
        s_d = shrink(sd[n], mid2)
        return d_d, d_s, s_d + d_d, ss[n] + d_s

    def inv2(n, carry):
        d_d, d_s, b_d, b_s = carry
        after = one_x(n + 1)
        pair_d = undo(d_d, after[2], b_d)
        pair_s = undo(d_s, after[3], b_s)
        for i in range(2):
            y_d, y_s = pair_d[i], pair_s[i]
            one = y_s + pltpu.roll(y_d, yrows - 1, 0)
            even, odd = undo(y_d, one, pltpu.roll(one, 1, 0))
            r1[2 * n + i, pl.ds(0, yrows, stride=2), :] = even
            r1[2 * n + i, pl.ds(1, yrows, stride=2), :] = odd
        return after

    lax.fori_loop(0, qx + 1, inv2, one_x(0), unroll=3)
    x1, y1 = hx + 2, hy + PAD
    back = times(r1[:, PAD : PAD + y1].reshape(x1 * y1, LANES), v2).reshape(x1, y1, LANES)
    s0[...] = back[1:]
    inv1(d1s, s1s, 0, p1s, mid1, None)

    def inv1_y(n):
        for h in range(2):
            y_d = p1d[n, h, 0:hy]
            y_n = p1d[n, h, 1 : hy + 1]
            s = p1s[n, h, PAD : PAD + hy]
            s_b = p1s[n, h, PAD - 1 : PAD - 1 + hy]
            even, odd = undo(y_d, s + y_n, s_b + y_d)
            o1[n, h, pl.ds(0, hy, stride=2), :] = even
            o1[n, h, pl.ds(1, hy, stride=2), :] = odd

    layers = 8
    outs = []
    for n in range(layers):
        inv1_y(n)
    for i in range(cx // layers):
        for n in range((i + 1) * layers, min((i + 2) * layers, cx)):
            inv1_y(n)
        xs = slice(i * layers, (i + 1) * layers)
        rows = jnp.concatenate(
            [o1[xs, h].reshape(layers * cy, LANES) for h in range(2)], axis=1)
        ob[xs] = times(rows, v1).reshape(layers, cy, cz)
        c = pltpu.make_async_copy(ob.at[xs], out.at[xs], osem.at[i])
        c.start()
        outs.append(c)
    for c in outs:
        c.wait()


def on_device(nx, ny, volume):
    cx, cy, cz = volume.shape
    hx, hy, qx, qy = cx // 2, cy // 2, cx // 4, cy // 4
    n3, h3 = qx // 2 + 2, qy // 2 + PAD
    f32 = jnp.float32
    count = cx * nx * cy * ny * cz // 8
    weights = [
        halves(forward_matrix(cz), cz), halves(forward_matrix(cz // 2), LANES),
        halves(forward_matrix(cz // 4), LANES), halves(inverse_matrix(cz), cz),
        halves(inverse_matrix(cz // 2), LANES), halves(inverse_matrix(cz // 4), LANES),
    ]
    vmem = lambda *s: pltpu.VMEM(s, f32)
    ey, ey2, ey3 = cy + 2 * PAD, hy + 2 * PAD, qy + 2 * PAD
    wide = lambda *s: pltpu.VMEM((2,) + s, jnp.bfloat16)
    made = (
        *[vmem(hx + 1, 2, hy + PAD, LANES) for _ in range(4)],
        *[vmem(qx + 2, ey3, LANES) for _ in range(3)],
        vmem(qx + 4, ey3, LANES), vmem(4, n3, h3, LANES), vmem(1, LANES),
        wide(cz, cz), wide(LANES, LANES), wide(LANES, LANES),
    )
    rows = 4 * cy + 4 * cx + 8 + 6 * (hy + 2 * PAD) + 2 * hx * PAD + nx * ny
    scratch = [
        wide(cz, cz), wide(LANES, LANES), wide(LANES, LANES),
        vmem(cx, 2, ey, LANES), vmem(2, 2, ey, LANES), vmem(2, 2, cy, LANES),
        vmem(2, cx, 2, 1, LANES), vmem(2, cx, 2, 1, LANES),
        vmem(2, 2, 2, 1, LANES), vmem(2, 2, 2, 1, LANES),
        vmem(hx + 1, 2, ey, LANES), vmem(hx + 1, 2, ey, LANES),
        vmem(hx, ey2, LANES), vmem(4, hy, LANES), vmem(2, hy, LANES),
        vmem(4, ey2, LANES), vmem(2, ey2, LANES),
        vmem(qx + 2, ey2, LANES), vmem(qx + 4, ey2, LANES),
        vmem(n3, ey3, LANES), vmem(n3, ey3, LANES),
        vmem(1, LANES), vmem(nx * ny - 1, 1, LANES), vmem(max(rows, cz * cz // 32), 1, LANES),
        pltpu.SemaphoreType.DMA((1,)), pltpu.SemaphoreType.DMA((5,)),
        pltpu.SemaphoreType.DMA((2,)), pltpu.SemaphoreType.DMA((2,)),
    ]
    near = pl.BlockSpec(memory_space=pltpu.VMEM)
    passed = pl.pallas_call(
        functools.partial(kernel, (cx, cy, cz), nx, ny),
        out_shape=made,
        in_specs=[pl.BlockSpec(memory_space=pltpu.HBM)] * 7,
        out_specs=(near,) * len(made),
        scratch_shapes=scratch,
        compiler_params=pltpu.CompilerParams(
            collective_id=0, has_side_effects=True, vmem_limit_bytes=56 * 1024 * 1024),
    )(volume, *[jnp.asarray(w) for w in weights])
    return pl.pallas_call(
        functools.partial(finish, (cx, cy, cz), count),
        out_shape=jax.ShapeDtypeStruct(volume.shape, f32),
        in_specs=[near] * len(made),
        out_specs=pl.BlockSpec(memory_space=pltpu.HBM),
        scratch_shapes=[
            vmem(qx + 2, ey3, LANES), vmem(qx + 2, ey3, LANES), vmem(hx + 2, 2 * ey3, LANES),
            vmem(hx + 1, hy + PAD, LANES),
            vmem(cx, 2, hy + PAD, LANES), vmem(cx, 2, hy + PAD, LANES),
            vmem(cx, 2, cy, LANES), vmem(cx, cy, cz), pltpu.SemaphoreType.DMA((cx // 8,)),
        ],
        compiler_params=pltpu.CompilerParams(vmem_limit_bytes=24 * 1024 * 1024),
    )(*passed)


def solution(mesh):
    spec = P("gx", "gy", None)
    body = functools.partial(on_device, mesh.shape["gx"], mesh.shape["gy"])
    return jax.shard_map(body, mesh=mesh, in_specs=(spec,), out_specs=spec, check_vma=False)
```

```python
import functools
import math

import jax
import jax.numpy as jnp
import numpy as np
from jax import lax
from jax.experimental import pallas as pl
from jax.experimental.pallas import tpu as pltpu
from jax.sharding import PartitionSpec as P

ROOT3 = math.sqrt(3.0)
NEAR = math.sqrt(3.0) / 4.0
FAR = (math.sqrt(3.0) - 2.0) / 4.0
LOW = (math.sqrt(3.0) - 1.0) / math.sqrt(2.0)
HIGH = (math.sqrt(3.0) + 1.0) / math.sqrt(2.0)
LANES = 128
PAD = 8


def forward_matrix(size):
    lines = np.eye(size)
    even, odd = lines[:, 0::2], lines[:, 1::2]
    smooth = even + ROOT3 * odd
    detail = odd - NEAR * smooth - FAR * np.roll(smooth, 1, 1)
    smooth = smooth - np.roll(detail, -1, 1)
    return np.concatenate([LOW * smooth, HIGH * detail], 1)


def inverse_matrix(size):
    lines = np.eye(size)
    smooth, detail = lines[:, : size // 2] / LOW, lines[:, size // 2 :] / HIGH
    first = smooth + np.roll(detail, -1, 1)
    odd = detail + NEAR * first + FAR * np.roll(first, 1, 1)
    even = first - ROOT3 * odd
    return np.stack([even, odd], 2).reshape(size, size)


def halves(matrix, size):
    full = np.zeros((size, size))
    full[: matrix.shape[0], : matrix.shape[1]] = matrix
    high = full.astype(jnp.bfloat16)
    low = (full - high.astype(np.float64)).astype(jnp.bfloat16)
    return np.stack([high, low])


def times(values, w_ref):
    high = values.astype(jnp.bfloat16)
    low = (values - high.astype(jnp.float32)).astype(jnp.bfloat16)
    dot = functools.partial(jnp.dot, preferred_element_type=jnp.float32)
    return dot(high, w_ref[0]) + (dot(low, w_ref[0]) + dot(high, w_ref[1]))


def folded(matrix):
    high, low = halves(matrix, LANES)
    return np.block([[high, low], [high, np.zeros_like(low)]])


def times_folded(values, w_ref):
    high = values.astype(jnp.bfloat16)
    low = (values - high.astype(jnp.float32)).astype(jnp.bfloat16)
    both = jnp.dot(jnp.concatenate([high, low], axis=1), w_ref[...],
                   preferred_element_type=jnp.float32)
    return both[:, :LANES] + both[:, LANES:]


def shrink(values, noise):
    return values - jnp.clip(values, -noise, noise)


def sums(even, odd):
    smooth = even + ROOT3 * odd
    return smooth, odd - NEAR * smooth


def undo(detail, first, before):
    odd = detail + NEAR * first + FAR * before
    return first - ROOT3 * odd, odd


def weave(even, odd):
    both = jnp.stack([even, odd], axis=1)
    return both.reshape((2 * even.shape[0],) + even.shape[1:])


def forward_rows(even, odd):
    axis = even.ndim - 2
    smooth, part = sums(even, odd)
    detail = part - FAR * pltpu.roll(smooth, 1, axis)
    return detail, smooth - pltpu.roll(detail, even.shape[axis] - 1, axis)


def limits(noise, level):
    base = noise * (1.0 / LOW ** (2 * (level - 1)))
    return base * (1.0 / (HIGH * HIGH)), base * (1.0 / (HIGH * LOW)), base * (1.0 / (LOW * LOW))


def spread(total, count_all):
    return jnp.sum(total, axis=(0, 1), keepdims=True) * (
        HIGH * HIGH * math.sqrt(math.pi / 2.0) / count_all)


def inverse1(hx, one_x, put):
    def step(n, carry):
        d, before = carry
        after, one = one_x(n + 1)
        even, odd = undo(d, one, before)
        put(2 * n, even)
        put(2 * n + 1, odd)
        return after, one

    lax.fori_loop(0, hx, step, one_x(0), unroll=4)


def kernel(shape, count_all, nx, ny, vol, g1, g2, g3, g4, g5, g6,
           d1s, p1d, p1s1, dd, ds, sd, ep3, b3, noise, v1, v2, v3,
           w1, w2, w3, d1d, s1d, s1s,
           e1, hx1, sx1, hy1, sy1, hc1, sc1, xd1, xs1,
           e2, xl, xh, xlow, xhigh, xd2, xs2, t3d, t3s,
           mine, rows_in, dummy, send, recv, lsem, wsem):
    cx, cy, cz = shape
    hx, hy, qx, qy = cx // 2, cy // 2, cx // 4, cy // 4
    ix, iy = lax.axis_index("gx"), lax.axis_index("gy")

    def device(dx, dy):
        return (lax.rem(ix + dx + nx, nx), lax.rem(iy + dy + ny, ny))

    near = [(dx, dy) for dx in (-1, 0, 1) for dy in (-1, 0, 1) if dx or dy]
    peers = [(dx, dy) for dx in range(nx) for dy in range(ny) if dx or dy]
    taken = {(dx % nx, dy % ny) for dx, dy in near}
    barrier = pltpu.get_barrier_semaphore()

    def greet(dx, dy):
        pl.semaphore_signal(barrier, inc=1, device_id=device(dx, dy),
                            device_id_type=pl.DeviceIdType.MESH)

    for d in sorted(taken):
        greet(*d)
    loads = [
        pltpu.make_async_copy(
            vol.at[:, :, pl.ds(h * LANES, LANES)],
            e1.at[:, h, pl.ds(PAD, cy), :], lsem.at[h])
        for h in range(2)
    ]
    for c in loads:
        c.start()
    for d in peers:
        if d not in taken:
            greet(*d)
    first_weight = pltpu.make_async_copy(g1, w1, wsem.at[0])
    first_weight.start()
    more = list(zip((g2, g3, g4, g5, g6), (w2, w3, v1, v2, v3)))
    for src, dst in more:
        pltpu.make_async_copy(src, dst, wsem.at[1]).start()

    sent = [0]

    def post(src, dst, dx, dy, group):
        sent[0] += math.prod(src.shape) // LANES
        pltpu.make_async_remote_copy(
            src_ref=src, dst_ref=dst, send_sem=send.at[0], recv_sem=recv.at[group],
            device_id=device(dx, dy), device_id_type=pl.DeviceIdType.MESH).start()
        return math.prod(src.shape) // LANES

    def land(sem, rows):
        part = dummy.at[pl.ds(0, rows)]
        pltpu.make_async_copy(part, part, sem).wait()

    ep3[:, 0 : PAD // 2] = jnp.zeros((qx + 4, PAD // 2, LANES), jnp.float32)
    ep3[:, PAD // 2 + hy // 2 + PAD :] = jnp.zeros((qx + 4, PAD // 2, LANES), jnp.float32)
    for ref in (dd, ds, sd):
        ref[:, 0 : PAD // 2] = jnp.zeros((qx + 2, PAD // 2, LANES), jnp.float32)
        ref[:, PAD // 2 + hy // 2 + PAD :] = jnp.zeros((qx + 2, PAD // 2, LANES), jnp.float32)

    top = PAD + cy
    own1, own = slice(PAD, top), slice(PAD, PAD + hy)
    for c in loads:
        c.wait()
    first_weight.wait()

    def depth(xs, ys):
        shape = (xs.stop - xs.start, ys.stop - ys.start, LANES)
        rows = jnp.concatenate(
            [e1[xs, h, ys].reshape(shape[0] * shape[1], LANES) for h in range(2)], axis=1)
        got = times(rows, w1)
        for h in range(2):
            e1[xs, h, ys] = got[:, h * LANES : (h + 1) * LANES].reshape(shape)

    inner = slice(2 * PAD, top - PAD)
    depth(slice(0, cx), slice(PAD, 2 * PAD))
    depth(slice(0, cx), slice(top - PAD, top))
    depth(slice(0, 2), inner)
    depth(slice(cx - 2, cx), inner)
    sx1[1] = sums(e1[0, :, own1], e1[1, :, own1])[1]
    sx1[0] = sums(e1[cx - 2, :, own1], e1[cx - 1, :, own1])[0]
    sy1[1] = sums(e1[:, :, PAD : PAD + 1], e1[:, :, PAD + 1 : PAD + 2])[1]
    sy1[0] = sums(e1[:, :, top - 2 : top - 1], e1[:, :, top - 1 : top])[0]
    for x in range(2):
        sc1[x, 1] = sums(sx1[x, :, 0:1], sx1[x, :, 1:2])[1]
        sc1[x, 0] = sums(sx1[x, :, cy - 2 : cy - 1], sx1[x, :, cy - 1 : cy])[0]
    pl.semaphore_wait(barrier, len(peers))
    step = (1, -1)
    post_x = lambda x, h, g: post(
        sx1.at[x, h], hx1.at[x, h, pl.ds(PAD, cy), :], step[x], 0, g)
    post_y = lambda y, h, g: post(sy1.at[y, :, h], hy1.at[y, :, h], 0, step[y], g)
    post_c = lambda x, y, h, g: post(
        sc1.at[x, y, h], hc1.at[x, y, h], step[x], step[y], g)
    noise1 = post_c(0, 0, 1, 0) + post_x(0, 1, 0) + post_y(0, 1, 0)
    coarse1 = post_c(1, 1, 0, 1) + post_x(1, 0, 1) + post_y(1, 0, 1)
    later1 = (post_c(0, 0, 0, 2) + post_c(1, 1, 1, 2) + post_x(0, 0, 2) + post_x(1, 1, 2)
              + post_y(0, 0, 2) + post_y(1, 1, 2))
    for h in range(2):
        later1 += post_c(0, 1, h, 2) + post_c(1, 0, h, 2)

    slab = 4
    for lo in range(2, cx - 2, slab):
        depth(slice(lo, min(lo + slab, cx - 2)), inner)

    def pair1(n, rows=slice(None)):
        return sums(e1[2 * n, :, rows], e1[2 * n + 1, :, rows])

    def lift1(rows):
        def step(n, carry):
            _, part_n = pair1(n, rows)
            before, _ = pair1(n - 1, rows)
            detail = part_n - FAR * before
            xd1[n, :, rows] = detail
            xs1[n, :, rows] = before - detail
            return carry

        lax.fori_loop(1, hx, step, 0)

    def shrunk(n):
        load = lambda start: xs1[n, 0, pl.ds(start, hy, stride=2), :]
        s0, _ = sums(load(PAD), load(PAD + 1))
        _, tp = sums(load(PAD + 2), load(PAD + 3))
        s1s[n, 0, own] = s0 - (tp - FAR * s0)

    def finest(n):
        load = lambda start: xd1[n, 1, pl.ds(start, hy, stride=2), :]
        _, t0 = sums(load(PAD), load(PAD + 1))
        sm, _ = sums(load(PAD - 2), load(PAD - 1))
        return jnp.abs(t0 - FAR * sm)

    def fold(values):
        return jnp.sum(values.reshape(hy // PAD, PAD, LANES), axis=0)

    known = lax.broadcasted_iota(jnp.int32, (hy, LANES), 0) > 0

    def inside(n, magnitude):
        shrunk(n)
        return magnitude + fold(jnp.where(known, finest(n), 0.0))

    lift1(own1)
    magnitude = lax.fori_loop(1, hx, inside, jnp.zeros((PAD, LANES), jnp.float32))
    land(wsem.at[1], sum(2 * math.prod(dst.shape) // (4 * LANES) for _, dst in more))
    done = hy - PAD
    rows = s1s[1:hx, 0, PAD : PAD + done].reshape((hx - 1) * done, LANES)
    e2[0 : hx - 1, PAD : PAD + done] = times_folded(rows, w2).reshape(hx - 1, done, LANES)

    land(recv.at[0], noise1)
    edge = hy1[0, :, 1].reshape(hx, 2, 1, LANES)
    edge_s, edge_t = sums(edge[:, 0], edge[:, 1])
    edge_d = edge_t - FAR * jnp.concatenate([hc1[0, 0, 1][None], edge_s[:-1]], axis=0)
    xd1[0, 1, own1] = sums(e1[0, 1, own1], e1[1, 1, own1])[1] - FAR * hx1[0, 1, own1]
    xd1[0, 1, PAD - 2 : PAD - 1] = edge_d[0]
    xd1[0, 1, PAD - 1 : PAD] = jnp.zeros((1, LANES), jnp.float32)
    _, edge_t = sums(xd1[1:hx, 1, PAD : PAD + 1], xd1[1:hx, 1, PAD + 1 : PAD + 2])
    row = jnp.sum(jnp.abs(edge_t - FAR * edge_d[1:]), axis=0)
    mine[...] = row + jnp.sum(magnitude + fold(finest(0)), axis=0, keepdims=True)
    landed = 0
    for k, d in enumerate(peers):
        landed += post(mine, rows_in.at[k], d[0], d[1], 4)

    land(recv.at[1], coarse1)
    edge, _ = sums(e1[cx - 2, 0, own1], e1[cx - 1, 0, own1])
    xs1[hx, 0, own1] = edge - (hx1[1, 0, own1] - FAR * edge)
    shrunk(hx)
    edge = hy1[1, :, 0].reshape(hx, 2, 1, LANES)
    edge_s, edge_t = sums(edge[:, 0], edge[:, 1])
    after = jnp.concatenate([edge_t[1:], hc1[1, 1, 0][None]], axis=0)
    last_t = edge_s - (after - FAR * edge_s)
    last_s, _ = sums(xs1[1 : hx + 1, 0, top - 2 : top - 1], xs1[1 : hx + 1, 0, top - 1 : top])
    s1s[1 : hx + 1, 0, PAD + hy - 1 : PAD + hy] = last_s - (last_t - FAR * last_s)
    rows = jnp.concatenate(
        [s1s[1:hx, 0, PAD + done : PAD + hy].reshape((hx - 1) * PAD, LANES), s1s[hx, 0, own]],
        axis=0)
    got = times_folded(rows, w2)
    e2[0 : hx - 1, PAD + done : PAD + hy] = got[: (hx - 1) * PAD].reshape(hx - 1, PAD, LANES)
    e2[hx - 1, own] = got[(hx - 1) * PAD :]

    def pair2(m, rows):
        return sums(e2[2 * m, rows], e2[2 * m + 1, rows])

    def coarse2(m, rows):
        return pair2(m, rows)[0] * (1.0 + FAR) - pair2(m + 1, rows)[1]

    xl[0] = pair2(qx - 2, own)[0]
    xl[1] = e2[hx - 2, own]
    xl[2] = e2[hx - 1, own]
    xl[3] = sums(coarse2(qx - 4, own), coarse2(qx - 3, own))[0]
    xh[0] = pair2(0, own)[1]
    xh[1] = sums(coarse2(0, own), coarse2(1, own))[1]
    y_own, y_low, y_high = pl.ds(PAD, hy), pl.ds(0, PAD), pl.ds(PAD + hy, PAD)
    s_own, s_first, s_last = pl.ds(0, hy), pl.ds(0, PAD), pl.ds(hy - PAD, PAD)
    round2 = 0
    for rows_s, rows_d, dy in ((s_last, y_low, 1), (s_first, y_high, -1), (s_own, y_own, 0)):
        round2 += post(xl.at[:, rows_s, :], xlow.at[:, rows_d, :], 1, dy, 3)
        round2 += post(xh.at[:, rows_s, :], xhigh.at[:, rows_d, :], -1, dy, 3)
    round2 += post(e2.at[:, pl.ds(PAD, PAD), :], e2.at[:, y_high, :], 0, -1, 3)
    round2 += post(e2.at[:, pl.ds(hy, PAD), :], e2.at[:, y_low, :], 0, 1, 3)

    land(recv.at[2], later1)

    def place(ref, rows, side):
        if side == 0:
            ref[..., PAD - 2 : PAD - 1, :] = rows
            ref[..., PAD - 1 : PAD, :] = jnp.zeros_like(rows)
        else:
            ref[..., top : top + 1, :] = -ROOT3 * rows
            ref[..., top + 1 : top + 2, :] = rows

    for side in range(2):
        place(e1, hy1[side], side)
        for x in range(2):
            place(hx1.at[x], hc1[x, side], side)
    lift1(slice(PAD - 2, PAD))
    lift1(slice(top, top + 2))
    wide = slice(PAD - 2, top + 2)
    _, edge = pair1(0, wide)
    detail = edge - FAR * hx1[0, :, wide]
    xd1[0, :, wide] = detail
    xs1[0, :, wide] = hx1[0, :, wide] - detail
    edge, _ = pair1(hx - 1, wide)
    detail = hx1[1, :, wide] - FAR * edge
    xd1[hx, :, wide] = detail
    xs1[hx, :, wide] = edge - detail

    def cols1(src, det, smo):
        def step(n, carry):
            for h in range(2):
                load = lambda start: src[n, h, pl.ds(start, hy + 1, stride=2), :]
                s0, t0 = sums(load(PAD), load(PAD + 1))
                sm, _ = sums(load(PAD - 2), load(PAD - 1))
                d = t0 - FAR * sm
                det[n, h, 0 : hy + 1] = d
                smo[n, h, PAD - 1 : PAD + hy] = sm - d
            return carry

        lax.fori_loop(0, hx + 1, step, 0)

    cols1(xd1, d1d, d1s)
    cols1(xs1, s1d, s1s)

    land(recv.at[4], landed)
    acc = mine[...]
    for k in range(len(peers)):
        acc = acc + rows_in[k]
    noise[...] = acc
    far1, mid1, near1 = limits(spread(acc, count_all), 1)

    def put_into(dst, h):
        def put(n, rows):
            if h is None:
                dst[n] = rows
            else:
                dst[n, h] = rows
        return put

    def bands1(det, smo, h, limit_d, limit_s):
        def one_x(n):
            d = shrink(det[n, h], limit_d)
            return d, shrink(smo[n, h], limit_s) + d
        return one_x

    for h in range(2):
        inverse1(hx, bands1(d1d, s1d, h, far1, mid1), put_into(p1d, h))
    inverse1(hx, bands1(d1s, s1s, 1, mid1, near1), put_into(p1s1, None))

    land(recv.at[3], round2)
    every = slice(0, hy + 2 * PAD)
    before = xlow[0]
    xs2[0] = xlow[3]
    for m in range(-1, qx + 1):
        if m == qx:
            smooth, part = None, xhigh[0]
        elif m == -1:
            smooth, part = sums(xlow[1], xlow[2])
        else:
            smooth, part = pair2(m, every)
        detail = part - FAR * before
        xd2[m + 1] = detail
        xs2[m + 2] = before - detail
        before = smooth
    xs2[qx + 3] = xhigh[1]
    pairs = hy // 2 + PAD

    def rows2(src):
        return forward_rows(src[:, pl.ds(0, pairs, stride=2), :],
                            src[:, pl.ds(1, pairs, stride=2), :])

    mid = slice(PAD // 2, PAD // 2 + pairs)
    dd[:, mid], ds[:, mid] = rows2(xd2)
    det, smo = rows2(xs2)
    sd[:, mid] = det[1 : qx + 3]
    ep3[:, mid] = smo

    n_own, n3, h3 = qx // 2, qx // 2 + 2, qy // 2 + PAD
    low_s, low_t = [ep3[0]], [None]
    for n in range(n_own + 1):
        s, t = sums(ep3[1 + 2 * n], ep3[2 + 2 * n])
        low_s.append(s)
        low_t.append(t)
    low_t.append(ep3[qx + 3])
    for n in range(n3):
        detail = low_t[n + 1] - FAR * low_s[n]
        t3d[n] = detail
        t3s[n] = low_s[n] - detail
    bands = []
    for src in (t3d, t3s):
        bands += forward_rows(src[:, pl.ds(0, h3, stride=2), :], src[:, pl.ds(1, h3, stride=2), :])
    for i, band in enumerate(bands):
        b3[i] = times_folded(band.reshape(n3 * h3, LANES), w3).reshape(n3, h3, LANES)

    land(send.at[0], sent[0])


def finish(shape, count_all, d1s, p1d, p1s1, dd, ds, sd, ep3, b3, total, v1, v2, v3, out,
           ss, r2, r1, s0, p1s0, o1, ob, osem):
    cx, cy, cz = shape
    hx, hy, qx, qy = cx // 2, cy // 2, cx // 4, cy // 4
    n3, h3, x2, yrows = qx // 2 + 2, qy // 2 + PAD, qx + 2, qy + 2 * PAD
    noise = spread(total[...], count_all)


    far3, mid3, near3 = (v.reshape(1, 1, 1) for v in limits(noise, 3))
    lane3 = lax.broadcasted_iota(jnp.int32, (n3, h3, LANES), 2)
    b_dd, b_ds, b_sd = shrink(b3[0], far3), shrink(b3[1], mid3), shrink(b3[2], mid3)
    b_ss = jnp.where(lane3 < cz // 8, b3[3], shrink(b3[3], near3))

    def inverse_x(det, smo):
        one = smo + det
        even, odd = undo(det[:-1], one[1:], one[:-1])
        return weave(even, odd)

    y_d = inverse_x(b_dd, b_sd)
    y_s = inverse_x(b_ds, b_ss)
    one = y_s + pltpu.roll(y_d, h3 - 1, 1)
    even, odd = undo(y_d, one, pltpu.roll(one, 1, 1))
    r2[:, pl.ds(0, h3, stride=2), :] = even
    r2[:, pl.ds(1, h3, stride=2), :] = odd
    back = times_folded(r2[...].reshape(x2 * yrows, LANES), v3).reshape(x2, yrows, LANES)

    far2, mid2, near2 = limits(noise, 2)
    lane2 = lax.broadcasted_iota(jnp.int32, (x2, yrows, LANES), 2)
    ss[...] = jnp.where(lane2 < cz // 4, back, shrink(ep3[1 : qx + 3], near2.reshape(1, 1, 1)))

    def one_x(n):
        d_d = shrink(dd[n], far2)
        d_s = shrink(ds[n], mid2)
        s_d = shrink(sd[n], mid2)
        return d_d, d_s, s_d + d_d, ss[n] + d_s

    def inv2(n, carry):
        d_d, d_s, b_d, b_s = carry
        after = one_x(n + 1)
        pair_d = undo(d_d, after[2], b_d)
        pair_s = undo(d_s, after[3], b_s)
        for i in range(2):
            y_d, y_s = pair_d[i], pair_s[i]
            one = y_s + pltpu.roll(y_d, yrows - 1, 0)
            even, odd = undo(y_d, one, pltpu.roll(one, 1, 0))
            r1[2 * n + i, pl.ds(0, yrows, stride=2), :] = even
            r1[2 * n + i, pl.ds(1, yrows, stride=2), :] = odd
        return after

    lax.fori_loop(0, qx + 1, inv2, one_x(0), unroll=3)
    x1, y1 = hx + 2, hy + PAD
    back = times_folded(r1[:, PAD : PAD + y1].reshape(x1 * y1, LANES), v2).reshape(x1, y1, LANES)
    s0[...] = back[1:]
    _, mid1, _ = limits(noise, 1)

    def low_x(n):
        d = shrink(d1s[n, 0], mid1)
        return d, s0[n] + d

    def put_low(n, rows):
        p1s0[n] = rows

    inverse1(hx, low_x, put_low)

    def inv1_y(n):
        for h in range(2):
            y_d = p1d[n, h, 0:hy]
            y_n = p1d[n, h, 1 : hy + 1]
            p1s = p1s1 if h else p1s0
            s = p1s[n, PAD : PAD + hy]
            s_b = p1s[n, PAD - 1 : PAD - 1 + hy]
            even, odd = undo(y_d, s + y_n, s_b + y_d)
            o1[n, h, pl.ds(0, hy, stride=2), :] = even
            o1[n, h, pl.ds(1, hy, stride=2), :] = odd

    layers = 8
    outs = []
    for n in range(layers):
        inv1_y(n)
    for i in range(cx // layers):
        for n in range((i + 1) * layers, min((i + 2) * layers, cx)):
            inv1_y(n)
        xs = slice(i * layers, (i + 1) * layers)
        rows = jnp.concatenate(
            [o1[xs, h].reshape(layers * cy, LANES) for h in range(2)], axis=1)
        ob[xs] = times(rows, v1).reshape(layers, cy, cz)
        c = pltpu.make_async_copy(ob.at[xs], out.at[xs], osem.at[i])
        c.start()
        outs.append(c)
    for c in outs:
        c.wait()


def on_device(nx, ny, volume):
    cx, cy, cz = volume.shape
    hx, hy, qx, qy = cx // 2, cy // 2, cx // 4, cy // 4
    n3, h3 = qx // 2 + 2, qy // 2 + PAD
    f32 = jnp.float32
    count = cx * nx * cy * ny * cz // 8
    weights = [
        halves(forward_matrix(cz), cz), folded(forward_matrix(cz // 2)),
        folded(forward_matrix(cz // 4)), halves(inverse_matrix(cz), cz),
        folded(inverse_matrix(cz // 2)), folded(inverse_matrix(cz // 4)),
    ]
    vmem = lambda *s: pltpu.VMEM(s, f32)
    ey, ey2, ey3 = cy + 2 * PAD, hy + 2 * PAD, qy + 2 * PAD
    wide = lambda *s: pltpu.VMEM(s, jnp.bfloat16)
    pair = (2 * LANES, 2 * LANES)
    made = (
        vmem(hx + 1, 2, hy + PAD, LANES), vmem(cx, 2, hy + PAD, LANES),
        vmem(cx, hy + PAD, LANES), *[vmem(qx + 2, ey3, LANES) for _ in range(3)],
        vmem(qx + 4, ey3, LANES), vmem(4, n3, h3, LANES), vmem(1, LANES),
        wide(2, cz, cz), wide(*pair), wide(*pair),
    )
    rows = 4 * cy + 4 * cx + 8 + 6 * (hy + 2 * PAD) + 2 * hx * PAD + nx * ny
    scratch = [
        wide(2, cz, cz), wide(*pair), wide(*pair),
        *[vmem(hx + 1, 2, hy + PAD, LANES) for _ in range(3)],
        vmem(cx, 2, ey, LANES), vmem(2, 2, ey, LANES), vmem(2, 2, cy, LANES),
        vmem(2, cx, 2, 1, LANES), vmem(2, cx, 2, 1, LANES),
        vmem(2, 2, 2, 1, LANES), vmem(2, 2, 2, 1, LANES),
        vmem(hx + 1, 2, ey, LANES), vmem(hx + 1, 2, ey, LANES),
        vmem(hx, ey2, LANES), vmem(4, hy, LANES), vmem(2, hy, LANES),
        vmem(4, ey2, LANES), vmem(2, ey2, LANES),
        vmem(qx + 2, ey2, LANES), vmem(qx + 4, ey2, LANES),
        vmem(n3, ey3, LANES), vmem(n3, ey3, LANES),
        vmem(1, LANES), vmem(nx * ny - 1, 1, LANES), vmem(max(rows, cz * cz // 32), 1, LANES),
        pltpu.SemaphoreType.DMA((1,)), pltpu.SemaphoreType.DMA((5,)),
        pltpu.SemaphoreType.DMA((2,)), pltpu.SemaphoreType.DMA((2,)),
    ]
    near = pl.BlockSpec(memory_space=pltpu.VMEM)
    passed = pl.pallas_call(
        functools.partial(kernel, (cx, cy, cz), count, nx, ny),
        out_shape=made,
        in_specs=[pl.BlockSpec(memory_space=pltpu.HBM)] * 7,
        out_specs=(near,) * len(made),
        scratch_shapes=scratch,
        compiler_params=pltpu.CompilerParams(
            collective_id=0, has_side_effects=True, vmem_limit_bytes=56 * 1024 * 1024),
    )(volume, *[jnp.asarray(w) for w in weights])
    return pl.pallas_call(
        functools.partial(finish, (cx, cy, cz), count),
        out_shape=jax.ShapeDtypeStruct(volume.shape, f32),
        in_specs=[near] * len(made),
        out_specs=pl.BlockSpec(memory_space=pltpu.HBM),
        scratch_shapes=[
            vmem(qx + 2, ey3, LANES), vmem(qx + 2, ey3, LANES), vmem(hx + 2, 2 * ey3, LANES),
            vmem(hx + 1, hy + PAD, LANES),
            vmem(cx, hy + PAD, LANES), vmem(cx, 2, cy, LANES), vmem(cx, cy, cz), pltpu.SemaphoreType.DMA((cx // 8,)),
        ],
        compiler_params=pltpu.CompilerParams(vmem_limit_bytes=24 * 1024 * 1024),
    )(*passed)


def solution(mesh):
    spec = P("gx", "gy", None)
    body = functools.partial(on_device, mesh.shape["gx"], mesh.shape["gy"])
    return jax.shard_map(body, mesh=mesh, in_specs=(spec,), out_specs=spec, check_vma=False)
```

```python
import functools
import math

import jax
import jax.numpy as jnp
import numpy as np
from jax import lax
from jax.experimental import pallas as pl
from jax.experimental.pallas import tpu as pltpu
from jax.sharding import PartitionSpec as P

ROOT3 = math.sqrt(3.0)
NEAR = math.sqrt(3.0) / 4.0
FAR = (math.sqrt(3.0) - 2.0) / 4.0
LOW = (math.sqrt(3.0) - 1.0) / math.sqrt(2.0)
HIGH = (math.sqrt(3.0) + 1.0) / math.sqrt(2.0)
LANES = 128
PAD = 8


def forward_matrix(size):
    lines = np.eye(size)
    even, odd = lines[:, 0::2], lines[:, 1::2]
    smooth = even + ROOT3 * odd
    detail = odd - NEAR * smooth - FAR * np.roll(smooth, 1, 1)
    smooth = smooth - np.roll(detail, -1, 1)
    return np.concatenate([LOW * smooth, HIGH * detail], 1)


def inverse_matrix(size):
    lines = np.eye(size)
    smooth, detail = lines[:, : size // 2] / LOW, lines[:, size // 2 :] / HIGH
    first = smooth + np.roll(detail, -1, 1)
    odd = detail + NEAR * first + FAR * np.roll(first, 1, 1)
    even = first - ROOT3 * odd
    return np.stack([even, odd], 2).reshape(size, size)


def halves(matrix, size):
    full = np.zeros((size, size))
    full[: matrix.shape[0], : matrix.shape[1]] = matrix
    high = full.astype(jnp.bfloat16)
    low = (full - high.astype(np.float64)).astype(jnp.bfloat16)
    return np.stack([high, low])


def times(values, w_ref):
    high = values.astype(jnp.bfloat16)
    low = (values - high.astype(jnp.float32)).astype(jnp.bfloat16)
    dot = functools.partial(jnp.dot, preferred_element_type=jnp.float32)
    return dot(high, w_ref[0]) + (dot(low, w_ref[0]) + dot(high, w_ref[1]))


def folded(matrix):
    high, low = halves(matrix, LANES)
    return np.block([[high, low], [high, np.zeros_like(low)]])


def times_folded(values, w_ref):
    high = values.astype(jnp.bfloat16)
    low = (values - high.astype(jnp.float32)).astype(jnp.bfloat16)
    both = jnp.dot(jnp.concatenate([high, low], axis=1), w_ref[...],
                   preferred_element_type=jnp.float32)
    return both[:, :LANES] + both[:, LANES:]


def shrink(values, noise):
    return values - jnp.clip(values, -noise, noise)


def sums(even, odd):
    smooth = even + ROOT3 * odd
    return smooth, odd - NEAR * smooth


def undo(detail, first, before):
    odd = detail + NEAR * first + FAR * before
    return first - ROOT3 * odd, odd


def weave(even, odd):
    both = jnp.stack([even, odd], axis=1)
    return both.reshape((2 * even.shape[0],) + even.shape[1:])


def forward_rows(even, odd):
    axis = even.ndim - 2
    smooth, part = sums(even, odd)
    detail = part - FAR * pltpu.roll(smooth, 1, axis)
    return detail, smooth - pltpu.roll(detail, even.shape[axis] - 1, axis)


def limits(noise, level):
    base = noise * (1.0 / LOW ** (2 * (level - 1)))
    return base * (1.0 / (HIGH * HIGH)), base * (1.0 / (HIGH * LOW)), base * (1.0 / (LOW * LOW))


def spread(total, count_all):
    return jnp.sum(total, axis=(0, 1), keepdims=True) * (
        HIGH * HIGH * math.sqrt(math.pi / 2.0) / count_all)


def inverse1(hx, one_x, put):
    def step(n, carry):
        d, before = carry
        after, one = one_x(n + 1)
        even, odd = undo(d, one, before)
        put(2 * n, even)
        put(2 * n + 1, odd)
        return after, one

    lax.fori_loop(0, hx, step, one_x(0), unroll=4)


def kernel(shape, count_all, nx, ny, vol, g1, g2, g3, g4, g5, g6,
           d1s, p1d, p1s1, dd, ds, sd, ep3, b3, noise, v1, v2, v3,
           w1, w2, w3, d1d, s1d, s1s,
           e1, lx, rx, hx1, sx1, hy1, sy1, hc1, sc1, xd1, xs1,
           e2, xl, xh, xlow, xhigh, xd2, xs2, t3d, t3s,
           mine, rows_in, dummy, send, recv, lsem, wsem):
    cx, cy, cz = shape
    hx, hy, qx, qy = cx // 2, cy // 2, cx // 4, cy // 4
    ix, iy = lax.axis_index("gx"), lax.axis_index("gy")

    def device(dx, dy):
        return (lax.rem(ix + dx + nx, nx), lax.rem(iy + dy + ny, ny))

    near = [(dx, dy) for dx in (-1, 0, 1) for dy in (-1, 0, 1) if dx or dy]
    peers = [(dx, dy) for dx in range(nx) for dy in range(ny) if dx or dy]
    taken = {(dx % nx, dy % ny) for dx, dy in near}
    barrier = pltpu.get_barrier_semaphore()

    def greet(dx, dy):
        pl.semaphore_signal(barrier, inc=1, device_id=device(dx, dy),
                            device_id_type=pl.DeviceIdType.MESH)

    for d in sorted(taken):
        greet(*d)
    loads = [
        pltpu.make_async_copy(
            vol.at[:, :, pl.ds(h * LANES, LANES)],
            e1.at[:, h, pl.ds(PAD, cy), :], lsem.at[h])
        for h in range(2)
    ]
    for c in loads:
        c.start()
    for d in peers:
        if d not in taken:
            greet(*d)
    first_weight = pltpu.make_async_copy(g1, w1, wsem.at[0])
    first_weight.start()
    more = list(zip((g2, g3, g4, g5, g6), (w2, w3, v1, v2, v3)))
    for src, dst in more:
        pltpu.make_async_copy(src, dst, wsem.at[1]).start()

    sent = [0]

    def post(src, dst, dx, dy, group):
        sent[0] += math.prod(src.shape) // LANES
        pltpu.make_async_remote_copy(
            src_ref=src, dst_ref=dst, send_sem=send.at[0], recv_sem=recv.at[group],
            device_id=device(dx, dy), device_id_type=pl.DeviceIdType.MESH).start()
        return math.prod(src.shape) // LANES

    def land(sem, rows):
        part = dummy.at[pl.ds(0, rows)]
        pltpu.make_async_copy(part, part, sem).wait()

    ep3[:, 0 : PAD // 2] = jnp.zeros((qx + 4, PAD // 2, LANES), jnp.float32)
    ep3[:, PAD // 2 + hy // 2 + PAD :] = jnp.zeros((qx + 4, PAD // 2, LANES), jnp.float32)
    for ref in (dd, ds, sd):
        ref[:, 0 : PAD // 2] = jnp.zeros((qx + 2, PAD // 2, LANES), jnp.float32)
        ref[:, PAD // 2 + hy // 2 + PAD :] = jnp.zeros((qx + 2, PAD // 2, LANES), jnp.float32)

    top = PAD + cy
    own1, own = slice(PAD, top), slice(PAD, PAD + hy)
    for c in loads:
        c.wait()
    first_weight.wait()

    def depth(xs, ys):
        shape = (xs.stop - xs.start, ys.stop - ys.start, LANES)
        rows = jnp.concatenate(
            [e1[xs, h, ys].reshape(shape[0] * shape[1], LANES) for h in range(2)], axis=1)
        got = times(rows, w1)
        for h in range(2):
            e1[xs, h, ys] = got[:, h * LANES : (h + 1) * LANES].reshape(shape)

    inner = slice(2 * PAD, top - PAD)
    depth(slice(0, cx), slice(PAD, 2 * PAD))
    depth(slice(0, cx), slice(top - PAD, top))
    depth(slice(0, 2), inner)
    depth(slice(cx - 2, cx), inner)
    sx1[1] = sums(e1[0, :, own1], e1[1, :, own1])[1]
    sx1[0] = sums(e1[cx - 2, :, own1], e1[cx - 1, :, own1])[0]
    sy1[1] = sums(e1[:, :, PAD : PAD + 1], e1[:, :, PAD + 1 : PAD + 2])[1]
    sy1[0] = sums(e1[:, :, top - 2 : top - 1], e1[:, :, top - 1 : top])[0]
    for x in range(2):
        sc1[x, 1] = sums(sx1[x, :, 0:1], sx1[x, :, 1:2])[1]
        sc1[x, 0] = sums(sx1[x, :, cy - 2 : cy - 1], sx1[x, :, cy - 1 : cy])[0]
    line = lax.broadcasted_iota(jnp.int32, (hy, LANES), 0)
    for x in range(2):
        load = lambda start: sx1[x, 1 - x, pl.ds(start, hy, stride=2), :]
        smooth, part = sums(load(0), load(1))
        detail = part - jnp.where(line > 0, FAR * pltpu.roll(smooth, 1, 0), 0.0)
        lx[x, 0] = detail
        lx[x, 1] = smooth - jnp.where(line < hy - 1, pltpu.roll(detail, hy - 1, 0), 0.0)
    pl.semaphore_wait(barrier, len(peers))
    step = (1, -1)
    post_x = lambda x, h, g: post(
        sx1.at[x, h], hx1.at[x, h, pl.ds(PAD, cy), :], step[x], 0, g)
    post_y = lambda y, h, g: post(sy1.at[y, :, h], hy1.at[y, :, h], 0, step[y], g)
    post_c = lambda x, y, h, g: post(
        sc1.at[x, y, h], hc1.at[x, y, h], step[x], step[y], g)
    post_l = lambda x, k, g: post(lx.at[x, k], rx.at[x, k], step[x], 0, g)
    noise1 = post_c(0, 0, 1, 0)
    coarse1 = post_c(1, 1, 0, 1) + post_l(1, 1, 1)
    noise1 += post_l(0, 0, 0) + post_y(0, 1, 0)
    coarse1 += post_y(1, 0, 1)
    later1 = (post_c(0, 0, 0, 2) + post_c(1, 1, 1, 2) + post_x(0, 0, 2) + post_x(1, 1, 2)
              + post_l(0, 1, 2) + post_l(1, 0, 2)
              + post_y(0, 0, 2) + post_y(1, 1, 2))
    for h in range(2):
        later1 += post_c(0, 1, h, 2) + post_c(1, 0, h, 2)

    slab = 4
    for lo in range(2, cx - 2, slab):
        depth(slice(lo, min(lo + slab, cx - 2)), inner)

    def pair1(n, rows=slice(None)):
        return sums(e1[2 * n, :, rows], e1[2 * n + 1, :, rows])

    def lift1(rows):
        def step(n, carry):
            _, part_n = pair1(n, rows)
            before, _ = pair1(n - 1, rows)
            detail = part_n - FAR * before
            xd1[n, :, rows] = detail
            xs1[n, :, rows] = before - detail
            return carry

        lax.fori_loop(1, hx, step, 0)

    def shrunk(n):
        load = lambda start: xs1[n, 0, pl.ds(start, hy, stride=2), :]
        s0, _ = sums(load(PAD), load(PAD + 1))
        _, tp = sums(load(PAD + 2), load(PAD + 3))
        s1s[n, 0, own] = s0 - (tp - FAR * s0)

    def finest(n):
        load = lambda start: xd1[n, 1, pl.ds(start, hy, stride=2), :]
        _, t0 = sums(load(PAD), load(PAD + 1))
        sm, _ = sums(load(PAD - 2), load(PAD - 1))
        return t0 - FAR * sm

    def fold(values):
        return jnp.sum(values.reshape(hy // PAD, PAD, LANES), axis=0)

    known = line > 0

    def inside(n, magnitude):
        shrunk(n)
        return magnitude + fold(jnp.where(known, jnp.abs(finest(n)), 0.0))

    lift1(own1)
    magnitude = lax.fori_loop(1, hx, inside, jnp.zeros((PAD, LANES), jnp.float32))
    land(wsem.at[1], sum(2 * math.prod(dst.shape) // (4 * LANES) for _, dst in more))
    done = hy - PAD
    rows = s1s[1:hx, 0, PAD : PAD + done].reshape((hx - 1) * done, LANES)
    e2[0 : hx - 1, PAD : PAD + done] = times_folded(rows, w2).reshape(hx - 1, done, LANES)

    land(recv.at[0], noise1)
    edge = hy1[0, :, 1].reshape(hx, 2, 1, LANES)
    edge_s, edge_t = sums(edge[:, 0], edge[:, 1])
    edge_d = edge_t - FAR * jnp.concatenate([hc1[0, 0, 1][None], edge_s[:-1]], axis=0)
    xd1[0, 1, own1] = sums(e1[0, 1, own1], e1[1, 1, own1])[1]
    xd1[0, 1, PAD - 2 : PAD - 1] = edge_d[0]
    xd1[0, 1, PAD - 1 : PAD] = jnp.zeros((1, LANES), jnp.float32)
    _, edge_t = sums(xd1[1:hx, 1, PAD : PAD + 1], xd1[1:hx, 1, PAD + 1 : PAD + 2])
    row = jnp.sum(jnp.abs(edge_t - FAR * edge_d[1:]), axis=0)
    mine[...] = row + jnp.sum(magnitude + fold(jnp.abs(finest(0) - FAR * rx[0, 0])), axis=0, keepdims=True)
    landed = 0
    for k, d in enumerate(peers):
        landed += post(mine, rows_in.at[k], d[0], d[1], 4)

    land(recv.at[1], coarse1)
    edge, _ = sums(e1[cx - 2, 0, own1], e1[cx - 1, 0, own1])
    xs1[hx, 0, own1] = edge * (1.0 + FAR)
    shrunk(hx)
    s1s[hx, 0, own] = s1s[hx, 0, own] - rx[1, 1]
    edge = hy1[1, :, 0].reshape(hx, 2, 1, LANES)
    edge_s, edge_t = sums(edge[:, 0], edge[:, 1])
    after = jnp.concatenate([edge_t[1:], hc1[1, 1, 0][None]], axis=0)
    last_t = edge_s - (after - FAR * edge_s)
    last_s, _ = sums(xs1[1 : hx + 1, 0, top - 2 : top - 1], xs1[1 : hx + 1, 0, top - 1 : top])
    last_s = jnp.concatenate([last_s[:-1], last_s[-1:] - rx[1, 1, hy - 1 : hy][None]], axis=0)
    s1s[1 : hx + 1, 0, PAD + hy - 1 : PAD + hy] = last_s - (last_t - FAR * last_s)
    rows = jnp.concatenate(
        [s1s[1:hx, 0, PAD + done : PAD + hy].reshape((hx - 1) * PAD, LANES), s1s[hx, 0, own]],
        axis=0)
    got = times_folded(rows, w2)
    e2[0 : hx - 1, PAD + done : PAD + hy] = got[: (hx - 1) * PAD].reshape(hx - 1, PAD, LANES)
    e2[hx - 1, own] = got[(hx - 1) * PAD :]

    def pair2(m, rows):
        return sums(e2[2 * m, rows], e2[2 * m + 1, rows])

    def coarse2(m, rows):
        return pair2(m, rows)[0] * (1.0 + FAR) - pair2(m + 1, rows)[1]

    xl[0] = pair2(qx - 2, own)[0]
    xl[1] = e2[hx - 2, own]
    xl[2] = e2[hx - 1, own]
    xl[3] = sums(coarse2(qx - 4, own), coarse2(qx - 3, own))[0]
    xh[0] = pair2(0, own)[1]
    xh[1] = sums(coarse2(0, own), coarse2(1, own))[1]
    y_own, y_low, y_high = pl.ds(PAD, hy), pl.ds(0, PAD), pl.ds(PAD + hy, PAD)
    s_own, s_first, s_last = pl.ds(0, hy), pl.ds(0, PAD), pl.ds(hy - PAD, PAD)
    round2 = 0
    for rows_s, rows_d, dy in ((s_own, y_own, 0), (s_last, y_low, 1), (s_first, y_high, -1)):
        round2 += post(xl.at[:, rows_s, :], xlow.at[:, rows_d, :], 1, dy, 3)
        round2 += post(xh.at[:, rows_s, :], xhigh.at[:, rows_d, :], -1, dy, 3)
    round2 += post(e2.at[:, pl.ds(PAD, PAD), :], e2.at[:, y_high, :], 0, -1, 3)
    round2 += post(e2.at[:, pl.ds(hy, PAD), :], e2.at[:, y_low, :], 0, 1, 3)

    land(recv.at[2], later1)

    def place(ref, rows, side):
        if side == 0:
            ref[..., PAD - 2 : PAD - 1, :] = rows
            ref[..., PAD - 1 : PAD, :] = jnp.zeros_like(rows)
        else:
            ref[..., top : top + 1, :] = -ROOT3 * rows
            ref[..., top + 1 : top + 2, :] = rows

    for x in range(2):
        detail, smooth = rx[x, 0], rx[x, 1]
        smooth = smooth + jnp.where(line < hy - 1, pltpu.roll(detail, hy - 1, 0), 0.0)
        part = detail + jnp.where(line > 0, FAR * pltpu.roll(smooth, 1, 0), 0.0)
        odd = part + NEAR * smooth
        hx1[x, 1 - x, pl.ds(PAD, hy, stride=2), :] = smooth - ROOT3 * odd
        hx1[x, 1 - x, pl.ds(PAD + 1, hy, stride=2), :] = odd
    for side in range(2):
        place(e1, hy1[side], side)
        for x in range(2):
            place(hx1.at[x], hc1[x, side], side)
    lift1(slice(PAD - 2, PAD))
    lift1(slice(top, top + 2))
    wide = slice(PAD - 2, top + 2)
    _, edge = pair1(0, wide)
    detail = edge - FAR * hx1[0, :, wide]
    xd1[0, :, wide] = detail
    xs1[0, :, wide] = hx1[0, :, wide] - detail
    edge, _ = pair1(hx - 1, wide)
    detail = hx1[1, :, wide] - FAR * edge
    xd1[hx, :, wide] = detail
    xs1[hx, :, wide] = edge - detail

    def cols1(src, det, smo):
        def step(n, carry):
            for h in range(2):
                load = lambda start: src[n, h, pl.ds(start, hy + 1, stride=2), :]
                s0, t0 = sums(load(PAD), load(PAD + 1))
                sm, _ = sums(load(PAD - 2), load(PAD - 1))
                d = t0 - FAR * sm
                det[n, h, 0 : hy + 1] = d
                smo[n, h, PAD - 1 : PAD + hy] = sm - d
            return carry

        lax.fori_loop(0, hx + 1, step, 0)

    cols1(xd1, d1d, d1s)
    cols1(xs1, s1d, s1s)

    land(recv.at[4], landed)
    acc = mine[...]
    for k in range(len(peers)):
        acc = acc + rows_in[k]
    level = spread(acc, count_all)
    noise[...] = jnp.broadcast_to(level, (PAD, LANES))
    far1, mid1, near1 = limits(level, 1)

    def put_into(dst, h):
        def put(n, rows):
            if h is None:
                dst[n] = rows
            else:
                dst[n, h] = rows
        return put

    def bands1(det, smo, h, limit_d, limit_s):
        def one_x(n):
            d = shrink(det[n, h], limit_d)
            return d, shrink(smo[n, h], limit_s) + d
        return one_x

    for h in range(2):
        inverse1(hx, bands1(d1d, s1d, h, far1, mid1), put_into(p1d, h))
    inverse1(hx, bands1(d1s, s1s, 1, mid1, near1), put_into(p1s1, None))

    land(recv.at[3], round2)
    every = slice(0, hy + 2 * PAD)
    before = xlow[0]
    xs2[0] = xlow[3]
    for m in range(-1, qx + 1):
        if m == qx:
            smooth, part = None, xhigh[0]
        elif m == -1:
            smooth, part = sums(xlow[1], xlow[2])
        else:
            smooth, part = pair2(m, every)
        detail = part - FAR * before
        xd2[m + 1] = detail
        xs2[m + 2] = before - detail
        before = smooth
    xs2[qx + 3] = xhigh[1]
    pairs = hy // 2 + PAD

    def rows2(src):
        return forward_rows(src[:, pl.ds(0, pairs, stride=2), :],
                            src[:, pl.ds(1, pairs, stride=2), :])

    mid = slice(PAD // 2, PAD // 2 + pairs)
    dd[:, mid], ds[:, mid] = rows2(xd2)
    det, smo = rows2(xs2)
    sd[:, mid] = det[1 : qx + 3]
    ep3[:, mid] = smo

    n_own, n3, h3 = qx // 2, qx // 2 + 2, qy // 2 + PAD
    low_s, low_t = [ep3[0]], [None]
    for n in range(n_own + 1):
        s, t = sums(ep3[1 + 2 * n], ep3[2 + 2 * n])
        low_s.append(s)
        low_t.append(t)
    low_t.append(ep3[qx + 3])
    for n in range(n3):
        detail = low_t[n + 1] - FAR * low_s[n]
        t3d[n] = detail
        t3s[n] = low_s[n] - detail
    bands = []
    for src in (t3d, t3s):
        bands += forward_rows(src[:, pl.ds(0, h3, stride=2), :], src[:, pl.ds(1, h3, stride=2), :])
    for i, band in enumerate(bands):
        b3[i] = times_folded(band.reshape(n3 * h3, LANES), w3).reshape(n3, h3, LANES)

    land(send.at[0], sent[0])


def finish(shape, d1s, p1d, p1s1, dd, ds, sd, ep3, b3, total, v1, v2, v3, out,
           ss, r2, r1, s0, p1s0, o1, ob, osem):
    cx, cy, cz = shape
    hx, hy, qx, qy = cx // 2, cy // 2, cx // 4, cy // 4
    n3, h3, x2, yrows = qx // 2 + 2, qy // 2 + PAD, qx + 2, qy + 2 * PAD
    noise = total[0:1]


    far3, mid3, near3 = (v[None] for v in limits(noise, 3))
    lane3 = lax.broadcasted_iota(jnp.int32, (n3, h3, LANES), 2)
    b_dd, b_ds, b_sd = shrink(b3[0], far3), shrink(b3[1], mid3), shrink(b3[2], mid3)
    b_ss = jnp.where(lane3 < cz // 8, b3[3], shrink(b3[3], near3))

    def inverse_x(det, smo):
        one = smo + det
        even, odd = undo(det[:-1], one[1:], one[:-1])
        return weave(even, odd)

    y_d = inverse_x(b_dd, b_sd)
    y_s = inverse_x(b_ds, b_ss)
    one = y_s + pltpu.roll(y_d, h3 - 1, 1)
    even, odd = undo(y_d, one, pltpu.roll(one, 1, 1))
    r2[:, pl.ds(0, h3, stride=2), :] = even
    r2[:, pl.ds(1, h3, stride=2), :] = odd
    back = times_folded(r2[...].reshape(x2 * yrows, LANES), v3).reshape(x2, yrows, LANES)

    far2, mid2, near2 = limits(noise, 2)
    lane2 = lax.broadcasted_iota(jnp.int32, (x2, yrows, LANES), 2)
    ss[...] = jnp.where(lane2 < cz // 4, back, shrink(ep3[1 : qx + 3], near2[None]))

    def one_x(n):
        d_d = shrink(dd[n], far2)
        d_s = shrink(ds[n], mid2)
        s_d = shrink(sd[n], mid2)
        return d_d, d_s, s_d + d_d, ss[n] + d_s

    def inv2(n, carry):
        d_d, d_s, b_d, b_s = carry
        after = one_x(n + 1)
        pair_d = undo(d_d, after[2], b_d)
        pair_s = undo(d_s, after[3], b_s)
        for i in range(2):
            y_d, y_s = pair_d[i], pair_s[i]
            one = y_s + pltpu.roll(y_d, yrows - 1, 0)
            even, odd = undo(y_d, one, pltpu.roll(one, 1, 0))
            r1[2 * n + i, pl.ds(0, yrows, stride=2), :] = even
            r1[2 * n + i, pl.ds(1, yrows, stride=2), :] = odd
        return after

    lax.fori_loop(0, qx + 1, inv2, one_x(0), unroll=3)
    x1, y1 = hx + 2, hy + PAD
    back = times_folded(r1[:, PAD : PAD + y1].reshape(x1 * y1, LANES), v2).reshape(x1, y1, LANES)
    s0[...] = back[1:]
    _, mid1, _ = limits(noise, 1)

    def low_x(n):
        d = shrink(d1s[n, 0], mid1)
        return d, s0[n] + d

    def put_low(n, rows):
        p1s0[n] = rows

    inverse1(hx, low_x, put_low)

    def inv1_y(n):
        for h in range(2):
            y_d = p1d[n, h, 0:hy]
            y_n = p1d[n, h, 1 : hy + 1]
            p1s = p1s1 if h else p1s0
            s = p1s[n, PAD : PAD + hy]
            s_b = p1s[n, PAD - 1 : PAD - 1 + hy]
            even, odd = undo(y_d, s + y_n, s_b + y_d)
            o1[n, h, pl.ds(0, hy, stride=2), :] = even
            o1[n, h, pl.ds(1, hy, stride=2), :] = odd

    layers = 8
    outs = []
    for n in range(layers):
        inv1_y(n)
    for i in range(cx // layers):
        for n in range((i + 1) * layers, min((i + 2) * layers, cx)):
            inv1_y(n)
        xs = slice(i * layers, (i + 1) * layers)
        rows = jnp.concatenate(
            [o1[xs, h].reshape(layers * cy, LANES) for h in range(2)], axis=1)
        ob[xs] = times(rows, v1).reshape(layers, cy, cz)
        c = pltpu.make_async_copy(ob.at[xs], out.at[xs], osem.at[i])
        c.start()
        outs.append(c)
    for c in outs:
        c.wait()


def on_device(nx, ny, volume):
    cx, cy, cz = volume.shape
    hx, hy, qx, qy = cx // 2, cy // 2, cx // 4, cy // 4
    n3, h3 = qx // 2 + 2, qy // 2 + PAD
    f32 = jnp.float32
    count = cx * nx * cy * ny * cz // 8
    weights = [
        halves(forward_matrix(cz), cz), folded(forward_matrix(cz // 2)),
        folded(forward_matrix(cz // 4)), halves(inverse_matrix(cz), cz),
        folded(inverse_matrix(cz // 2)), folded(inverse_matrix(cz // 4)),
    ]
    vmem = lambda *s: pltpu.VMEM(s, f32)
    ey, ey2, ey3 = cy + 2 * PAD, hy + 2 * PAD, qy + 2 * PAD
    wide = lambda *s: pltpu.VMEM(s, jnp.bfloat16)
    pair = (2 * LANES, 2 * LANES)
    made = (
        vmem(hx + 1, 2, hy + PAD, LANES), vmem(cx, 2, hy + PAD, LANES),
        vmem(cx, hy + PAD, LANES), *[vmem(qx + 2, ey3, LANES) for _ in range(3)],
        vmem(qx + 4, ey3, LANES), vmem(4, n3, h3, LANES), vmem(PAD, LANES),
        wide(2, cz, cz), wide(*pair), wide(*pair),
    )
    rows = 4 * cy + 4 * cx + 8 + 6 * (hy + 2 * PAD) + 2 * hx * PAD + nx * ny
    scratch = [
        wide(2, cz, cz), wide(*pair), wide(*pair),
        *[vmem(hx + 1, 2, hy + PAD, LANES) for _ in range(3)],
        vmem(cx, 2, ey, LANES), vmem(2, 2, hy, LANES), vmem(2, 2, hy, LANES),
        vmem(2, 2, ey, LANES), vmem(2, 2, cy, LANES),
        vmem(2, cx, 2, 1, LANES), vmem(2, cx, 2, 1, LANES),
        vmem(2, 2, 2, 1, LANES), vmem(2, 2, 2, 1, LANES),
        vmem(hx + 1, 2, ey, LANES), vmem(hx + 1, 2, ey, LANES),
        vmem(hx, ey2, LANES), vmem(4, hy, LANES), vmem(2, hy, LANES),
        vmem(4, ey2, LANES), vmem(2, ey2, LANES),
        vmem(qx + 2, ey2, LANES), vmem(qx + 4, ey2, LANES),
        vmem(n3, ey3, LANES), vmem(n3, ey3, LANES),
        vmem(1, LANES), vmem(nx * ny - 1, 1, LANES), vmem(max(rows, cz * cz // 32), 1, LANES),
        pltpu.SemaphoreType.DMA((1,)), pltpu.SemaphoreType.DMA((5,)),
        pltpu.SemaphoreType.DMA((2,)), pltpu.SemaphoreType.DMA((2,)),
    ]
    near = pl.BlockSpec(memory_space=pltpu.VMEM)
    passed = pl.pallas_call(
        functools.partial(kernel, (cx, cy, cz), count, nx, ny),
        out_shape=made,
        in_specs=[pl.BlockSpec(memory_space=pltpu.HBM)] * 7,
        out_specs=(near,) * len(made),
        scratch_shapes=scratch,
        compiler_params=pltpu.CompilerParams(
            collective_id=0, has_side_effects=True, vmem_limit_bytes=56 * 1024 * 1024),
    )(volume, *[jnp.asarray(w) for w in weights])
    return pl.pallas_call(
        functools.partial(finish, (cx, cy, cz)),
        out_shape=jax.ShapeDtypeStruct(volume.shape, f32),
        in_specs=[near] * len(made),
        out_specs=pl.BlockSpec(memory_space=pltpu.HBM),
        scratch_shapes=[
            vmem(qx + 2, ey3, LANES), vmem(qx + 2, ey3, LANES), vmem(hx + 2, 2 * ey3, LANES),
            vmem(hx + 1, hy + PAD, LANES),
            vmem(cx, hy + PAD, LANES), vmem(cx, 2, cy, LANES), vmem(cx, cy, cz), pltpu.SemaphoreType.DMA((cx // 8,)),
        ],
        compiler_params=pltpu.CompilerParams(vmem_limit_bytes=24 * 1024 * 1024),
    )(*passed)


def solution(mesh):
    spec = P("gx", "gy", None)
    body = functools.partial(on_device, mesh.shape["gx"], mesh.shape["gy"])
    return jax.shard_map(body, mesh=mesh, in_specs=(spec,), out_specs=spec, check_vma=False)
```

```python
import functools
import math

import jax
import jax.numpy as jnp
import numpy as np
from jax import lax
from jax.experimental import pallas as pl
from jax.experimental.pallas import tpu as pltpu
from jax.sharding import PartitionSpec as P

ROOT3 = math.sqrt(3.0)
NEAR = math.sqrt(3.0) / 4.0
FAR = (math.sqrt(3.0) - 2.0) / 4.0
LOW = (math.sqrt(3.0) - 1.0) / math.sqrt(2.0)
HIGH = (math.sqrt(3.0) + 1.0) / math.sqrt(2.0)
LANES = 128
PAD = 8


def forward_matrix(size):
    lines = np.eye(size)
    even, odd = lines[:, 0::2], lines[:, 1::2]
    smooth = even + ROOT3 * odd
    detail = odd - NEAR * smooth - FAR * np.roll(smooth, 1, 1)
    smooth = smooth - np.roll(detail, -1, 1)
    return np.concatenate([LOW * smooth, HIGH * detail], 1)


def inverse_matrix(size):
    lines = np.eye(size)
    smooth, detail = lines[:, : size // 2] / LOW, lines[:, size // 2 :] / HIGH
    first = smooth + np.roll(detail, -1, 1)
    odd = detail + NEAR * first + FAR * np.roll(first, 1, 1)
    even = first - ROOT3 * odd
    return np.stack([even, odd], 2).reshape(size, size)


def halves(matrix, size):
    full = np.zeros((size, size))
    full[: matrix.shape[0], : matrix.shape[1]] = matrix
    high = full.astype(jnp.bfloat16)
    low = (full - high.astype(np.float64)).astype(jnp.bfloat16)
    return np.stack([high, low])


def times(values, w_ref):
    high = values.astype(jnp.bfloat16)
    low = (values - high.astype(jnp.float32)).astype(jnp.bfloat16)
    dot = functools.partial(jnp.dot, preferred_element_type=jnp.float32)
    return dot(high, w_ref[0]) + (dot(low, w_ref[0]) + dot(high, w_ref[1]))


def folded(matrix):
    high, low = halves(matrix, LANES)
    return np.block([[high, low], [high, np.zeros_like(low)]])


def times_folded(values, w_ref):
    high = values.astype(jnp.bfloat16)
    low = (values - high.astype(jnp.float32)).astype(jnp.bfloat16)
    both = jnp.dot(jnp.concatenate([high, low], axis=1), w_ref[...],
                   preferred_element_type=jnp.float32)
    return both[:, :LANES] + both[:, LANES:]


def shrink(values, noise):
    return values - jnp.clip(values, -noise, noise)


def sums(even, odd):
    smooth = even + ROOT3 * odd
    return smooth, odd - NEAR * smooth


def undo(detail, first, before):
    odd = detail + NEAR * first + FAR * before
    return first - ROOT3 * odd, odd


def weave(even, odd):
    both = jnp.stack([even, odd], axis=1)
    return both.reshape((2 * even.shape[0],) + even.shape[1:])


def forward_rows(even, odd):
    axis = even.ndim - 2
    smooth, part = sums(even, odd)
    detail = part - FAR * pltpu.roll(smooth, 1, axis)
    return detail, smooth - pltpu.roll(detail, even.shape[axis] - 1, axis)


def limits(noise, level):
    base = noise * (1.0 / LOW ** (2 * (level - 1)))
    return base * (1.0 / (HIGH * HIGH)), base * (1.0 / (HIGH * LOW)), base * (1.0 / (LOW * LOW))


def spread(total, count_all):
    return jnp.sum(total, axis=(0, 1), keepdims=True) * (
        HIGH * HIGH * math.sqrt(math.pi / 2.0) / count_all)


def inverse1(hx, one_x, put):
    def step(n, carry):
        d, before = carry
        after, one = one_x(n + 1)
        even, odd = undo(d, one, before)
        put(2 * n, even)
        put(2 * n + 1, odd)
        return after, one

    lax.fori_loop(0, hx, step, one_x(0), unroll=4)


def kernel(shape, count_all, nx, ny, vol, g1, g2, g3, g4, g5, g6,
           d1s, p1d, p1s1, dd, ds, sd, ep3, b3, noise, v1, v2, v3,
           w1, w2, w3, d1d, s1d, s1s,
           e1, lx, rx, tc, fix, hx1, sx1, hy1, sy1, hc1, sc1, xd1, xs1,
           e2, xl, xh, xlow, xhigh, xd2, xs2, t3d, t3s,
           mine, rows_in, dummy, send, recv, lsem, wsem):
    cx, cy, cz = shape
    hx, hy, qx, qy = cx // 2, cy // 2, cx // 4, cy // 4
    ix, iy = lax.axis_index("gx"), lax.axis_index("gy")

    def device(dx, dy):
        return (lax.rem(ix + dx + nx, nx), lax.rem(iy + dy + ny, ny))

    near = [(dx, dy) for dx in (-1, 0, 1) for dy in (-1, 0, 1) if dx or dy]
    peers = [(dx, dy) for dx in range(nx) for dy in range(ny) if dx or dy]
    taken = {(dx % nx, dy % ny) for dx, dy in near}
    barrier = pltpu.get_barrier_semaphore()

    def greet(dx, dy):
        pl.semaphore_signal(barrier, inc=1, device_id=device(dx, dy),
                            device_id_type=pl.DeviceIdType.MESH)

    for d in sorted(taken):
        greet(*d)
    loads = [
        pltpu.make_async_copy(
            vol.at[:, :, pl.ds(h * LANES, LANES)],
            e1.at[:, h, pl.ds(PAD, cy), :], lsem.at[h])
        for h in range(2)
    ]
    for c in loads:
        c.start()
    for d in peers:
        if d not in taken:
            greet(*d)
    first_weight = pltpu.make_async_copy(g1, w1, wsem.at[0])
    first_weight.start()
    more = list(zip((g2, g3, g4, g5, g6), (w2, w3, v1, v2, v3)))
    for src, dst in more:
        pltpu.make_async_copy(src, dst, wsem.at[1]).start()

    sent = [0]

    def post(src, dst, dx, dy, group):
        sent[0] += math.prod(src.shape) // LANES
        pltpu.make_async_remote_copy(
            src_ref=src, dst_ref=dst, send_sem=send.at[0], recv_sem=recv.at[group],
            device_id=device(dx, dy), device_id_type=pl.DeviceIdType.MESH).start()
        return math.prod(src.shape) // LANES

    def land(sem, rows):
        part = dummy.at[pl.ds(0, rows)]
        pltpu.make_async_copy(part, part, sem).wait()

    ep3[:, 0 : PAD // 2] = jnp.zeros((qx + 4, PAD // 2, LANES), jnp.float32)
    ep3[:, PAD // 2 + hy // 2 + PAD :] = jnp.zeros((qx + 4, PAD // 2, LANES), jnp.float32)
    fix[...] = jnp.zeros((2, hy + 2 * PAD, LANES), jnp.float32)
    for ref in (dd, ds, sd):
        ref[:, 0 : PAD // 2] = jnp.zeros((qx + 2, PAD // 2, LANES), jnp.float32)
        ref[:, PAD // 2 + hy // 2 + PAD :] = jnp.zeros((qx + 2, PAD // 2, LANES), jnp.float32)

    top = PAD + cy
    own1, own = slice(PAD, top), slice(PAD, PAD + hy)
    for c in loads:
        c.wait()
    first_weight.wait()

    def depth(xs, ys):
        shape = (xs.stop - xs.start, ys.stop - ys.start, LANES)
        rows = jnp.concatenate(
            [e1[xs, h, ys].reshape(shape[0] * shape[1], LANES) for h in range(2)], axis=1)
        got = times(rows, w1)
        for h in range(2):
            e1[xs, h, ys] = got[:, h * LANES : (h + 1) * LANES].reshape(shape)

    inner = slice(2 * PAD, top - PAD)
    depth(slice(0, cx), slice(PAD, 2 * PAD))
    depth(slice(0, cx), slice(top - PAD, top))
    depth(slice(0, 2), inner)
    depth(slice(cx - 2, cx), inner)
    sx1[1] = sums(e1[0, :, own1], e1[1, :, own1])[1]
    sx1[0] = sums(e1[cx - 2, :, own1], e1[cx - 1, :, own1])[0]
    sy1[1] = sums(e1[:, :, PAD : PAD + 1], e1[:, :, PAD + 1 : PAD + 2])[1]
    sy1[0] = sums(e1[:, :, top - 2 : top - 1], e1[:, :, top - 1 : top])[0]
    for x in range(2):
        sc1[x, 1] = sums(sx1[x, :, 0:1], sx1[x, :, 1:2])[1]
        sc1[x, 0] = sums(sx1[x, :, cy - 2 : cy - 1], sx1[x, :, cy - 1 : cy])[0]
    line = lax.broadcasted_iota(jnp.int32, (hy, LANES), 0)
    for x in range(2):
        load = lambda start: sx1[x, 1 - x, pl.ds(start, hy, stride=2), :]
        smooth, part = sums(load(0), load(1))
        detail = part - jnp.where(line > 0, FAR * pltpu.roll(smooth, 1, 0), 0.0)
        lx[x, 0] = detail
        lx[x, 1] = smooth - jnp.where(line < hy - 1, pltpu.roll(detail, hy - 1, 0), 0.0)
    pl.semaphore_wait(barrier, len(peers))
    step = (1, -1)
    post_x = lambda x, h, g: post(
        sx1.at[x, h], hx1.at[x, h, pl.ds(PAD, cy), :], step[x], 0, g)
    post_y = lambda y, h, g: post(sy1.at[y, :, h], hy1.at[y, :, h], 0, step[y], g)
    post_c = lambda x, y, h, g: post(
        sc1.at[x, y, h], hc1.at[x, y, h], step[x], step[y], g)
    post_l = lambda x, k, g: post(lx.at[x, k], rx.at[x, k], step[x], 0, g)
    noise1 = post_c(0, 0, 1, 0)
    coarse1 = post_l(1, 1, 1)
    noise1 += post_l(0, 0, 0) + post_y(0, 1, 0)
    coarse1 += post_y(1, 0, 1)
    later1 = (post_c(1, 1, 0, 2) + post(sc1.at[1, 1, 0], tc.at[0], 0, -1, 2)
              + post(sc1.at[1, 1, 0], tc.at[1], -1, 0, 2) + post_c(0, 0, 0, 2) + post_c(1, 1, 1, 2) + post_x(0, 0, 2) + post_x(1, 1, 2)
              + post_l(0, 1, 2) + post_l(1, 0, 2)
              + post_y(0, 0, 2) + post_y(1, 1, 2))
    for h in range(2):
        later1 += post_c(0, 1, h, 2) + post_c(1, 0, h, 2)

    slab = 4
    for lo in range(2, cx - 2, slab):
        depth(slice(lo, min(lo + slab, cx - 2)), inner)

    def pair1(n, rows=slice(None)):
        return sums(e1[2 * n, :, rows], e1[2 * n + 1, :, rows])

    def lift1(rows):
        def step(n, carry):
            _, part_n = pair1(n, rows)
            before, _ = pair1(n - 1, rows)
            detail = part_n - FAR * before
            xd1[n, :, rows] = detail
            xs1[n, :, rows] = before - detail
            return carry

        lax.fori_loop(1, hx, step, 0)

    def shrunk(n):
        load = lambda start: xs1[n, 0, pl.ds(start, hy, stride=2), :]
        s0, _ = sums(load(PAD), load(PAD + 1))
        _, tp = sums(load(PAD + 2), load(PAD + 3))
        s1s[n, 0, own] = s0 - (tp - FAR * s0)

    def finest(n):
        load = lambda start: xd1[n, 1, pl.ds(start, hy, stride=2), :]
        _, t0 = sums(load(PAD), load(PAD + 1))
        sm, _ = sums(load(PAD - 2), load(PAD - 1))
        return t0 - FAR * sm

    def fold(values):
        return jnp.sum(values.reshape(hy // PAD, PAD, LANES), axis=0)

    known = line > 0

    def inside(n, magnitude):
        shrunk(n)
        return magnitude + fold(jnp.where(known, jnp.abs(finest(n)), 0.0))

    lift1(own1)
    magnitude = lax.fori_loop(1, hx, inside, jnp.zeros((PAD, LANES), jnp.float32))
    land(wsem.at[1], sum(2 * math.prod(dst.shape) // (4 * LANES) for _, dst in more))
    done = hy - PAD
    rows = s1s[1:hx, 0, PAD : PAD + done].reshape((hx - 1) * done, LANES)
    e2[0 : hx - 1, PAD : PAD + done] = times_folded(rows, w2).reshape(hx - 1, done, LANES)

    land(recv.at[0], noise1)
    edge = hy1[0, :, 1].reshape(hx, 2, 1, LANES)
    edge_s, edge_t = sums(edge[:, 0], edge[:, 1])
    edge_d = edge_t - FAR * jnp.concatenate([hc1[0, 0, 1][None], edge_s[:-1]], axis=0)
    xd1[0, 1, own1] = sums(e1[0, 1, own1], e1[1, 1, own1])[1]
    xd1[0, 1, PAD - 2 : PAD - 1] = edge_d[0]
    xd1[0, 1, PAD - 1 : PAD] = jnp.zeros((1, LANES), jnp.float32)
    _, edge_t = sums(xd1[1:hx, 1, PAD : PAD + 1], xd1[1:hx, 1, PAD + 1 : PAD + 2])
    row = jnp.sum(jnp.abs(edge_t - FAR * edge_d[1:]), axis=0)
    mine[...] = row + jnp.sum(magnitude + fold(jnp.abs(finest(0) - FAR * rx[0, 0])), axis=0, keepdims=True)
    landed = 0
    for k, d in enumerate(peers):
        landed += post(mine, rows_in.at[k], d[0], d[1], 4)

    land(recv.at[1], coarse1)
    edge, _ = sums(e1[cx - 2, 0, own1], e1[cx - 1, 0, own1])
    xs1[hx, 0, own1] = edge * (1.0 + FAR)
    shrunk(hx)
    s1s[hx, 0, own] = s1s[hx, 0, own] - rx[1, 1]
    edge = hy1[1, :, 0].reshape(hx, 2, 1, LANES)
    edge_s, edge_t = sums(edge[:, 0], edge[:, 1])
    after = jnp.concatenate([edge_t[1:], jnp.zeros_like(edge_t[:1])], axis=0)
    last_t = edge_s - (after - FAR * edge_s)
    last_s, _ = sums(xs1[1 : hx + 1, 0, top - 2 : top - 1], xs1[1 : hx + 1, 0, top - 1 : top])
    last_s = jnp.concatenate([last_s[:-1], last_s[-1:] - rx[1, 1, hy - 1 : hy][None]], axis=0)
    s1s[1 : hx + 1, 0, PAD + hy - 1 : PAD + hy] = last_s - (last_t - FAR * last_s)
    rows = jnp.concatenate(
        [s1s[1:hx, 0, PAD + done : PAD + hy].reshape((hx - 1) * PAD, LANES), s1s[hx, 0, own]],
        axis=0)
    got = times_folded(rows, w2)
    e2[0 : hx - 1, PAD + done : PAD + hy] = got[: (hx - 1) * PAD].reshape(hx - 1, PAD, LANES)
    e2[hx - 1, own] = got[(hx - 1) * PAD :]

    def pair2(m, rows):
        return sums(e2[2 * m, rows], e2[2 * m + 1, rows])

    def coarse2(m, rows):
        return pair2(m, rows)[0] * (1.0 + FAR) - pair2(m + 1, rows)[1]

    xl[0] = pair2(qx - 2, own)[0]
    xl[1] = e2[hx - 2, own]
    xl[2] = e2[hx - 1, own]
    xl[3] = sums(coarse2(qx - 4, own), coarse2(qx - 3, own))[0]
    xh[0] = pair2(0, own)[1]
    xh[1] = sums(coarse2(0, own), coarse2(1, own))[1]
    y_own, y_low, y_high = pl.ds(PAD, hy), pl.ds(0, PAD), pl.ds(PAD + hy, PAD)
    s_own, s_first, s_last = pl.ds(0, hy), pl.ds(0, PAD), pl.ds(hy - PAD, PAD)
    round2 = 0
    for rows_s, rows_d, dy in ((s_own, y_own, 0), (s_last, y_low, 1), (s_first, y_high, -1)):
        round2 += post(xl.at[:, rows_s, :], xlow.at[:, rows_d, :], 1, dy, 3)
        round2 += post(xh.at[:, rows_s, :], xhigh.at[:, rows_d, :], -1, dy, 3)
    round2 += post(e2.at[:, pl.ds(PAD, PAD), :], e2.at[:, y_high, :], 0, -1, 3)
    round2 += post(e2.at[:, pl.ds(hy, PAD), :], e2.at[:, y_low, :], 0, 1, 3)

    land(recv.at[2], later1)

    def place(ref, rows, side):
        if side == 0:
            ref[..., PAD - 2 : PAD - 1, :] = rows
            ref[..., PAD - 1 : PAD, :] = jnp.zeros_like(rows)
        else:
            ref[..., top : top + 1, :] = -ROOT3 * rows
            ref[..., top + 1 : top + 2, :] = rows

    corners = jnp.concatenate(
        [sc1[1, 1, 0], tc[0], tc[1], hc1[1, 1, 0], jnp.zeros((PAD - 4, LANES), jnp.float32)], axis=0)
    corners = times_folded(corners, w2)
    for i in range(4):
        at = PAD - 1 + hy * (i % 2)
        fix[i // 2, at : at + 1] = corners[i : i + 1]
    for x in range(2):
        detail, smooth = rx[x, 0], rx[x, 1]
        smooth = smooth + jnp.where(line < hy - 1, pltpu.roll(detail, hy - 1, 0), 0.0)
        part = detail + jnp.where(line > 0, FAR * pltpu.roll(smooth, 1, 0), 0.0)
        odd = part + NEAR * smooth
        hx1[x, 1 - x, pl.ds(PAD, hy, stride=2), :] = smooth - ROOT3 * odd
        hx1[x, 1 - x, pl.ds(PAD + 1, hy, stride=2), :] = odd
    for side in range(2):
        place(e1, hy1[side], side)
        for x in range(2):
            place(hx1.at[x], hc1[x, side], side)
    lift1(slice(PAD - 2, PAD))
    lift1(slice(top, top + 2))
    wide = slice(PAD - 2, top + 2)
    _, edge = pair1(0, wide)
    detail = edge - FAR * hx1[0, :, wide]
    xd1[0, :, wide] = detail
    xs1[0, :, wide] = hx1[0, :, wide] - detail
    edge, _ = pair1(hx - 1, wide)
    detail = hx1[1, :, wide] - FAR * edge
    xd1[hx, :, wide] = detail
    xs1[hx, :, wide] = edge - detail

    def cols1(src, det, smo):
        def step(n, carry):
            for h in range(2):
                load = lambda start: src[n, h, pl.ds(start, hy + 1, stride=2), :]
                s0, t0 = sums(load(PAD), load(PAD + 1))
                sm, _ = sums(load(PAD - 2), load(PAD - 1))
                d = t0 - FAR * sm
                det[n, h, 0 : hy + 1] = d
                smo[n, h, PAD - 1 : PAD + hy] = sm - d
            return carry

        lax.fori_loop(0, hx + 1, step, 0)

    cols1(xd1, d1d, d1s)
    cols1(xs1, s1d, s1s)

    land(recv.at[4], landed)
    acc = mine[...]
    for k in range(len(peers)):
        acc = acc + rows_in[k]
    level = spread(acc, count_all)
    noise[...] = jnp.broadcast_to(level, (PAD, LANES))
    far1, mid1, near1 = limits(level, 1)

    def put_into(dst, h):
        def put(n, rows):
            if h is None:
                dst[n] = rows
            else:
                dst[n, h] = rows
        return put

    def bands1(det, smo, h, limit_d, limit_s):
        def one_x(n):
            d = shrink(det[n, h], limit_d)
            return d, shrink(smo[n, h], limit_s) + d
        return one_x

    for h in range(2):
        inverse1(hx, bands1(d1d, s1d, h, far1, mid1), put_into(p1d, h))
    inverse1(hx, bands1(d1s, s1s, 1, mid1, near1), put_into(p1s1, None))

    land(recv.at[3], round2)
    every = slice(0, hy + 2 * PAD)
    before = xlow[0]
    xs2[0] = xlow[3]
    for m in range(-1, qx + 1):
        if m == qx:
            smooth, part = None, xhigh[0]
        elif m == -1:
            smooth, part = sums(xlow[1], xlow[2] + fix[0])
        elif m == qx - 1:
            smooth, part = sums(e2[hx - 2, every], e2[hx - 1, every] + fix[1])
        else:
            smooth, part = pair2(m, every)
        detail = part - FAR * before
        xd2[m + 1] = detail
        xs2[m + 2] = before - detail
        before = smooth
    xs2[qx + 3] = xhigh[1]
    pairs = hy // 2 + PAD

    def rows2(src):
        return forward_rows(src[:, pl.ds(0, pairs, stride=2), :],
                            src[:, pl.ds(1, pairs, stride=2), :])

    mid = slice(PAD // 2, PAD // 2 + pairs)
    dd[:, mid], ds[:, mid] = rows2(xd2)
    det, smo = rows2(xs2)
    sd[:, mid] = det[1 : qx + 3]
    ep3[:, mid] = smo

    n_own, n3, h3 = qx // 2, qx // 2 + 2, qy // 2 + PAD
    low_s, low_t = [ep3[0]], [None]
    for n in range(n_own + 1):
        s, t = sums(ep3[1 + 2 * n], ep3[2 + 2 * n])
        low_s.append(s)
        low_t.append(t)
    low_t.append(ep3[qx + 3])
    for n in range(n3):
        detail = low_t[n + 1] - FAR * low_s[n]
        t3d[n] = detail
        t3s[n] = low_s[n] - detail
    bands = []
    for src in (t3d, t3s):
        bands += forward_rows(src[:, pl.ds(0, h3, stride=2), :], src[:, pl.ds(1, h3, stride=2), :])
    for i, band in enumerate(bands):
        b3[i] = times_folded(band.reshape(n3 * h3, LANES), w3).reshape(n3, h3, LANES)

    land(send.at[0], sent[0])


def finish(shape, d1s, p1d, p1s1, dd, ds, sd, ep3, b3, total, v1, v2, v3, out,
           ss, r2, r1, s0, p1s0, o1, ob, osem):
    cx, cy, cz = shape
    hx, hy, qx, qy = cx // 2, cy // 2, cx // 4, cy // 4
    n3, h3, x2, yrows = qx // 2 + 2, qy // 2 + PAD, qx + 2, qy + 2 * PAD
    noise = total[0:1]


    far3, mid3, near3 = (v[None] for v in limits(noise, 3))
    lane3 = lax.broadcasted_iota(jnp.int32, (n3, h3, LANES), 2)
    b_dd, b_ds, b_sd = shrink(b3[0], far3), shrink(b3[1], mid3), shrink(b3[2], mid3)
    b_ss = jnp.where(lane3 < cz // 8, b3[3], shrink(b3[3], near3))

    def inverse_x(det, smo):
        one = smo + det
        even, odd = undo(det[:-1], one[1:], one[:-1])
        return weave(even, odd)

    y_d = inverse_x(b_dd, b_sd)
    y_s = inverse_x(b_ds, b_ss)
    one = y_s + pltpu.roll(y_d, h3 - 1, 1)
    even, odd = undo(y_d, one, pltpu.roll(one, 1, 1))
    r2[:, pl.ds(0, h3, stride=2), :] = even
    r2[:, pl.ds(1, h3, stride=2), :] = odd
    back = times_folded(r2[...].reshape(x2 * yrows, LANES), v3).reshape(x2, yrows, LANES)

    far2, mid2, near2 = limits(noise, 2)
    lane2 = lax.broadcasted_iota(jnp.int32, (x2, yrows, LANES), 2)
    ss[...] = jnp.where(lane2 < cz // 4, back, shrink(ep3[1 : qx + 3], near2[None]))

    def one_x(n):
        d_d = shrink(dd[n], far2)
        d_s = shrink(ds[n], mid2)
        s_d = shrink(sd[n], mid2)
        return d_d, d_s, s_d + d_d, ss[n] + d_s

    def inv2(n, carry):
        d_d, d_s, b_d, b_s = carry
        after = one_x(n + 1)
        pair_d = undo(d_d, after[2], b_d)
        pair_s = undo(d_s, after[3], b_s)
        for i in range(2):
            y_d, y_s = pair_d[i], pair_s[i]
            one = y_s + pltpu.roll(y_d, yrows - 1, 0)
            even, odd = undo(y_d, one, pltpu.roll(one, 1, 0))
            r1[2 * n + i, pl.ds(0, yrows, stride=2), :] = even
            r1[2 * n + i, pl.ds(1, yrows, stride=2), :] = odd
        return after

    lax.fori_loop(0, qx + 1, inv2, one_x(0), unroll=True)
    x1, y1 = hx + 2, hy + PAD
    back = times_folded(r1[:, PAD : PAD + y1].reshape(x1 * y1, LANES), v2).reshape(x1, y1, LANES)
    s0[...] = back[1:]
    _, mid1, _ = limits(noise, 1)

    def low_x(n):
        d = shrink(d1s[n, 0], mid1)
        return d, s0[n] + d

    def put_low(n, rows):
        p1s0[n] = rows

    inverse1(hx, low_x, put_low)

    def inv1_y(n):
        for h in range(2):
            y_d = p1d[n, h, 0:hy]
            y_n = p1d[n, h, 1 : hy + 1]
            p1s = p1s1 if h else p1s0
            s = p1s[n, PAD : PAD + hy]
            s_b = p1s[n, PAD - 1 : PAD - 1 + hy]
            even, odd = undo(y_d, s + y_n, s_b + y_d)
            o1[n, h, pl.ds(0, hy, stride=2), :] = even
            o1[n, h, pl.ds(1, hy, stride=2), :] = odd

    layers = 4
    outs = []
    for n in range(layers):
        inv1_y(n)
    for i in range(cx // layers):
        for n in range((i + 1) * layers, min((i + 2) * layers, cx)):
            inv1_y(n)
        xs = slice(i * layers, (i + 1) * layers)
        rows = jnp.concatenate(
            [o1[xs, h].reshape(layers * cy, LANES) for h in range(2)], axis=1)
        ob[xs] = times(rows, v1).reshape(layers, cy, cz)
        c = pltpu.make_async_copy(ob.at[xs], out.at[xs], osem.at[i])
        c.start()
        outs.append(c)
    for c in outs:
        c.wait()


def on_device(nx, ny, volume):
    cx, cy, cz = volume.shape
    hx, hy, qx, qy = cx // 2, cy // 2, cx // 4, cy // 4
    n3, h3 = qx // 2 + 2, qy // 2 + PAD
    f32 = jnp.float32
    count = cx * nx * cy * ny * cz // 8
    weights = [
        halves(forward_matrix(cz), cz), folded(forward_matrix(cz // 2)),
        folded(forward_matrix(cz // 4)), halves(inverse_matrix(cz), cz),
        folded(inverse_matrix(cz // 2)), folded(inverse_matrix(cz // 4)),
    ]
    vmem = lambda *s: pltpu.VMEM(s, f32)
    ey, ey2, ey3 = cy + 2 * PAD, hy + 2 * PAD, qy + 2 * PAD
    wide = lambda *s: pltpu.VMEM(s, jnp.bfloat16)
    pair = (2 * LANES, 2 * LANES)
    made = (
        vmem(hx + 1, 2, hy + PAD, LANES), vmem(cx, 2, hy + PAD, LANES),
        vmem(cx, hy + PAD, LANES), *[vmem(qx + 2, ey3, LANES) for _ in range(3)],
        vmem(qx + 4, ey3, LANES), vmem(4, n3, h3, LANES), vmem(PAD, LANES),
        wide(2, cz, cz), wide(*pair), wide(*pair),
    )
    rows = 4 * cy + 4 * cx + 10 + 6 * (hy + 2 * PAD) + 2 * hx * PAD + nx * ny
    scratch = [
        wide(2, cz, cz), wide(*pair), wide(*pair),
        *[vmem(hx + 1, 2, hy + PAD, LANES) for _ in range(3)],
        vmem(cx, 2, ey, LANES), vmem(2, 2, hy, LANES), vmem(2, 2, hy, LANES),
        vmem(2, 1, LANES), vmem(2, ey2, LANES),
        vmem(2, 2, ey, LANES), vmem(2, 2, cy, LANES),
        vmem(2, cx, 2, 1, LANES), vmem(2, cx, 2, 1, LANES),
        vmem(2, 2, 2, 1, LANES), vmem(2, 2, 2, 1, LANES),
        vmem(hx + 1, 2, ey, LANES), vmem(hx + 1, 2, ey, LANES),
        vmem(hx, ey2, LANES), vmem(4, hy, LANES), vmem(2, hy, LANES),
        vmem(4, ey2, LANES), vmem(2, ey2, LANES),
        vmem(qx + 2, ey2, LANES), vmem(qx + 4, ey2, LANES),
        vmem(n3, ey3, LANES), vmem(n3, ey3, LANES),
        vmem(1, LANES), vmem(nx * ny - 1, 1, LANES), vmem(max(rows, cz * cz // 32), 1, LANES),
        pltpu.SemaphoreType.DMA((1,)), pltpu.SemaphoreType.DMA((5,)),
        pltpu.SemaphoreType.DMA((2,)), pltpu.SemaphoreType.DMA((2,)),
    ]
    near = pl.BlockSpec(memory_space=pltpu.VMEM)
    passed = pl.pallas_call(
        functools.partial(kernel, (cx, cy, cz), count, nx, ny),
        out_shape=made,
        in_specs=[pl.BlockSpec(memory_space=pltpu.HBM)] * 7,
        out_specs=(near,) * len(made),
        scratch_shapes=scratch,
        compiler_params=pltpu.CompilerParams(
            collective_id=0, has_side_effects=True, vmem_limit_bytes=56 * 1024 * 1024),
    )(volume, *[jnp.asarray(w) for w in weights])
    return pl.pallas_call(
        functools.partial(finish, (cx, cy, cz)),
        out_shape=jax.ShapeDtypeStruct(volume.shape, f32),
        in_specs=[near] * len(made),
        out_specs=pl.BlockSpec(memory_space=pltpu.HBM),
        scratch_shapes=[
            vmem(qx + 2, ey3, LANES), vmem(qx + 2, ey3, LANES), vmem(hx + 2, 2 * ey3, LANES),
            vmem(hx + 1, hy + PAD, LANES),
            vmem(cx, hy + PAD, LANES), vmem(cx, 2, cy, LANES), vmem(cx, cy, cz), pltpu.SemaphoreType.DMA((cx // 4,)),
        ],
        compiler_params=pltpu.CompilerParams(vmem_limit_bytes=24 * 1024 * 1024),
    )(*passed)


def solution(mesh):
    spec = P("gx", "gy", None)
    body = functools.partial(on_device, mesh.shape["gx"], mesh.shape["gy"])
    return jax.shard_map(body, mesh=mesh, in_specs=(spec,), out_specs=spec, check_vma=False)
```

```python
import functools
import math

import jax
import jax.numpy as jnp
import numpy as np
from jax import lax
from jax.experimental import pallas as pl
from jax.experimental.pallas import tpu as pltpu
from jax.sharding import PartitionSpec as P

ROOT3 = math.sqrt(3.0)
NEAR = math.sqrt(3.0) / 4.0
FAR = (math.sqrt(3.0) - 2.0) / 4.0
LOW = (math.sqrt(3.0) - 1.0) / math.sqrt(2.0)
HIGH = (math.sqrt(3.0) + 1.0) / math.sqrt(2.0)
LANES = 128
PAD = 8


def forward_matrix(size):
    lines = np.eye(size)
    even, odd = lines[:, 0::2], lines[:, 1::2]
    smooth = even + ROOT3 * odd
    detail = odd - NEAR * smooth - FAR * np.roll(smooth, 1, 1)
    smooth = smooth - np.roll(detail, -1, 1)
    return np.concatenate([LOW * smooth, HIGH * detail], 1)


def inverse_matrix(size):
    lines = np.eye(size)
    smooth, detail = lines[:, : size // 2] / LOW, lines[:, size // 2 :] / HIGH
    first = smooth + np.roll(detail, -1, 1)
    odd = detail + NEAR * first + FAR * np.roll(first, 1, 1)
    even = first - ROOT3 * odd
    return np.stack([even, odd], 2).reshape(size, size)


def halves(matrix, size):
    full = np.zeros((size, size))
    full[: matrix.shape[0], : matrix.shape[1]] = matrix
    high = full.astype(jnp.bfloat16)
    low = (full - high.astype(np.float64)).astype(jnp.bfloat16)
    return np.stack([high, low])


def times(values, w_ref):
    high = values.astype(jnp.bfloat16)
    low = (values - high.astype(jnp.float32)).astype(jnp.bfloat16)
    dot = functools.partial(jnp.dot, preferred_element_type=jnp.float32)
    return dot(high, w_ref[0]) + (dot(low, w_ref[0]) + dot(high, w_ref[1]))


def folded(matrix):
    high, low = halves(matrix, LANES)
    return np.block([[high, low], [high, np.zeros_like(low)]])


def times_folded(values, w_ref):
    high = values.astype(jnp.bfloat16)
    low = (values - high.astype(jnp.float32)).astype(jnp.bfloat16)
    both = jnp.dot(jnp.concatenate([high, low], axis=1), w_ref[...],
                   preferred_element_type=jnp.float32)
    return both[:, :LANES] + both[:, LANES:]


def half_product(matrix, h):
    high, low = halves(matrix, len(matrix))
    mine = slice(h * LANES, (h + 1) * LANES)
    return np.concatenate([high[mine], high[mine], low[mine]], axis=0)


def times_half(values, w_ref):
    high = values.astype(jnp.bfloat16)
    low = (values - high.astype(jnp.float32)).astype(jnp.bfloat16)
    dot = functools.partial(jnp.dot, preferred_element_type=jnp.float32)
    return (dot(jnp.concatenate([high, low], axis=1), w_ref[: 2 * LANES])
            + dot(high, w_ref[2 * LANES :]))


def shrink(values, noise):
    return values - jnp.clip(values, -noise, noise)


def sums(even, odd):
    smooth = even + ROOT3 * odd
    return smooth, odd - NEAR * smooth


def undo(detail, first, before):
    odd = detail + NEAR * first + FAR * before
    return first - ROOT3 * odd, odd


def weave(even, odd):
    both = jnp.stack([even, odd], axis=1)
    return both.reshape((2 * even.shape[0],) + even.shape[1:])


def forward_rows(even, odd):
    axis = even.ndim - 2
    smooth, part = sums(even, odd)
    detail = part - FAR * pltpu.roll(smooth, 1, axis)
    return detail, smooth - pltpu.roll(detail, even.shape[axis] - 1, axis)


def limits(noise, level):
    base = noise * (1.0 / LOW ** (2 * (level - 1)))
    return base * (1.0 / (HIGH * HIGH)), base * (1.0 / (HIGH * LOW)), base * (1.0 / (LOW * LOW))


def spread(total, count_all):
    return jnp.sum(total, axis=(0, 1), keepdims=True) * (
        HIGH * HIGH * math.sqrt(math.pi / 2.0) / count_all)


def inverse1(hx, one_x, put):
    def step(n, carry):
        d, before = carry
        after, one = one_x(n + 1)
        even, odd = undo(d, one, before)
        put(2 * n, even)
        put(2 * n + 1, odd)
        return after, one

    lax.fori_loop(0, hx, step, one_x(0), unroll=4)


def inverse1_y(hy, det, smo, n, dst):
    y_d, y_n = det[n, 0:hy], det[n, 1 : hy + 1]
    even, odd = undo(
        y_d, smo[n, PAD : PAD + hy] + y_n, smo[n, PAD - 1 : PAD - 1 + hy] + y_d)
    dst[n, pl.ds(0, hy, stride=2), :] = even
    dst[n, pl.ds(1, hy, stride=2), :] = odd


def kernel(shape, count_all, nx, ny, vol, g1, g2, g3, g4, g5, g6, g7,
           d1s, p1d0, known1, dd, ds, sd, ep3, b3, noise, v1, v2, v3,
           w1, w2, w3, v4, p1d1, p1s1, o1, d1d, s1d, s1s,
           e1, lx, rx, tc, fix, hx1, sx1, hy1, sy1, hc1, sc1, xd1, xs1,
           e2, xl, xh, xlow, xhigh, xd2, xs2, t3d, t3s,
           mine, rows_in, dummy, send, recv, lsem, wsem):
    cx, cy, cz = shape
    hx, hy, qx, qy = cx // 2, cy // 2, cx // 4, cy // 4
    ix, iy = lax.axis_index("gx"), lax.axis_index("gy")

    def device(dx, dy):
        return (lax.rem(ix + dx + nx, nx), lax.rem(iy + dy + ny, ny))

    near = [(dx, dy) for dx in (-1, 0, 1) for dy in (-1, 0, 1) if dx or dy]
    peers = [(dx, dy) for dx in range(nx) for dy in range(ny) if dx or dy]
    taken = {(dx % nx, dy % ny) for dx, dy in near}
    barrier = pltpu.get_barrier_semaphore()

    def greet(dx, dy):
        pl.semaphore_signal(barrier, inc=1, device_id=device(dx, dy),
                            device_id_type=pl.DeviceIdType.MESH)

    for d in sorted(taken):
        greet(*d)
    loads = [
        pltpu.make_async_copy(
            vol.at[:, :, pl.ds(h * LANES, LANES)],
            e1.at[:, h, pl.ds(PAD, cy), :], lsem.at[h])
        for h in range(2)
    ]
    for c in loads:
        c.start()
    for d in peers:
        if d not in taken:
            greet(*d)
    first_weight = pltpu.make_async_copy(g1, w1, wsem.at[0])
    first_weight.start()
    more = list(zip((g2, g3, g4, g5, g6, g7), (w2, w3, v1, v2, v3, v4)))
    for src, dst in more:
        pltpu.make_async_copy(src, dst, wsem.at[1]).start()

    sent = [0]

    def post(src, dst, dx, dy, group):
        sent[0] += math.prod(src.shape) // LANES
        pltpu.make_async_remote_copy(
            src_ref=src, dst_ref=dst, send_sem=send.at[0], recv_sem=recv.at[group],
            device_id=device(dx, dy), device_id_type=pl.DeviceIdType.MESH).start()
        return math.prod(src.shape) // LANES

    def land(sem, rows):
        part = dummy.at[pl.ds(0, rows)]
        pltpu.make_async_copy(part, part, sem).wait()

    ep3[:, 0 : PAD // 2] = jnp.zeros((qx + 4, PAD // 2, LANES), jnp.float32)
    ep3[:, PAD // 2 + hy // 2 + PAD :] = jnp.zeros((qx + 4, PAD // 2, LANES), jnp.float32)
    fix[...] = jnp.zeros((2, hy + 2 * PAD, LANES), jnp.float32)
    for ref in (dd, ds, sd):
        ref[:, 0 : PAD // 2] = jnp.zeros((qx + 2, PAD // 2, LANES), jnp.float32)
        ref[:, PAD // 2 + hy // 2 + PAD :] = jnp.zeros((qx + 2, PAD // 2, LANES), jnp.float32)

    top = PAD + cy
    own1, own = slice(PAD, top), slice(PAD, PAD + hy)
    for c in loads:
        c.wait()
    first_weight.wait()

    def depth(xs, ys):
        shape = (xs.stop - xs.start, ys.stop - ys.start, LANES)
        rows = jnp.concatenate(
            [e1[xs, h, ys].reshape(shape[0] * shape[1], LANES) for h in range(2)], axis=1)
        got = times(rows, w1)
        for h in range(2):
            e1[xs, h, ys] = got[:, h * LANES : (h + 1) * LANES].reshape(shape)

    inner = slice(2 * PAD, top - PAD)
    depth(slice(0, cx), slice(PAD, 2 * PAD))
    depth(slice(0, cx), slice(top - PAD, top))
    depth(slice(0, 2), inner)
    depth(slice(cx - 2, cx), inner)
    sx1[1] = sums(e1[0, :, own1], e1[1, :, own1])[1]
    sx1[0] = sums(e1[cx - 2, :, own1], e1[cx - 1, :, own1])[0]
    sy1[1] = sums(e1[:, :, PAD : PAD + 1], e1[:, :, PAD + 1 : PAD + 2])[1]
    sy1[0] = sums(e1[:, :, top - 2 : top - 1], e1[:, :, top - 1 : top])[0]
    for x in range(2):
        sc1[x, 1] = sums(sx1[x, :, 0:1], sx1[x, :, 1:2])[1]
        sc1[x, 0] = sums(sx1[x, :, cy - 2 : cy - 1], sx1[x, :, cy - 1 : cy])[0]
    line = lax.broadcasted_iota(jnp.int32, (hy, LANES), 0)
    for x in range(2):
        load = lambda start: sx1[x, 1 - x, pl.ds(start, hy, stride=2), :]
        smooth, part = sums(load(0), load(1))
        detail = part - jnp.where(line > 0, FAR * pltpu.roll(smooth, 1, 0), 0.0)
        lx[x, 0] = detail
        lx[x, 1] = smooth - jnp.where(line < hy - 1, pltpu.roll(detail, hy - 1, 0), 0.0)
    pl.semaphore_wait(barrier, len(peers))
    step = (1, -1)
    post_x = lambda x, h, g: post(
        sx1.at[x, h], hx1.at[x, h, pl.ds(PAD, cy), :], step[x], 0, g)
    post_y = lambda y, h, g: post(sy1.at[y, :, h], hy1.at[y, :, h], 0, step[y], g)
    post_c = lambda x, y, h, g: post(
        sc1.at[x, y, h], hc1.at[x, y, h], step[x], step[y], g)
    post_l = lambda x, k, g: post(lx.at[x, k], rx.at[x, k], step[x], 0, g)
    noise1 = post_c(0, 0, 1, 0)
    coarse1 = post_l(1, 1, 1)
    noise1 += post_l(0, 0, 0) + post_y(0, 1, 0)
    coarse1 += post_y(1, 0, 1)
    later1 = (post_c(1, 1, 0, 2) + post(sc1.at[1, 1, 0], tc.at[0], 0, -1, 2)
              + post(sc1.at[1, 1, 0], tc.at[1], -1, 0, 2) + post_c(0, 0, 0, 2) + post_c(1, 1, 1, 2) + post_x(0, 0, 2) + post_x(1, 1, 2)
              + post_l(0, 1, 2) + post_l(1, 0, 2)
              + post_y(0, 0, 2) + post_y(1, 1, 2))
    for h in range(2):
        later1 += post_c(0, 1, h, 2) + post_c(1, 0, h, 2)

    slab = 4
    for lo in range(2, cx - 2, slab):
        depth(slice(lo, min(lo + slab, cx - 2)), inner)

    def pair1(n, rows=slice(None)):
        return sums(e1[2 * n, :, rows], e1[2 * n + 1, :, rows])

    def lift1(rows):
        def step(n, carry):
            _, part_n = pair1(n, rows)
            before, _ = pair1(n - 1, rows)
            detail = part_n - FAR * before
            xd1[n, :, rows] = detail
            xs1[n, :, rows] = before - detail
            return carry

        lax.fori_loop(1, hx, step, 0)

    def shrunk(n):
        load = lambda start: xs1[n, 0, pl.ds(start, hy, stride=2), :]
        s0, _ = sums(load(PAD), load(PAD + 1))
        _, tp = sums(load(PAD + 2), load(PAD + 3))
        s1s[n, 0, own] = s0 - (tp - FAR * s0)

    def finest(n):
        load = lambda start: xd1[n, 1, pl.ds(start, hy, stride=2), :]
        _, t0 = sums(load(PAD), load(PAD + 1))
        sm, _ = sums(load(PAD - 2), load(PAD - 1))
        return t0 - FAR * sm

    def fold(values):
        return jnp.sum(values.reshape(hy // PAD, PAD, LANES), axis=0)

    known = line > 0

    def inside(n, magnitude):
        shrunk(n)
        return magnitude + fold(jnp.where(known, jnp.abs(finest(n)), 0.0))

    lift1(own1)
    magnitude = lax.fori_loop(1, hx, inside, jnp.zeros((PAD, LANES), jnp.float32))
    land(wsem.at[1], sum(2 * math.prod(dst.shape) // (4 * LANES) for _, dst in more))
    done = hy - PAD
    rows = s1s[1:hx, 0, PAD : PAD + done].reshape((hx - 1) * done, LANES)
    e2[0 : hx - 1, PAD : PAD + done] = times_folded(rows, w2).reshape(hx - 1, done, LANES)

    land(recv.at[0], noise1)
    edge = hy1[0, :, 1].reshape(hx, 2, 1, LANES)
    edge_s, edge_t = sums(edge[:, 0], edge[:, 1])
    edge_d = edge_t - FAR * jnp.concatenate([hc1[0, 0, 1][None], edge_s[:-1]], axis=0)
    xd1[0, 1, own1] = sums(e1[0, 1, own1], e1[1, 1, own1])[1]
    xd1[0, 1, PAD - 2 : PAD - 1] = edge_d[0]
    xd1[0, 1, PAD - 1 : PAD] = jnp.zeros((1, LANES), jnp.float32)
    _, edge_t = sums(xd1[1:hx, 1, PAD : PAD + 1], xd1[1:hx, 1, PAD + 1 : PAD + 2])
    row = jnp.sum(jnp.abs(edge_t - FAR * edge_d[1:]), axis=0)
    mine[...] = row + jnp.sum(magnitude + fold(jnp.abs(finest(0) - FAR * rx[0, 0])), axis=0, keepdims=True)
    landed = 0
    for k, d in enumerate(peers):
        landed += post(mine, rows_in.at[k], d[0], d[1], 4)

    land(recv.at[1], coarse1)
    edge, _ = sums(e1[cx - 2, 0, own1], e1[cx - 1, 0, own1])
    xs1[hx, 0, own1] = edge * (1.0 + FAR)
    shrunk(hx)
    s1s[hx, 0, own] = s1s[hx, 0, own] - rx[1, 1]
    edge = hy1[1, :, 0].reshape(hx, 2, 1, LANES)
    edge_s, edge_t = sums(edge[:, 0], edge[:, 1])
    after = jnp.concatenate([edge_t[1:], jnp.zeros_like(edge_t[:1])], axis=0)
    last_t = edge_s - (after - FAR * edge_s)
    last_s, _ = sums(xs1[1 : hx + 1, 0, top - 2 : top - 1], xs1[1 : hx + 1, 0, top - 1 : top])
    last_s = jnp.concatenate([last_s[:-1], last_s[-1:] - rx[1, 1, hy - 1 : hy][None]], axis=0)
    s1s[1 : hx + 1, 0, PAD + hy - 1 : PAD + hy] = last_s - (last_t - FAR * last_s)
    rows = jnp.concatenate(
        [s1s[1:hx, 0, PAD + done : PAD + hy].reshape((hx - 1) * PAD, LANES), s1s[hx, 0, own]],
        axis=0)
    got = times_folded(rows, w2)
    e2[0 : hx - 1, PAD + done : PAD + hy] = got[: (hx - 1) * PAD].reshape(hx - 1, PAD, LANES)
    e2[hx - 1, own] = got[(hx - 1) * PAD :]

    def pair2(m, rows):
        return sums(e2[2 * m, rows], e2[2 * m + 1, rows])

    def coarse2(m, rows):
        return pair2(m, rows)[0] * (1.0 + FAR) - pair2(m + 1, rows)[1]

    xl[0] = pair2(qx - 2, own)[0]
    xl[1] = e2[hx - 2, own]
    xl[2] = e2[hx - 1, own]
    xl[3] = sums(coarse2(qx - 4, own), coarse2(qx - 3, own))[0]
    xh[0] = pair2(0, own)[1]
    xh[1] = sums(coarse2(0, own), coarse2(1, own))[1]
    y_own, y_low, y_high = pl.ds(PAD, hy), pl.ds(0, PAD), pl.ds(PAD + hy, PAD)
    s_own, s_first, s_last = pl.ds(0, hy), pl.ds(0, PAD), pl.ds(hy - PAD, PAD)
    round2 = 0
    for rows_s, rows_d, dy in ((s_own, y_own, 0), (s_last, y_low, 1), (s_first, y_high, -1)):
        round2 += post(xl.at[:, rows_s, :], xlow.at[:, rows_d, :], 1, dy, 3)
        round2 += post(xh.at[:, rows_s, :], xhigh.at[:, rows_d, :], -1, dy, 3)
    round2 += post(e2.at[:, pl.ds(PAD, PAD), :], e2.at[:, y_high, :], 0, -1, 3)
    round2 += post(e2.at[:, pl.ds(hy, PAD), :], e2.at[:, y_low, :], 0, 1, 3)

    land(recv.at[2], later1)

    def place(ref, rows, side):
        if side == 0:
            ref[..., PAD - 2 : PAD - 1, :] = rows
            ref[..., PAD - 1 : PAD, :] = jnp.zeros_like(rows)
        else:
            ref[..., top : top + 1, :] = -ROOT3 * rows
            ref[..., top + 1 : top + 2, :] = rows

    corners = jnp.concatenate(
        [sc1[1, 1, 0], tc[0], tc[1], hc1[1, 1, 0], jnp.zeros((PAD - 4, LANES), jnp.float32)], axis=0)
    corners = times_folded(corners, w2)
    for i in range(4):
        at = PAD - 1 + hy * (i % 2)
        fix[i // 2, at : at + 1] = corners[i : i + 1]
    for x in range(2):
        detail, smooth = rx[x, 0], rx[x, 1]
        smooth = smooth + jnp.where(line < hy - 1, pltpu.roll(detail, hy - 1, 0), 0.0)
        part = detail + jnp.where(line > 0, FAR * pltpu.roll(smooth, 1, 0), 0.0)
        odd = part + NEAR * smooth
        hx1[x, 1 - x, pl.ds(PAD, hy, stride=2), :] = smooth - ROOT3 * odd
        hx1[x, 1 - x, pl.ds(PAD + 1, hy, stride=2), :] = odd
    for side in range(2):
        place(e1, hy1[side], side)
        for x in range(2):
            place(hx1.at[x], hc1[x, side], side)
    lift1(slice(PAD - 2, PAD))
    lift1(slice(top, top + 2))
    wide = slice(PAD - 2, top + 2)
    _, edge = pair1(0, wide)
    detail = edge - FAR * hx1[0, :, wide]
    xd1[0, :, wide] = detail
    xs1[0, :, wide] = hx1[0, :, wide] - detail
    edge, _ = pair1(hx - 1, wide)
    detail = hx1[1, :, wide] - FAR * edge
    xd1[hx, :, wide] = detail
    xs1[hx, :, wide] = edge - detail

    def cols1(src, det, smo):
        def step(n, carry):
            for h in range(2):
                load = lambda start: src[n, h, pl.ds(start, hy + 1, stride=2), :]
                s0, t0 = sums(load(PAD), load(PAD + 1))
                sm, _ = sums(load(PAD - 2), load(PAD - 1))
                d = t0 - FAR * sm
                det[n, h, 0 : hy + 1] = d
                smo[n, h, PAD - 1 : PAD + hy] = sm - d
            return carry

        lax.fori_loop(0, hx + 1, step, 0)

    cols1(xd1, d1d, d1s)
    cols1(xs1, s1d, s1s)

    land(recv.at[4], landed)
    acc = mine[...]
    for k in range(len(peers)):
        acc = acc + rows_in[k]
    level = spread(acc, count_all)
    noise[...] = jnp.broadcast_to(level, (PAD, LANES))
    far1, mid1, near1 = limits(level, 1)

    def put_into(dst):
        def put(n, rows):
            dst[n] = rows
        return put

    def bands1(det, smo, h, limit_d, limit_s):
        def one_x(n):
            d = shrink(det[n, h], limit_d)
            return d, shrink(smo[n, h], limit_s) + d
        return one_x

    inverse1(hx, bands1(d1d, s1d, 1, far1, mid1), put_into(p1d1))
    inverse1(hx, bands1(d1s, s1s, 1, mid1, near1), put_into(p1s1))
    inverse1(hx, bands1(d1d, s1d, 0, far1, mid1), put_into(p1d0))
    layers = 4
    for n in range(layers):
        inverse1_y(hy, p1d1, p1s1, n, o1)
    for lo in range(0, cx, layers):
        for n in range(lo + layers, min(lo + 2 * layers, cx)):
            inverse1_y(hy, p1d1, p1s1, n, o1)
        rows = o1[lo : lo + layers].reshape(layers * cy, LANES)
        known1[lo : lo + layers] = times_half(rows, v4).reshape(layers, cy, cz)

    land(recv.at[3], round2)
    every = slice(0, hy + 2 * PAD)
    before = xlow[0]
    xs2[0] = xlow[3]
    for m in range(-1, qx + 1):
        if m == qx:
            smooth, part = None, xhigh[0]
        elif m == -1:
            smooth, part = sums(xlow[1], xlow[2] + fix[0])
        elif m == qx - 1:
            smooth, part = sums(e2[hx - 2, every], e2[hx - 1, every] + fix[1])
        else:
            smooth, part = pair2(m, every)
        detail = part - FAR * before
        xd2[m + 1] = detail
        xs2[m + 2] = before - detail
        before = smooth
    xs2[qx + 3] = xhigh[1]
    pairs = hy // 2 + PAD

    def rows2(src):
        return forward_rows(src[:, pl.ds(0, pairs, stride=2), :],
                            src[:, pl.ds(1, pairs, stride=2), :])

    mid = slice(PAD // 2, PAD // 2 + pairs)
    dd[:, mid], ds[:, mid] = rows2(xd2)
    det, smo = rows2(xs2)
    sd[:, mid] = det[1 : qx + 3]
    ep3[:, mid] = smo

    n_own, n3, h3 = qx // 2, qx // 2 + 2, qy // 2 + PAD
    low_s, low_t = [ep3[0]], [None]
    for n in range(n_own + 1):
        s, t = sums(ep3[1 + 2 * n], ep3[2 + 2 * n])
        low_s.append(s)
        low_t.append(t)
    low_t.append(ep3[qx + 3])
    for n in range(n3):
        detail = low_t[n + 1] - FAR * low_s[n]
        t3d[n] = detail
        t3s[n] = low_s[n] - detail
    bands = []
    for src in (t3d, t3s):
        bands += forward_rows(src[:, pl.ds(0, h3, stride=2), :], src[:, pl.ds(1, h3, stride=2), :])
    for i, band in enumerate(bands):
        b3[i] = times_folded(band.reshape(n3 * h3, LANES), w3).reshape(n3, h3, LANES)

    land(send.at[0], sent[0])


def finish(shape, d1s, p1d0, known1, dd, ds, sd, ep3, b3, total, v1, v2, v3, out,
           ss, r2, r1, s0, p1s0, o1, ob, osem):
    cx, cy, cz = shape
    hx, hy, qx, qy = cx // 2, cy // 2, cx // 4, cy // 4
    n3, h3, x2, yrows = qx // 2 + 2, qy // 2 + PAD, qx + 2, qy + 2 * PAD
    noise = total[0:1]


    far3, mid3, near3 = (v[None] for v in limits(noise, 3))
    lane3 = lax.broadcasted_iota(jnp.int32, (n3, h3, LANES), 2)
    b_dd, b_ds, b_sd = shrink(b3[0], far3), shrink(b3[1], mid3), shrink(b3[2], mid3)
    b_ss = jnp.where(lane3 < cz // 8, b3[3], shrink(b3[3], near3))

    def inverse_x(det, smo):
        one = smo + det
        even, odd = undo(det[:-1], one[1:], one[:-1])
        return weave(even, odd)

    y_d = inverse_x(b_dd, b_sd)
    y_s = inverse_x(b_ds, b_ss)
    one = y_s + pltpu.roll(y_d, h3 - 1, 1)
    even, odd = undo(y_d, one, pltpu.roll(one, 1, 1))
    r2[:, pl.ds(0, h3, stride=2), :] = even
    r2[:, pl.ds(1, h3, stride=2), :] = odd
    back = times_folded(r2[...].reshape(x2 * yrows, LANES), v3).reshape(x2, yrows, LANES)

    far2, mid2, near2 = limits(noise, 2)
    lane2 = lax.broadcasted_iota(jnp.int32, (x2, yrows, LANES), 2)
    ss[...] = jnp.where(lane2 < cz // 4, back, shrink(ep3[1 : qx + 3], near2[None]))

    def one_x(n):
        d_d = shrink(dd[n], far2)
        d_s = shrink(ds[n], mid2)
        s_d = shrink(sd[n], mid2)
        return d_d, d_s, s_d + d_d, ss[n] + d_s

    def inv2(n, carry):
        d_d, d_s, b_d, b_s = carry
        after = one_x(n + 1)
        pair_d = undo(d_d, after[2], b_d)
        pair_s = undo(d_s, after[3], b_s)
        for i in range(2):
            y_d, y_s = pair_d[i], pair_s[i]
            one = y_s + pltpu.roll(y_d, yrows - 1, 0)
            even, odd = undo(y_d, one, pltpu.roll(one, 1, 0))
            r1[2 * n + i, pl.ds(0, yrows, stride=2), :] = even
            r1[2 * n + i, pl.ds(1, yrows, stride=2), :] = odd
        return after

    lax.fori_loop(0, qx + 1, inv2, one_x(0), unroll=True)
    x1, y1 = hx + 2, hy + PAD
    back = times_folded(r1[:, PAD : PAD + y1].reshape(x1 * y1, LANES), v2).reshape(x1, y1, LANES)
    s0[...] = back[1:]
    _, mid1, _ = limits(noise, 1)

    def low_x(n):
        d = shrink(d1s[n, 0], mid1)
        return d, s0[n] + d

    def put_low(n, rows):
        p1s0[n] = rows

    inverse1(hx, low_x, put_low)

    layers = 4
    outs = []
    for n in range(layers):
        inverse1_y(hy, p1d0, p1s0, n, o1)
    for i in range(cx // layers):
        for n in range((i + 1) * layers, min((i + 2) * layers, cx)):
            inverse1_y(hy, p1d0, p1s0, n, o1)
        xs = slice(i * layers, (i + 1) * layers)
        rows = o1[xs].reshape(layers * cy, LANES)
        ob[xs] = known1[xs] + times_half(rows, v1).reshape(layers, cy, cz)
        c = pltpu.make_async_copy(ob.at[xs], out.at[xs], osem.at[i])
        c.start()
        outs.append(c)
    for c in outs:
        c.wait()


def on_device(nx, ny, volume):
    cx, cy, cz = volume.shape
    hx, hy, qx, qy = cx // 2, cy // 2, cx // 4, cy // 4
    n3, h3 = qx // 2 + 2, qy // 2 + PAD
    f32 = jnp.float32
    count = cx * nx * cy * ny * cz // 8
    weights = [
        halves(forward_matrix(cz), cz), folded(forward_matrix(cz // 2)),
        folded(forward_matrix(cz // 4)), half_product(inverse_matrix(cz), 0),
        folded(inverse_matrix(cz // 2)), folded(inverse_matrix(cz // 4)),
        half_product(inverse_matrix(cz), 1),
    ]
    vmem = lambda *s: pltpu.VMEM(s, f32)
    ey, ey2, ey3 = cy + 2 * PAD, hy + 2 * PAD, qy + 2 * PAD
    wide = lambda *s: pltpu.VMEM(s, jnp.bfloat16)
    pair = (2 * LANES, 2 * LANES)
    made = (
        vmem(hx + 1, 2, hy + PAD, LANES), vmem(cx, hy + PAD, LANES), vmem(cx, cy, cz), *[vmem(qx + 2, ey3, LANES) for _ in range(3)],
        vmem(qx + 4, ey3, LANES), vmem(4, n3, h3, LANES), vmem(PAD, LANES),
        wide(3 * LANES, cz), wide(*pair), wide(*pair),
    )
    rows = 4 * cy + 4 * cx + 10 + 6 * (hy + 2 * PAD) + 2 * hx * PAD + nx * ny
    scratch = [
        wide(2, cz, cz), wide(*pair), wide(*pair), wide(3 * LANES, cz),
        vmem(cx, hy + PAD, LANES), vmem(cx, hy + PAD, LANES), vmem(cx, cy, LANES),
        *[vmem(hx + 1, 2, hy + PAD, LANES) for _ in range(3)],
        vmem(cx, 2, ey, LANES), vmem(2, 2, hy, LANES), vmem(2, 2, hy, LANES),
        vmem(2, 1, LANES), vmem(2, ey2, LANES),
        vmem(2, 2, ey, LANES), vmem(2, 2, cy, LANES),
        vmem(2, cx, 2, 1, LANES), vmem(2, cx, 2, 1, LANES),
        vmem(2, 2, 2, 1, LANES), vmem(2, 2, 2, 1, LANES),
        vmem(hx + 1, 2, ey, LANES), vmem(hx + 1, 2, ey, LANES),
        vmem(hx, ey2, LANES), vmem(4, hy, LANES), vmem(2, hy, LANES),
        vmem(4, ey2, LANES), vmem(2, ey2, LANES),
        vmem(qx + 2, ey2, LANES), vmem(qx + 4, ey2, LANES),
        vmem(n3, ey3, LANES), vmem(n3, ey3, LANES),
        vmem(1, LANES), vmem(nx * ny - 1, 1, LANES), vmem(max(rows, cz * cz // 32), 1, LANES),
        pltpu.SemaphoreType.DMA((1,)), pltpu.SemaphoreType.DMA((5,)),
        pltpu.SemaphoreType.DMA((2,)), pltpu.SemaphoreType.DMA((2,)),
    ]
    near = pl.BlockSpec(memory_space=pltpu.VMEM)
    passed = pl.pallas_call(
        functools.partial(kernel, (cx, cy, cz), count, nx, ny),
        out_shape=made,
        in_specs=[pl.BlockSpec(memory_space=pltpu.HBM)] * 8,
        out_specs=(near,) * len(made),
        scratch_shapes=scratch,
        compiler_params=pltpu.CompilerParams(
            collective_id=0, has_side_effects=True, vmem_limit_bytes=56 * 1024 * 1024),
    )(volume, *[jnp.asarray(w) for w in weights])
    return pl.pallas_call(
        functools.partial(finish, (cx, cy, cz)),
        out_shape=jax.ShapeDtypeStruct(volume.shape, f32),
        in_specs=[near] * len(made),
        out_specs=pl.BlockSpec(memory_space=pltpu.HBM),
        scratch_shapes=[
            vmem(qx + 2, ey3, LANES), vmem(qx + 2, ey3, LANES), vmem(hx + 2, 2 * ey3, LANES),
            vmem(hx + 1, hy + PAD, LANES),
            vmem(cx, hy + PAD, LANES), vmem(cx, cy, LANES), vmem(cx, cy, cz), pltpu.SemaphoreType.DMA((cx // 4,)),
        ],
        compiler_params=pltpu.CompilerParams(vmem_limit_bytes=24 * 1024 * 1024),
    )(*passed)


def solution(mesh):
    spec = P("gx", "gy", None)
    body = functools.partial(on_device, mesh.shape["gx"], mesh.shape["gy"])
    return jax.shard_map(body, mesh=mesh, in_specs=(spec,), out_specs=spec, check_vma=False)
```

```python
import functools
import math

import jax
import jax.numpy as jnp
import numpy as np
from jax import lax
from jax.experimental import pallas as pl
from jax.experimental.pallas import tpu as pltpu
from jax.sharding import PartitionSpec as P

ROOT3 = math.sqrt(3.0)
NEAR = math.sqrt(3.0) / 4.0
FAR = (math.sqrt(3.0) - 2.0) / 4.0
LOW = (math.sqrt(3.0) - 1.0) / math.sqrt(2.0)
HIGH = (math.sqrt(3.0) + 1.0) / math.sqrt(2.0)
LANES = 128
PAD = 8


def forward_matrix(size):
    lines = np.eye(size)
    even, odd = lines[:, 0::2], lines[:, 1::2]
    smooth = even + ROOT3 * odd
    detail = odd - NEAR * smooth - FAR * np.roll(smooth, 1, 1)
    smooth = smooth - np.roll(detail, -1, 1)
    return np.concatenate([LOW * smooth, HIGH * detail], 1)


def inverse_matrix(size):
    lines = np.eye(size)
    smooth, detail = lines[:, : size // 2] / LOW, lines[:, size // 2 :] / HIGH
    first = smooth + np.roll(detail, -1, 1)
    odd = detail + NEAR * first + FAR * np.roll(first, 1, 1)
    even = first - ROOT3 * odd
    return np.stack([even, odd], 2).reshape(size, size)


def halves(matrix, size):
    full = np.zeros((size, size))
    full[: matrix.shape[0], : matrix.shape[1]] = matrix
    high = full.astype(jnp.bfloat16)
    low = (full - high.astype(np.float64)).astype(jnp.bfloat16)
    return np.stack([high, low])


def times(values, w_ref):
    high = values.astype(jnp.bfloat16)
    low = (values - high.astype(jnp.float32)).astype(jnp.bfloat16)
    dot = functools.partial(jnp.dot, preferred_element_type=jnp.float32)
    return dot(high, w_ref[0]) + (dot(low, w_ref[0]) + dot(high, w_ref[1]))


def folded(matrix):
    high, low = halves(matrix, LANES)
    return np.block([[high, low], [high, np.zeros_like(low)]])


def times_folded(values, w_ref):
    high = values.astype(jnp.bfloat16)
    low = (values - high.astype(jnp.float32)).astype(jnp.bfloat16)
    both = jnp.dot(jnp.concatenate([high, low], axis=1), w_ref[...],
                   preferred_element_type=jnp.float32)
    return both[:, :LANES] + both[:, LANES:]


def half_product(matrix, h):
    high, low = halves(matrix, len(matrix))
    mine = slice(h * LANES, (h + 1) * LANES)
    return np.concatenate([high[mine], high[mine], low[mine]], axis=0)


def times_half(values, w_ref):
    high = values.astype(jnp.bfloat16)
    low = (values - high.astype(jnp.float32)).astype(jnp.bfloat16)
    dot = functools.partial(jnp.dot, preferred_element_type=jnp.float32)
    return (dot(jnp.concatenate([high, low], axis=1), w_ref[: 2 * LANES])
            + dot(high, w_ref[2 * LANES :]))


def shrink(values, noise):
    return values - jnp.clip(values, -noise, noise)


def sums(even, odd):
    smooth = even + ROOT3 * odd
    return smooth, odd - NEAR * smooth


def undo(detail, first, before):
    odd = detail + NEAR * first + FAR * before
    return first - ROOT3 * odd, odd


def weave(even, odd):
    both = jnp.stack([even, odd], axis=1)
    return both.reshape((2 * even.shape[0],) + even.shape[1:])


def forward_rows(even, odd):
    axis = even.ndim - 2
    smooth, part = sums(even, odd)
    detail = part - FAR * pltpu.roll(smooth, 1, axis)
    return detail, smooth - pltpu.roll(detail, even.shape[axis] - 1, axis)


def limits(noise, level):
    base = noise * (1.0 / LOW ** (2 * (level - 1)))
    return base * (1.0 / (HIGH * HIGH)), base * (1.0 / (HIGH * LOW)), base * (1.0 / (LOW * LOW))


def spread(total, count_all):
    return jnp.sum(total, axis=(0, 1), keepdims=True) * (
        HIGH * HIGH * math.sqrt(math.pi / 2.0) / count_all)


def inverse1(hx, one_x, put, unroll=4):
    def step(n, carry):
        d, before = carry
        after, one = one_x(n + 1)
        even, odd = undo(d, one, before)
        put(2 * n, even)
        put(2 * n + 1, odd)
        return after, one

    lax.fori_loop(0, hx, step, one_x(0), unroll=unroll)


def inverse1_y(hy, det, smo, n, dst):
    y_d, y_n = det[n, 0:hy], det[n, 1 : hy + 1]
    even, odd = undo(
        y_d, smo[n, PAD : PAD + hy] + y_n, smo[n, PAD - 1 : PAD - 1 + hy] + y_d)
    dst[n, pl.ds(0, hy, stride=2), :] = even
    dst[n, pl.ds(1, hy, stride=2), :] = odd


def kernel(shape, count_all, nx, ny, vol, g1, g2, g3, g4, g5, g6, g7,
           d1s, p1d0, known1, dd, ds, sd, ep3, b3, noise, v1, v2, v3,
           w1, w2, w3, v4, p1d1, p1s1, o1, d1d, s1d, s1s,
           e1, lx, rx, tc, fix, hx1, sx1, hy1, sy1, hc1, sc1, xd1, xs1,
           e2, xl, xh, xlow, xhigh, xd2, xs2, t3d, t3s,
           mine, rows_in, dummy, send, recv, lsem, wsem):
    cx, cy, cz = shape
    hx, hy, qx, qy = cx // 2, cy // 2, cx // 4, cy // 4
    ix, iy = lax.axis_index("gx"), lax.axis_index("gy")

    def device(dx, dy):
        return (lax.rem(ix + dx + nx, nx), lax.rem(iy + dy + ny, ny))

    near = [(dx, dy) for dx in (-1, 0, 1) for dy in (-1, 0, 1) if dx or dy]
    peers = [(dx, dy) for dx in range(nx) for dy in range(ny) if dx or dy]
    taken = {(dx % nx, dy % ny) for dx, dy in near}
    barrier = pltpu.get_barrier_semaphore()

    def greet(dx, dy):
        pl.semaphore_signal(barrier, inc=1, device_id=device(dx, dy),
                            device_id_type=pl.DeviceIdType.MESH)

    for d in sorted(taken):
        greet(*d)
    loads = [
        pltpu.make_async_copy(
            vol.at[:, :, pl.ds(h * LANES, LANES)],
            e1.at[:, h, pl.ds(PAD, cy), :], lsem.at[h])
        for h in range(2)
    ]
    for c in loads:
        c.start()
    for d in peers:
        if d not in taken:
            greet(*d)
    first_weight = pltpu.make_async_copy(g1, w1, wsem.at[0])
    first_weight.start()
    more = list(zip((g2, g3, g4, g5, g6, g7), (w2, w3, v1, v2, v3, v4)))
    for src, dst in more:
        pltpu.make_async_copy(src, dst, wsem.at[1]).start()

    sent = [0]

    def post(src, dst, dx, dy, group):
        sent[0] += math.prod(src.shape) // LANES
        pltpu.make_async_remote_copy(
            src_ref=src, dst_ref=dst, send_sem=send.at[0], recv_sem=recv.at[group],
            device_id=device(dx, dy), device_id_type=pl.DeviceIdType.MESH).start()
        return math.prod(src.shape) // LANES

    def land(sem, rows):
        part = dummy.at[pl.ds(0, rows)]
        pltpu.make_async_copy(part, part, sem).wait()

    ep3[:, 0 : PAD // 2] = jnp.zeros((qx + 4, PAD // 2, LANES), jnp.float32)
    ep3[:, PAD // 2 + hy // 2 + PAD :] = jnp.zeros((qx + 4, PAD // 2, LANES), jnp.float32)
    fix[...] = jnp.zeros((2, hy + 2 * PAD, LANES), jnp.float32)
    for ref in (dd, ds, sd):
        ref[:, 0 : PAD // 2] = jnp.zeros((qx + 2, PAD // 2, LANES), jnp.float32)
        ref[:, PAD // 2 + hy // 2 + PAD :] = jnp.zeros((qx + 2, PAD // 2, LANES), jnp.float32)

    top = PAD + cy
    own1, own = slice(PAD, top), slice(PAD, PAD + hy)
    for c in loads:
        c.wait()
    first_weight.wait()

    def depth(xs, ys):
        shape = (xs.stop - xs.start, ys.stop - ys.start, LANES)
        rows = jnp.concatenate(
            [e1[xs, h, ys].reshape(shape[0] * shape[1], LANES) for h in range(2)], axis=1)
        got = times(rows, w1)
        for h in range(2):
            e1[xs, h, ys] = got[:, h * LANES : (h + 1) * LANES].reshape(shape)

    inner = slice(2 * PAD, top - PAD)
    depth(slice(0, cx), slice(PAD, 2 * PAD))
    depth(slice(0, cx), slice(top - PAD, top))
    depth(slice(0, 2), inner)
    depth(slice(cx - 2, cx), inner)
    sx1[1] = sums(e1[0, :, own1], e1[1, :, own1])[1]
    sx1[0] = sums(e1[cx - 2, :, own1], e1[cx - 1, :, own1])[0]
    sy1[1] = sums(e1[:, :, PAD : PAD + 1], e1[:, :, PAD + 1 : PAD + 2])[1]
    sy1[0] = sums(e1[:, :, top - 2 : top - 1], e1[:, :, top - 1 : top])[0]
    for x in range(2):
        sc1[x, 1] = sums(sx1[x, :, 0:1], sx1[x, :, 1:2])[1]
        sc1[x, 0] = sums(sx1[x, :, cy - 2 : cy - 1], sx1[x, :, cy - 1 : cy])[0]
    line = lax.broadcasted_iota(jnp.int32, (hy, LANES), 0)
    for x in range(2):
        load = lambda start: sx1[x, 1 - x, pl.ds(start, hy, stride=2), :]
        smooth, part = sums(load(0), load(1))
        detail = part - jnp.where(line > 0, FAR * pltpu.roll(smooth, 1, 0), 0.0)
        lx[x, 0] = detail
        lx[x, 1] = smooth - jnp.where(line < hy - 1, pltpu.roll(detail, hy - 1, 0), 0.0)
    pl.semaphore_wait(barrier, len(peers))
    step = (1, -1)
    post_x = lambda x, h, g: post(
        sx1.at[x, h], hx1.at[x, h, pl.ds(PAD, cy), :], step[x], 0, g)
    post_y = lambda y, h, g: post(sy1.at[y, :, h], hy1.at[y, :, h], 0, step[y], g)
    post_c = lambda x, y, h, g: post(
        sc1.at[x, y, h], hc1.at[x, y, h], step[x], step[y], g)
    post_l = lambda x, k, g: post(lx.at[x, k], rx.at[x, k], step[x], 0, g)
    noise1 = post_c(0, 0, 1, 0)
    coarse1 = post_l(1, 1, 1)
    noise1 += post_l(0, 0, 0) + post_y(0, 1, 0)
    coarse1 += post_y(1, 0, 1)
    later1 = (post_c(1, 1, 0, 2) + post(sc1.at[1, 1, 0], tc.at[0], 0, -1, 2)
              + post(sc1.at[1, 1, 0], tc.at[1], -1, 0, 2) + post_c(0, 0, 0, 2) + post_c(1, 1, 1, 2) + post_x(0, 0, 2) + post_x(1, 1, 2)
              + post_l(0, 1, 2) + post_l(1, 0, 2)
              + post_y(0, 0, 2) + post_y(1, 1, 2))
    for h in range(2):
        later1 += post_c(0, 1, h, 2) + post_c(1, 0, h, 2)

    slab = 4
    for lo in range(2, cx - 2, slab):
        depth(slice(lo, min(lo + slab, cx - 2)), inner)

    def pair1(n, rows=slice(None)):
        return sums(e1[2 * n, :, rows], e1[2 * n + 1, :, rows])

    def lift1(rows):
        def step(n, carry):
            _, part_n = pair1(n, rows)
            before, _ = pair1(n - 1, rows)
            detail = part_n - FAR * before
            xd1[n, :, rows] = detail
            xs1[n, :, rows] = before - detail
            return carry

        lax.fori_loop(1, hx, step, 0)

    def shrunk(n):
        load = lambda start: xs1[n, 0, pl.ds(start, hy, stride=2), :]
        s0, _ = sums(load(PAD), load(PAD + 1))
        _, tp = sums(load(PAD + 2), load(PAD + 3))
        s1s[n, 0, own] = s0 - (tp - FAR * s0)

    def finest(n):
        load = lambda start: xd1[n, 1, pl.ds(start, hy, stride=2), :]
        _, t0 = sums(load(PAD), load(PAD + 1))
        sm, _ = sums(load(PAD - 2), load(PAD - 1))
        return t0 - FAR * sm

    def fold(values):
        return jnp.sum(values.reshape(hy // PAD, PAD, LANES), axis=0)

    known = line > 0

    def inside(n, magnitude):
        shrunk(n)
        return magnitude + fold(jnp.where(known, jnp.abs(finest(n)), 0.0))

    lift1(own1)
    magnitude = lax.fori_loop(1, hx, inside, jnp.zeros((PAD, LANES), jnp.float32))
    land(wsem.at[1], sum(2 * math.prod(dst.shape) // (4 * LANES) for _, dst in more))
    done = hy - PAD
    rows = s1s[1:hx, 0, PAD : PAD + done].reshape((hx - 1) * done, LANES)
    e2[0 : hx - 1, PAD : PAD + done] = times_folded(rows, w2).reshape(hx - 1, done, LANES)

    land(recv.at[0], noise1)
    edge = hy1[0, :, 1].reshape(hx, 2, 1, LANES)
    edge_s, edge_t = sums(edge[:, 0], edge[:, 1])
    edge_d = edge_t - FAR * jnp.concatenate([hc1[0, 0, 1][None], edge_s[:-1]], axis=0)
    xd1[0, 1, own1] = sums(e1[0, 1, own1], e1[1, 1, own1])[1]
    xd1[0, 1, PAD - 2 : PAD - 1] = edge_d[0]
    xd1[0, 1, PAD - 1 : PAD] = jnp.zeros((1, LANES), jnp.float32)
    _, edge_t = sums(xd1[1:hx, 1, PAD : PAD + 1], xd1[1:hx, 1, PAD + 1 : PAD + 2])
    row = jnp.sum(jnp.abs(edge_t - FAR * edge_d[1:]), axis=0)
    mine[...] = row + jnp.sum(magnitude + fold(jnp.abs(finest(0) - FAR * rx[0, 0])), axis=0, keepdims=True)
    landed = 0
    for k, d in enumerate(peers):
        landed += post(mine, rows_in.at[k], d[0], d[1], 4)

    land(recv.at[1], coarse1)
    edge, _ = sums(e1[cx - 2, 0, own1], e1[cx - 1, 0, own1])
    xs1[hx, 0, own1] = edge * (1.0 + FAR)
    shrunk(hx)
    s1s[hx, 0, own] = s1s[hx, 0, own] - rx[1, 1]
    edge = hy1[1, :, 0].reshape(hx, 2, 1, LANES)
    edge_s, edge_t = sums(edge[:, 0], edge[:, 1])
    after = jnp.concatenate([edge_t[1:], jnp.zeros_like(edge_t[:1])], axis=0)
    last_t = edge_s - (after - FAR * edge_s)
    last_s, _ = sums(xs1[1 : hx + 1, 0, top - 2 : top - 1], xs1[1 : hx + 1, 0, top - 1 : top])
    last_s = jnp.concatenate([last_s[:-1], last_s[-1:] - rx[1, 1, hy - 1 : hy][None]], axis=0)
    s1s[1 : hx + 1, 0, PAD + hy - 1 : PAD + hy] = last_s - (last_t - FAR * last_s)
    rows = jnp.concatenate(
        [s1s[1:hx, 0, PAD + done : PAD + hy].reshape((hx - 1) * PAD, LANES), s1s[hx, 0, own]],
        axis=0)
    got = times_folded(rows, w2)
    e2[0 : hx - 1, PAD + done : PAD + hy] = got[: (hx - 1) * PAD].reshape(hx - 1, PAD, LANES)
    e2[hx - 1, own] = got[(hx - 1) * PAD :]

    def pair2(m, rows):
        return sums(e2[2 * m, rows], e2[2 * m + 1, rows])

    def coarse2(m, rows):
        return pair2(m, rows)[0] * (1.0 + FAR) - pair2(m + 1, rows)[1]

    xl[0] = pair2(qx - 2, own)[0]
    xl[1] = e2[hx - 2, own]
    xl[2] = e2[hx - 1, own]
    xl[3] = sums(coarse2(qx - 4, own), coarse2(qx - 3, own))[0]
    xh[0] = pair2(0, own)[1]
    xh[1] = sums(coarse2(0, own), coarse2(1, own))[1]
    y_own, y_low, y_high = pl.ds(PAD, hy), pl.ds(0, PAD), pl.ds(PAD + hy, PAD)
    s_own, s_first, s_last = pl.ds(0, hy), pl.ds(0, PAD), pl.ds(hy - PAD, PAD)
    round2 = 0
    for rows_s, rows_d, dy in ((s_own, y_own, 0), (s_last, y_low, 1), (s_first, y_high, -1)):
        round2 += post(xl.at[:, rows_s, :], xlow.at[:, rows_d, :], 1, dy, 3)
        round2 += post(xh.at[:, rows_s, :], xhigh.at[:, rows_d, :], -1, dy, 3)
    round2 += post(e2.at[:, pl.ds(PAD, PAD), :], e2.at[:, y_high, :], 0, -1, 3)
    round2 += post(e2.at[:, pl.ds(hy, PAD), :], e2.at[:, y_low, :], 0, 1, 3)

    land(recv.at[2], later1)

    def place(ref, rows, side):
        if side == 0:
            ref[..., PAD - 2 : PAD - 1, :] = rows
            ref[..., PAD - 1 : PAD, :] = jnp.zeros_like(rows)
        else:
            ref[..., top : top + 1, :] = -ROOT3 * rows
            ref[..., top + 1 : top + 2, :] = rows

    corners = jnp.concatenate(
        [sc1[1, 1, 0], tc[0], tc[1], hc1[1, 1, 0], jnp.zeros((PAD - 4, LANES), jnp.float32)], axis=0)
    corners = times_folded(corners, w2)
    for i in range(4):
        at = PAD - 1 + hy * (i % 2)
        fix[i // 2, at : at + 1] = corners[i : i + 1]
    for x in range(2):
        detail, smooth = rx[x, 0], rx[x, 1]
        smooth = smooth + jnp.where(line < hy - 1, pltpu.roll(detail, hy - 1, 0), 0.0)
        part = detail + jnp.where(line > 0, FAR * pltpu.roll(smooth, 1, 0), 0.0)
        odd = part + NEAR * smooth
        hx1[x, 1 - x, pl.ds(PAD, hy, stride=2), :] = smooth - ROOT3 * odd
        hx1[x, 1 - x, pl.ds(PAD + 1, hy, stride=2), :] = odd
    for side in range(2):
        place(e1, hy1[side], side)
        for x in range(2):
            place(hx1.at[x], hc1[x, side], side)
    lift1(slice(PAD - 2, PAD))
    lift1(slice(top, top + 2))
    wide = slice(PAD - 2, top + 2)
    _, edge = pair1(0, wide)
    detail = edge - FAR * hx1[0, :, wide]
    xd1[0, :, wide] = detail
    xs1[0, :, wide] = hx1[0, :, wide] - detail
    edge, _ = pair1(hx - 1, wide)
    detail = hx1[1, :, wide] - FAR * edge
    xd1[hx, :, wide] = detail
    xs1[hx, :, wide] = edge - detail

    def cols1(src, det, smo):
        def step(n, carry):
            for h in range(2):
                load = lambda start: src[n, h, pl.ds(start, hy + 1, stride=2), :]
                s0, t0 = sums(load(PAD), load(PAD + 1))
                sm, _ = sums(load(PAD - 2), load(PAD - 1))
                d = t0 - FAR * sm
                det[n, h, 0 : hy + 1] = d
                smo[n, h, PAD - 1 : PAD + hy] = sm - d
            return carry

        lax.fori_loop(0, hx + 1, step, 0)

    cols1(xd1, d1d, d1s)
    cols1(xs1, s1d, s1s)

    land(recv.at[4], landed)
    acc = mine[...]
    for k in range(len(peers)):
        acc = acc + rows_in[k]
    level = spread(acc, count_all)
    noise[...] = jnp.broadcast_to(level, (PAD, LANES))
    far1, mid1, near1 = limits(level, 1)

    def put_into(dst):
        def put(n, rows):
            dst[n] = rows
        return put

    def bands1(det, smo, h, limit_d, limit_s):
        def one_x(n):
            d = shrink(det[n, h], limit_d)
            return d, shrink(smo[n, h], limit_s) + d
        return one_x

    inverse1(hx, bands1(d1d, s1d, 1, far1, mid1), put_into(p1d1))
    inverse1(hx, bands1(d1s, s1s, 1, mid1, near1), put_into(p1s1))
    layers = 4
    detail_x = bands1(d1d, s1d, 0, far1, mid1)
    carry = detail_x(0)
    for n in range(layers):
        inverse1_y(hy, p1d1, p1s1, n, o1)
    for lo in range(0, cx, layers):
        for n in range(lo + layers, min(lo + 2 * layers, cx)):
            inverse1_y(hy, p1d1, p1s1, n, o1)
        for n in range(lo // 2, (lo + layers) // 2):
            d, before = carry
            carry = detail_x(n + 1)
            p1d0[2 * n], p1d0[2 * n + 1] = undo(d, carry[1], before)
        rows = o1[lo : lo + layers].reshape(layers * cy, LANES)
        known1[lo : lo + layers] = times_half(rows, v4).reshape(layers, cy, cz)

    land(recv.at[3], round2)
    every = slice(0, hy + 2 * PAD)
    before = xlow[0]
    xs2[0] = xlow[3]
    for m in range(-1, qx + 1):
        if m == qx:
            smooth, part = None, xhigh[0]
        elif m == -1:
            smooth, part = sums(xlow[1], xlow[2] + fix[0])
        elif m == qx - 1:
            smooth, part = sums(e2[hx - 2, every], e2[hx - 1, every] + fix[1])
        else:
            smooth, part = pair2(m, every)
        detail = part - FAR * before
        xd2[m + 1] = detail
        xs2[m + 2] = before - detail
        before = smooth
    xs2[qx + 3] = xhigh[1]
    pairs = hy // 2 + PAD

    def rows2(src):
        return forward_rows(src[:, pl.ds(0, pairs, stride=2), :],
                            src[:, pl.ds(1, pairs, stride=2), :])

    mid = slice(PAD // 2, PAD // 2 + pairs)
    dd[:, mid], ds[:, mid] = rows2(xd2)
    det, smo = rows2(xs2)
    sd[:, mid] = det[1 : qx + 3]
    ep3[:, mid] = smo

    n_own, n3, h3 = qx // 2, qx // 2 + 2, qy // 2 + PAD
    low_s, low_t = [ep3[0]], [None]
    for n in range(n_own + 1):
        s, t = sums(ep3[1 + 2 * n], ep3[2 + 2 * n])
        low_s.append(s)
        low_t.append(t)
    low_t.append(ep3[qx + 3])
    for n in range(n3):
        detail = low_t[n + 1] - FAR * low_s[n]
        t3d[n] = detail
        t3s[n] = low_s[n] - detail
    bands = []
    for src in (t3d, t3s):
        bands += forward_rows(src[:, pl.ds(0, h3, stride=2), :], src[:, pl.ds(1, h3, stride=2), :])
    rows = jnp.concatenate([band.reshape(n3 * h3, LANES) for band in bands], axis=0)
    b3[...] = times_folded(rows, w3).reshape(len(bands), n3, h3, LANES)

    land(send.at[0], sent[0])


def finish(shape, d1s, p1d0, known1, dd, ds, sd, ep3, b3, total, v1, v2, v3, out,
           ss, r2, r1, s0, p1s0, o1, ob, osem):
    cx, cy, cz = shape
    hx, hy, qx, qy = cx // 2, cy // 2, cx // 4, cy // 4
    n3, h3, x2, yrows = qx // 2 + 2, qy // 2 + PAD, qx + 2, qy + 2 * PAD
    noise = total[0:1]


    far3, mid3, near3 = (v[None] for v in limits(noise, 3))
    lane3 = lax.broadcasted_iota(jnp.int32, (n3, h3, LANES), 2)
    b_dd, b_ds, b_sd = shrink(b3[0], far3), shrink(b3[1], mid3), shrink(b3[2], mid3)
    b_ss = jnp.where(lane3 < cz // 8, b3[3], shrink(b3[3], near3))

    def inverse_x(det, smo):
        one = smo + det
        even, odd = undo(det[:-1], one[1:], one[:-1])
        return weave(even, odd)

    y_d = inverse_x(b_dd, b_sd)
    y_s = inverse_x(b_ds, b_ss)
    one = y_s + pltpu.roll(y_d, h3 - 1, 1)
    even, odd = undo(y_d, one, pltpu.roll(one, 1, 1))
    r2[:, pl.ds(0, h3, stride=2), :] = even
    r2[:, pl.ds(1, h3, stride=2), :] = odd
    back = times_folded(r2[...].reshape(x2 * yrows, LANES), v3).reshape(x2, yrows, LANES)

    far2, mid2, near2 = limits(noise, 2)
    lane2 = lax.broadcasted_iota(jnp.int32, (x2, yrows, LANES), 2)
    ss[...] = jnp.where(lane2 < cz // 4, back, shrink(ep3[1 : qx + 3], near2[None]))

    def one_x(n):
        d_d = shrink(dd[n], far2)
        d_s = shrink(ds[n], mid2)
        s_d = shrink(sd[n], mid2)
        return d_d, d_s, s_d + d_d, ss[n] + d_s

    def inv2(n, carry):
        d_d, d_s, b_d, b_s = carry
        after = one_x(n + 1)
        pair_d = undo(d_d, after[2], b_d)
        pair_s = undo(d_s, after[3], b_s)
        for i in range(2):
            y_d, y_s = pair_d[i], pair_s[i]
            one = y_s + pltpu.roll(y_d, yrows - 1, 0)
            even, odd = undo(y_d, one, pltpu.roll(one, 1, 0))
            r1[2 * n + i, pl.ds(0, yrows, stride=2), :] = even
            r1[2 * n + i, pl.ds(1, yrows, stride=2), :] = odd
        return after

    y1, group = hy + PAD, 3
    carry = one_x(0)
    for n in range(qx + 1):
        carry = inv2(n, carry)
        if (n + 1) % group == 0 or n == qx:
            lo, hi = 2 * (n // group * group), 2 * n + 2
            back = times_folded(r1[lo:hi, PAD : PAD + y1].reshape((hi - lo) * y1, LANES), v2)
            back = back.reshape(hi - lo, y1, LANES)
            s0[max(lo - 1, 0) : hi - 1] = back[1:] if lo == 0 else back
    _, mid1, _ = limits(noise, 1)

    def low_x(n):
        d = shrink(d1s[n, 0], mid1)
        return d, s0[n] + d

    def put_low(n, rows):
        p1s0[n] = rows

    inverse1(hx, low_x, put_low, True)

    layers = 4
    for n in range(layers):
        inverse1_y(hy, p1d0, p1s0, n, o1)
    for i in range(cx // layers):
        for n in range((i + 1) * layers, min((i + 2) * layers, cx)):
            inverse1_y(hy, p1d0, p1s0, n, o1)
        xs = slice(i * layers, (i + 1) * layers)
        rows = o1[xs].reshape(layers * cy, LANES)
        ob[xs] = known1[xs] + times_half(rows, v1).reshape(layers, cy, cz)
        for n in range(i * layers, (i + 1) * layers):
            pltpu.make_async_copy(ob.at[n], out.at[n], osem.at[0]).start()
    pltpu.make_async_copy(ob, out, osem.at[0]).wait()


def on_device(nx, ny, volume):
    cx, cy, cz = volume.shape
    hx, hy, qx, qy = cx // 2, cy // 2, cx // 4, cy // 4
    n3, h3 = qx // 2 + 2, qy // 2 + PAD
    f32 = jnp.float32
    count = cx * nx * cy * ny * cz // 8
    weights = [
        halves(forward_matrix(cz), cz), folded(forward_matrix(cz // 2)),
        folded(forward_matrix(cz // 4)), half_product(inverse_matrix(cz), 0),
        folded(inverse_matrix(cz // 2)), folded(inverse_matrix(cz // 4)),
        half_product(inverse_matrix(cz), 1),
    ]
    vmem = lambda *s: pltpu.VMEM(s, f32)
    ey, ey2, ey3 = cy + 2 * PAD, hy + 2 * PAD, qy + 2 * PAD
    wide = lambda *s: pltpu.VMEM(s, jnp.bfloat16)
    pair = (2 * LANES, 2 * LANES)
    made = (
        vmem(hx + 1, 2, hy + PAD, LANES), vmem(cx, hy + PAD, LANES), vmem(cx, cy, cz), *[vmem(qx + 2, ey3, LANES) for _ in range(3)],
        vmem(qx + 4, ey3, LANES), vmem(4, n3, h3, LANES), vmem(PAD, LANES),
        wide(3 * LANES, cz), wide(*pair), wide(*pair),
    )
    rows = 4 * cy + 4 * cx + 10 + 6 * (hy + 2 * PAD) + 2 * hx * PAD + nx * ny
    scratch = [
        wide(2, cz, cz), wide(*pair), wide(*pair), wide(3 * LANES, cz),
        vmem(cx, hy + PAD, LANES), vmem(cx, hy + PAD, LANES), vmem(cx, cy, LANES),
        *[vmem(hx + 1, 2, hy + PAD, LANES) for _ in range(3)],
        vmem(cx, 2, ey, LANES), vmem(2, 2, hy, LANES), vmem(2, 2, hy, LANES),
        vmem(2, 1, LANES), vmem(2, ey2, LANES),
        vmem(2, 2, ey, LANES), vmem(2, 2, cy, LANES),
        vmem(2, cx, 2, 1, LANES), vmem(2, cx, 2, 1, LANES),
        vmem(2, 2, 2, 1, LANES), vmem(2, 2, 2, 1, LANES),
        vmem(hx + 1, 2, ey, LANES), vmem(hx + 1, 2, ey, LANES),
        vmem(hx, ey2, LANES), vmem(4, hy, LANES), vmem(2, hy, LANES),
        vmem(4, ey2, LANES), vmem(2, ey2, LANES),
        vmem(qx + 2, ey2, LANES), vmem(qx + 4, ey2, LANES),
        vmem(n3, ey3, LANES), vmem(n3, ey3, LANES),
        vmem(1, LANES), vmem(nx * ny - 1, 1, LANES), vmem(max(rows, cz * cz // 32), 1, LANES),
        pltpu.SemaphoreType.DMA((1,)), pltpu.SemaphoreType.DMA((5,)),
        pltpu.SemaphoreType.DMA((2,)), pltpu.SemaphoreType.DMA((2,)),
    ]
    near = pl.BlockSpec(memory_space=pltpu.VMEM)
    passed = pl.pallas_call(
        functools.partial(kernel, (cx, cy, cz), count, nx, ny),
        out_shape=made,
        in_specs=[pl.BlockSpec(memory_space=pltpu.HBM)] * 8,
        out_specs=(near,) * len(made),
        scratch_shapes=scratch,
        compiler_params=pltpu.CompilerParams(
            collective_id=0, has_side_effects=True, vmem_limit_bytes=56 * 1024 * 1024),
    )(volume, *[jnp.asarray(w) for w in weights])
    return pl.pallas_call(
        functools.partial(finish, (cx, cy, cz)),
        out_shape=jax.ShapeDtypeStruct(volume.shape, f32),
        in_specs=[near] * len(made),
        out_specs=pl.BlockSpec(memory_space=pltpu.HBM),
        scratch_shapes=[
            vmem(qx + 2, ey3, LANES), vmem(qx + 2, ey3, LANES), vmem(hx + 2, 2 * ey3, LANES),
            vmem(hx + 1, hy + PAD, LANES),
            vmem(cx, hy + PAD, LANES), vmem(cx, cy, LANES), vmem(cx, cy, cz), pltpu.SemaphoreType.DMA((1,)),
        ],
        compiler_params=pltpu.CompilerParams(vmem_limit_bytes=24 * 1024 * 1024),
    )(*passed)


def solution(mesh):
    spec = P("gx", "gy", None)
    body = functools.partial(on_device, mesh.shape["gx"], mesh.shape["gy"])
    return jax.shard_map(body, mesh=mesh, in_specs=(spec,), out_specs=spec, check_vma=False)
```

```python
import functools
import math

import jax
import jax.numpy as jnp
import numpy as np
from jax import lax
from jax.experimental import pallas as pl
from jax.experimental.pallas import tpu as pltpu
from jax.sharding import PartitionSpec as P

ROOT3 = math.sqrt(3.0)
NEAR = math.sqrt(3.0) / 4.0
FAR = (math.sqrt(3.0) - 2.0) / 4.0
LOW = (math.sqrt(3.0) - 1.0) / math.sqrt(2.0)
HIGH = (math.sqrt(3.0) + 1.0) / math.sqrt(2.0)
LANES = 128
PAD = 8


def forward_matrix(size):
    lines = np.eye(size)
    even, odd = lines[:, 0::2], lines[:, 1::2]
    smooth = even + ROOT3 * odd
    detail = odd - NEAR * smooth - FAR * np.roll(smooth, 1, 1)
    smooth = smooth - np.roll(detail, -1, 1)
    return np.concatenate([LOW * smooth, HIGH * detail], 1)


def inverse_matrix(size):
    lines = np.eye(size)
    smooth, detail = lines[:, : size // 2] / LOW, lines[:, size // 2 :] / HIGH
    first = smooth + np.roll(detail, -1, 1)
    odd = detail + NEAR * first + FAR * np.roll(first, 1, 1)
    even = first - ROOT3 * odd
    return np.stack([even, odd], 2).reshape(size, size)


def halves(matrix, size):
    full = np.zeros((size, size))
    full[: matrix.shape[0], : matrix.shape[1]] = matrix
    high = full.astype(jnp.bfloat16)
    low = (full - high.astype(np.float64)).astype(jnp.bfloat16)
    return np.stack([high, low])


def times(values, w_ref):
    high = values.astype(jnp.bfloat16)
    low = (values - high.astype(jnp.float32)).astype(jnp.bfloat16)
    dot = functools.partial(jnp.dot, preferred_element_type=jnp.float32)
    return dot(high, w_ref[0]) + (dot(low, w_ref[0]) + dot(high, w_ref[1]))


def folded(matrix):
    high, low = halves(matrix, LANES)
    return np.block([[high, low], [high, np.zeros_like(low)]])


def times_folded(values, w_ref):
    high = values.astype(jnp.bfloat16)
    low = (values - high.astype(jnp.float32)).astype(jnp.bfloat16)
    both = jnp.dot(jnp.concatenate([high, low], axis=1), w_ref[...],
                   preferred_element_type=jnp.float32)
    return both[:, :LANES] + both[:, LANES:]


def half_product(matrix, h):
    high, low = halves(matrix, len(matrix))
    mine = slice(h * LANES, (h + 1) * LANES)
    return np.concatenate([high[mine], high[mine], low[mine]], axis=0)


def times_half(values, w_ref):
    high = values.astype(jnp.bfloat16)
    low = (values - high.astype(jnp.float32)).astype(jnp.bfloat16)
    dot = functools.partial(jnp.dot, preferred_element_type=jnp.float32)
    return (dot(jnp.concatenate([high, low], axis=1), w_ref[: 2 * LANES])
            + dot(high, w_ref[2 * LANES :]))


def shrink(values, noise):
    return values - jnp.clip(values, -noise, noise)


def sums(even, odd):
    smooth = even + ROOT3 * odd
    return smooth, odd - NEAR * smooth


def undo(detail, first, before):
    odd = detail + NEAR * first + FAR * before
    return first - ROOT3 * odd, odd


def weave(even, odd):
    both = jnp.stack([even, odd], axis=1)
    return both.reshape((2 * even.shape[0],) + even.shape[1:])


def forward_rows(even, odd):
    axis = even.ndim - 2
    smooth, part = sums(even, odd)
    detail = part - FAR * pltpu.roll(smooth, 1, axis)
    return detail, smooth - pltpu.roll(detail, even.shape[axis] - 1, axis)


def limits(noise, level):
    base = noise * (1.0 / LOW ** (2 * (level - 1)))
    return base * (1.0 / (HIGH * HIGH)), base * (1.0 / (HIGH * LOW)), base * (1.0 / (LOW * LOW))


def spread(total, count_all):
    return jnp.sum(total, axis=(0, 1), keepdims=True) * (
        HIGH * HIGH * math.sqrt(math.pi / 2.0) / count_all)


def inverse1(hx, one_x, put, unroll=4):
    def step(n, carry):
        d, before = carry
        after, one = one_x(n + 1)
        even, odd = undo(d, one, before)
        put(2 * n, even)
        put(2 * n + 1, odd)
        return after, one

    lax.fori_loop(0, hx, step, one_x(0), unroll=unroll)


def inverse1_y(hy, det, smo, n, dst):
    y_d, y_n = det[n, 0:hy], det[n, 1 : hy + 1]
    even, odd = undo(
        y_d, smo[n, PAD : PAD + hy] + y_n, smo[n, PAD - 1 : PAD - 1 + hy] + y_d)
    dst[n, pl.ds(0, hy, stride=2), :] = even
    dst[n, pl.ds(1, hy, stride=2), :] = odd


def kernel(shape, count_all, nx, ny, vol, g1, g2, g3, g4, g5, g6, g7,
           d1s, p1d0, known1, dd, ds, sd, ep3, b3, noise, v1, v2, v3,
           w1, w2, w3, v4, p1d1, p1s1, o1, d1d, s1d, s1s,
           e1, lx, rx, tc, fix, hx1, sx1, hy1, sy1, hc1, sc1, xd1, xs1,
           e2, xl, xh, xlow, xhigh, xd2, xs2, t3d, t3s,
           mine, rows_in, dummy, send, recv, lsem, wsem):
    cx, cy, cz = shape
    hx, hy, qx, qy = cx // 2, cy // 2, cx // 4, cy // 4
    ix, iy = lax.axis_index("gx"), lax.axis_index("gy")

    def device(dx, dy):
        return (lax.rem(ix + dx + nx, nx), lax.rem(iy + dy + ny, ny))

    near = [(dx, dy) for dx in (-1, 0, 1) for dy in (-1, 0, 1) if dx or dy]
    peers = [(dx, dy) for dx in range(nx) for dy in range(ny) if dx or dy]
    taken = {(dx % nx, dy % ny) for dx, dy in near}
    barrier = pltpu.get_barrier_semaphore()

    def greet(dx, dy):
        pl.semaphore_signal(barrier, inc=1, device_id=device(dx, dy),
                            device_id_type=pl.DeviceIdType.MESH)

    for d in sorted(taken):
        greet(*d)
    loads = [
        pltpu.make_async_copy(
            vol.at[:, :, pl.ds(h * LANES, LANES)],
            e1.at[:, h, pl.ds(PAD, cy), :], lsem.at[h])
        for h in range(2)
    ]
    for c in loads:
        c.start()
    for d in peers:
        if d not in taken:
            greet(*d)
    first_weight = pltpu.make_async_copy(g1, w1, wsem.at[0])
    first_weight.start()
    more = list(zip((g2, g3, g4, g5, g6, g7), (w2, w3, v1, v2, v3, v4)))
    for src, dst in more:
        pltpu.make_async_copy(src, dst, wsem.at[1]).start()

    sent = [0]

    def post(src, dst, dx, dy, group):
        sent[0] += math.prod(src.shape) // LANES
        pltpu.make_async_remote_copy(
            src_ref=src, dst_ref=dst, send_sem=send.at[0], recv_sem=recv.at[group],
            device_id=device(dx, dy), device_id_type=pl.DeviceIdType.MESH).start()
        return math.prod(src.shape) // LANES

    def land(sem, rows):
        part = dummy.at[pl.ds(0, rows)]
        pltpu.make_async_copy(part, part, sem).wait()

    ep3[:, 0 : PAD // 2] = jnp.zeros((qx + 4, PAD // 2, LANES), jnp.float32)
    ep3[:, PAD // 2 + hy // 2 + PAD :] = jnp.zeros((qx + 4, PAD // 2, LANES), jnp.float32)
    fix[...] = jnp.zeros((2, hy + 2 * PAD, LANES), jnp.float32)
    for ref in (dd, ds, sd):
        ref[:, 0 : PAD // 2] = jnp.zeros((qx + 2, PAD // 2, LANES), jnp.float32)
        ref[:, PAD // 2 + hy // 2 + PAD :] = jnp.zeros((qx + 2, PAD // 2, LANES), jnp.float32)

    top = PAD + cy
    own1, own = slice(PAD, top), slice(PAD, PAD + hy)
    for c in loads:
        c.wait()
    first_weight.wait()

    def depth(xs, ys):
        shape = (xs.stop - xs.start, ys.stop - ys.start, LANES)
        rows = jnp.concatenate(
            [e1[xs, h, ys].reshape(shape[0] * shape[1], LANES) for h in range(2)], axis=1)
        got = times(rows, w1)
        for h in range(2):
            e1[xs, h, ys] = got[:, h * LANES : (h + 1) * LANES].reshape(shape)

    inner = slice(2 * PAD, top - PAD)
    depth(slice(0, cx), slice(PAD, 2 * PAD))
    depth(slice(0, cx), slice(top - PAD, top))
    depth(slice(0, 2), inner)
    depth(slice(cx - 2, cx), inner)
    sx1[1] = sums(e1[0, :, own1], e1[1, :, own1])[1]
    sx1[0] = sums(e1[cx - 2, :, own1], e1[cx - 1, :, own1])[0]
    sy1[1] = sums(e1[:, :, PAD : PAD + 1], e1[:, :, PAD + 1 : PAD + 2])[1]
    sy1[0] = sums(e1[:, :, top - 2 : top - 1], e1[:, :, top - 1 : top])[0]
    for x in range(2):
        sc1[x, 1] = sums(sx1[x, :, 0:1], sx1[x, :, 1:2])[1]
        sc1[x, 0] = sums(sx1[x, :, cy - 2 : cy - 1], sx1[x, :, cy - 1 : cy])[0]
    line = lax.broadcasted_iota(jnp.int32, (hy, LANES), 0)
    for x in range(2):
        load = lambda start: sx1[x, 1 - x, pl.ds(start, hy, stride=2), :]
        smooth, part = sums(load(0), load(1))
        detail = part - jnp.where(line > 0, FAR * pltpu.roll(smooth, 1, 0), 0.0)
        lx[x, 0] = detail
        lx[x, 1] = smooth - jnp.where(line < hy - 1, pltpu.roll(detail, hy - 1, 0), 0.0)
    pl.semaphore_wait(barrier, len(peers))
    step = (1, -1)
    post_x = lambda x, h, g: post(
        sx1.at[x, h], hx1.at[x, h, pl.ds(PAD, cy), :], step[x], 0, g)
    post_y = lambda y, h, g: post(sy1.at[y, :, h], hy1.at[y, :, h], 0, step[y], g)
    post_c = lambda x, y, h, g: post(
        sc1.at[x, y, h], hc1.at[x, y, h], step[x], step[y], g)
    post_l = lambda x, k, g: post(lx.at[x, k], rx.at[x, k], step[x], 0, g)
    noise1 = post_c(0, 0, 1, 0)
    coarse1 = post_l(1, 1, 1)
    noise1 += post_l(0, 0, 0) + post_y(0, 1, 0)
    coarse1 += post_y(1, 0, 1)
    later1 = (post_c(1, 1, 0, 2) + post(sc1.at[1, 1, 0], tc.at[0], 0, -1, 2)
              + post(sc1.at[1, 1, 0], tc.at[1], -1, 0, 2) + post_c(0, 0, 0, 2) + post_c(1, 1, 1, 2) + post_x(0, 0, 2) + post_x(1, 1, 2)
              + post_l(0, 1, 2) + post_l(1, 0, 2)
              + post_y(0, 0, 2) + post_y(1, 1, 2))
    for h in range(2):
        later1 += post_c(0, 1, h, 2) + post_c(1, 0, h, 2)

    slab = 4
    for lo in range(2, cx - 2, slab):
        depth(slice(lo, min(lo + slab, cx - 2)), inner)

    def pair1(n, rows=slice(None)):
        return sums(e1[2 * n, :, rows], e1[2 * n + 1, :, rows])

    def lift1(rows):
        def step(n, carry):
            _, part_n = pair1(n, rows)
            before, _ = pair1(n - 1, rows)
            detail = part_n - FAR * before
            xd1[n, :, rows] = detail
            xs1[n, :, rows] = before - detail
            return carry

        lax.fori_loop(1, hx, step, 0)

    def shrunk(n):
        load = lambda start: xs1[n, 0, pl.ds(start, hy, stride=2), :]
        s0, _ = sums(load(PAD), load(PAD + 1))
        _, tp = sums(load(PAD + 2), load(PAD + 3))
        s1s[n, 0, own] = s0 - (tp - FAR * s0)

    def finest(n):
        load = lambda start: xd1[n, 1, pl.ds(start, hy, stride=2), :]
        _, t0 = sums(load(PAD), load(PAD + 1))
        sm, _ = sums(load(PAD - 2), load(PAD - 1))
        return t0 - FAR * sm

    def fold(values):
        return jnp.sum(values.reshape(hy // PAD, PAD, LANES), axis=0)

    known = line > 0

    def inside(n, magnitude):
        shrunk(n)
        return magnitude + fold(jnp.where(known, jnp.abs(finest(n)), 0.0))

    lift1(own1)
    magnitude = lax.fori_loop(1, hx, inside, jnp.zeros((PAD, LANES), jnp.float32))
    land(wsem.at[1], sum(2 * math.prod(dst.shape) // (4 * LANES) for _, dst in more))
    done = hy - PAD
    rows = s1s[1:hx, 0, PAD : PAD + done].reshape((hx - 1) * done, LANES)
    e2[0 : hx - 1, PAD : PAD + done] = times_folded(rows, w2).reshape(hx - 1, done, LANES)

    land(recv.at[0], noise1)
    edge = hy1[0, :, 1].reshape(hx, 2, 1, LANES)
    edge_s, edge_t = sums(edge[:, 0], edge[:, 1])
    edge_d = edge_t - FAR * jnp.concatenate([hc1[0, 0, 1][None], edge_s[:-1]], axis=0)
    xd1[0, 1, own1] = sums(e1[0, 1, own1], e1[1, 1, own1])[1]
    xd1[0, 1, PAD - 2 : PAD - 1] = edge_d[0]
    xd1[0, 1, PAD - 1 : PAD] = jnp.zeros((1, LANES), jnp.float32)
    _, edge_t = sums(xd1[1:hx, 1, PAD : PAD + 1], xd1[1:hx, 1, PAD + 1 : PAD + 2])
    row = jnp.sum(jnp.abs(edge_t - FAR * edge_d[1:]), axis=0)
    mine[...] = row + jnp.sum(magnitude + fold(jnp.abs(finest(0) - FAR * rx[0, 0])), axis=0, keepdims=True)
    landed = 0
    for k, d in enumerate(peers):
        landed += post(mine, rows_in.at[k], d[0], d[1], 4)

    land(recv.at[1], coarse1)
    edge, _ = sums(e1[cx - 2, 0, own1], e1[cx - 1, 0, own1])
    xs1[hx, 0, own1] = edge * (1.0 + FAR)
    shrunk(hx)
    s1s[hx, 0, own] = s1s[hx, 0, own] - rx[1, 1]
    edge = hy1[1, :, 0].reshape(hx, 2, 1, LANES)
    edge_s, edge_t = sums(edge[:, 0], edge[:, 1])
    after = jnp.concatenate([edge_t[1:], jnp.zeros_like(edge_t[:1])], axis=0)
    last_t = edge_s - (after - FAR * edge_s)
    last_s, _ = sums(xs1[1 : hx + 1, 0, top - 2 : top - 1], xs1[1 : hx + 1, 0, top - 1 : top])
    last_s = jnp.concatenate([last_s[:-1], last_s[-1:] - rx[1, 1, hy - 1 : hy][None]], axis=0)
    s1s[1 : hx + 1, 0, PAD + hy - 1 : PAD + hy] = last_s - (last_t - FAR * last_s)
    rows = jnp.concatenate(
        [s1s[1:hx, 0, PAD + done : PAD + hy].reshape((hx - 1) * PAD, LANES), s1s[hx, 0, own]],
        axis=0)
    got = times_folded(rows, w2)
    e2[0 : hx - 1, PAD + done : PAD + hy] = got[: (hx - 1) * PAD].reshape(hx - 1, PAD, LANES)
    e2[hx - 1, own] = got[(hx - 1) * PAD :]

    def pair2(m, rows):
        return sums(e2[2 * m, rows], e2[2 * m + 1, rows])

    def coarse2(m, rows):
        return pair2(m, rows)[0] * (1.0 + FAR) - pair2(m + 1, rows)[1]

    xl[0] = pair2(qx - 2, own)[0]
    xl[1] = e2[hx - 2, own]
    xl[2] = e2[hx - 1, own]
    xl[3] = sums(coarse2(qx - 4, own), coarse2(qx - 3, own))[0]
    xh[0] = pair2(0, own)[1]
    xh[1] = sums(coarse2(0, own), coarse2(1, own))[1]
    y_own, y_low, y_high = pl.ds(PAD, hy), pl.ds(0, PAD), pl.ds(PAD + hy, PAD)
    s_own, s_first, s_last = pl.ds(0, hy), pl.ds(0, PAD), pl.ds(hy - PAD, PAD)
    round2 = 0
    for rows_s, rows_d, dy in ((s_own, y_own, 0), (s_last, y_low, 1), (s_first, y_high, -1)):
        round2 += post(xl.at[:, rows_s, :], xlow.at[:, rows_d, :], 1, dy, 3)
        round2 += post(xh.at[:, rows_s, :], xhigh.at[:, rows_d, :], -1, dy, 3)
    round2 += post(e2.at[:, pl.ds(PAD, PAD), :], e2.at[:, y_high, :], 0, -1, 3)
    round2 += post(e2.at[:, pl.ds(hy, PAD), :], e2.at[:, y_low, :], 0, 1, 3)

    land(recv.at[2], later1)

    def place(ref, rows, side):
        if side == 0:
            ref[..., PAD - 2 : PAD - 1, :] = rows
            ref[..., PAD - 1 : PAD, :] = jnp.zeros_like(rows)
        else:
            ref[..., top : top + 1, :] = -ROOT3 * rows
            ref[..., top + 1 : top + 2, :] = rows

    corners = jnp.concatenate(
        [sc1[1, 1, 0], tc[0], tc[1], hc1[1, 1, 0], jnp.zeros((PAD - 4, LANES), jnp.float32)], axis=0)
    corners = times_folded(corners, w2)
    for i in range(4):
        at = PAD - 1 + hy * (i % 2)
        fix[i // 2, at : at + 1] = corners[i : i + 1]
    for x in range(2):
        detail, smooth = rx[x, 0], rx[x, 1]
        smooth = smooth + jnp.where(line < hy - 1, pltpu.roll(detail, hy - 1, 0), 0.0)
        part = detail + jnp.where(line > 0, FAR * pltpu.roll(smooth, 1, 0), 0.0)
        odd = part + NEAR * smooth
        hx1[x, 1 - x, pl.ds(PAD, hy, stride=2), :] = smooth - ROOT3 * odd
        hx1[x, 1 - x, pl.ds(PAD + 1, hy, stride=2), :] = odd
    for side in range(2):
        place(e1, hy1[side], side)
        for x in range(2):
            place(hx1.at[x], hc1[x, side], side)
    lift1(slice(PAD - 2, PAD))
    lift1(slice(top, top + 2))
    wide = slice(PAD - 2, top + 2)
    _, edge = pair1(0, wide)
    detail = edge - FAR * hx1[0, :, wide]
    xd1[0, :, wide] = detail
    xs1[0, :, wide] = hx1[0, :, wide] - detail
    edge, _ = pair1(hx - 1, wide)
    detail = hx1[1, :, wide] - FAR * edge
    xd1[hx, :, wide] = detail
    xs1[hx, :, wide] = edge - detail

    def cols1(src, det, smo):
        def step(n, carry):
            for h in range(2):
                load = lambda start: src[n, h, pl.ds(start, hy + 1, stride=2), :]
                s0, t0 = sums(load(PAD), load(PAD + 1))
                sm, _ = sums(load(PAD - 2), load(PAD - 1))
                d = t0 - FAR * sm
                det[n, h, 0 : hy + 1] = d
                smo[n, h, PAD - 1 : PAD + hy] = sm - d
            return carry

        lax.fori_loop(0, hx + 1, step, 0)

    cols1(xd1, d1d, d1s)
    cols1(xs1, s1d, s1s)

    land(recv.at[4], landed)
    acc = mine[...]
    for k in range(len(peers)):
        acc = acc + rows_in[k]
    level = spread(acc, count_all)
    noise[...] = jnp.broadcast_to(level, (PAD, LANES))
    far1, mid1, near1 = limits(level, 1)

    def put_into(dst):
        def put(n, rows):
            dst[n] = rows
        return put

    def bands1(det, smo, h, limit_d, limit_s):
        def one_x(n):
            d = shrink(det[n, h], limit_d)
            return d, shrink(smo[n, h], limit_s) + d
        return one_x

    inverse1(hx, bands1(d1d, s1d, 1, far1, mid1), put_into(p1d1))
    inverse1(hx, bands1(d1s, s1s, 1, mid1, near1), put_into(p1s1))
    layers = 2
    detail_x = bands1(d1d, s1d, 0, far1, mid1)
    carry = detail_x(0)
    for n in range(layers):
        inverse1_y(hy, p1d1, p1s1, n, o1)
    for lo in range(0, cx, layers):
        for n in range(lo + layers, min(lo + 2 * layers, cx)):
            inverse1_y(hy, p1d1, p1s1, n, o1)
        for n in range(lo // 2, (lo + layers) // 2):
            d, before = carry
            carry = detail_x(n + 1)
            p1d0[2 * n], p1d0[2 * n + 1] = undo(d, carry[1], before)
        rows = o1[lo : lo + layers].reshape(layers * cy, LANES)
        known1[lo : lo + layers] = times_half(rows, v4).reshape(layers, cy, cz)

    land(recv.at[3], round2)
    every = slice(0, hy + 2 * PAD)
    before = xlow[0]
    xs2[0] = xlow[3]
    for m in range(-1, qx + 1):
        if m == qx:
            smooth, part = None, xhigh[0]
        elif m == -1:
            smooth, part = sums(xlow[1], xlow[2] + fix[0])
        elif m == qx - 1:
            smooth, part = sums(e2[hx - 2, every], e2[hx - 1, every] + fix[1])
        else:
            smooth, part = pair2(m, every)
        detail = part - FAR * before
        xd2[m + 1] = detail
        xs2[m + 2] = before - detail
        before = smooth
    xs2[qx + 3] = xhigh[1]
    pairs = hy // 2 + PAD

    def rows2(src):
        return forward_rows(src[:, pl.ds(0, pairs, stride=2), :],
                            src[:, pl.ds(1, pairs, stride=2), :])

    mid = slice(PAD // 2, PAD // 2 + pairs)
    dd[:, mid], ds[:, mid] = rows2(xd2)
    det, smo = rows2(xs2)
    sd[:, mid] = det[1 : qx + 3]
    ep3[:, mid] = smo

    n_own, n3, h3 = qx // 2, qx // 2 + 2, qy // 2 + PAD
    low_s, low_t = [ep3[0]], [None]
    for n in range(n_own + 1):
        s, t = sums(ep3[1 + 2 * n], ep3[2 + 2 * n])
        low_s.append(s)
        low_t.append(t)
    low_t.append(ep3[qx + 3])
    for n in range(n3):
        detail = low_t[n + 1] - FAR * low_s[n]
        t3d[n] = detail
        t3s[n] = low_s[n] - detail
    bands = []
    for src in (t3d, t3s):
        bands += forward_rows(src[:, pl.ds(0, h3, stride=2), :], src[:, pl.ds(1, h3, stride=2), :])
    rows = jnp.concatenate([band.reshape(n3 * h3, LANES) for band in bands], axis=0)
    b3[...] = times_folded(rows, w3).reshape(len(bands), n3, h3, LANES)

    land(send.at[0], sent[0])


def finish(shape, d1s, p1d0, known1, dd, ds, sd, ep3, b3, total, v1, v2, v3, out,
           ss, r2, r1, s0, p1s0, o1, ob, osem):
    cx, cy, cz = shape
    hx, hy, qx, qy = cx // 2, cy // 2, cx // 4, cy // 4
    n3, h3, x2, yrows = qx // 2 + 2, qy // 2 + PAD, qx + 2, qy + 2 * PAD
    noise = total[0:1]


    far3, mid3, near3 = (v[None] for v in limits(noise, 3))
    lane3 = lax.broadcasted_iota(jnp.int32, (n3, h3, LANES), 2)
    b_dd, b_ds, b_sd = shrink(b3[0], far3), shrink(b3[1], mid3), shrink(b3[2], mid3)
    b_ss = jnp.where(lane3 < cz // 8, b3[3], shrink(b3[3], near3))

    def inverse_x(det, smo):
        one = smo + det
        even, odd = undo(det[:-1], one[1:], one[:-1])
        return weave(even, odd)

    y_d = inverse_x(b_dd, b_sd)
    y_s = inverse_x(b_ds, b_ss)
    one = y_s + pltpu.roll(y_d, h3 - 1, 1)
    even, odd = undo(y_d, one, pltpu.roll(one, 1, 1))
    r2[:, pl.ds(0, h3, stride=2), :] = even
    r2[:, pl.ds(1, h3, stride=2), :] = odd
    back = times_folded(r2[...].reshape(x2 * yrows, LANES), v3).reshape(x2, yrows, LANES)

    far2, mid2, near2 = limits(noise, 2)
    lane2 = lax.broadcasted_iota(jnp.int32, (x2, yrows, LANES), 2)
    ss[...] = jnp.where(lane2 < cz // 4, back, shrink(ep3[1 : qx + 3], near2[None]))

    def one_x(n):
        d_d = shrink(dd[n], far2)
        d_s = shrink(ds[n], mid2)
        s_d = shrink(sd[n], mid2)
        return d_d, d_s, s_d + d_d, ss[n] + d_s

    def inv2(n, carry):
        d_d, d_s, b_d, b_s = carry
        after = one_x(n + 1)
        pair_d = undo(d_d, after[2], b_d)
        pair_s = undo(d_s, after[3], b_s)
        for i in range(2):
            y_d, y_s = pair_d[i], pair_s[i]
            one = y_s + pltpu.roll(y_d, yrows - 1, 0)
            even, odd = undo(y_d, one, pltpu.roll(one, 1, 0))
            r1[2 * n + i, pl.ds(0, yrows, stride=2), :] = even
            r1[2 * n + i, pl.ds(1, yrows, stride=2), :] = odd
        return after

    y1, group = hy + PAD, 3
    carry = one_x(0)
    for n in range(qx + 1):
        carry = inv2(n, carry)
        if (n + 1) % group == 0 or n == qx:
            lo, hi = 2 * (n // group * group), 2 * n + 2
            back = times_folded(r1[lo:hi, PAD : PAD + y1].reshape((hi - lo) * y1, LANES), v2)
            back = back.reshape(hi - lo, y1, LANES)
            s0[max(lo - 1, 0) : hi - 1] = back[1:] if lo == 0 else back
    _, mid1, _ = limits(noise, 1)

    def low_x(n):
        d = shrink(d1s[n, 0], mid1)
        return d, s0[n] + d

    def put_low(n, rows):
        p1s0[n] = rows

    inverse1(hx, low_x, put_low, True)

    layers = 2
    for n in range(layers):
        inverse1_y(hy, p1d0, p1s0, n, o1)
    for i in range(cx // layers):
        for n in range((i + 1) * layers, min((i + 2) * layers, cx)):
            inverse1_y(hy, p1d0, p1s0, n, o1)
        xs = slice(i * layers, (i + 1) * layers)
        rows = o1[xs].reshape(layers * cy, LANES)
        ob[xs] = known1[xs] + times_half(rows, v1).reshape(layers, cy, cz)
        for n in range(i * layers, (i + 1) * layers):
            pltpu.make_async_copy(ob.at[n], out.at[n], osem.at[0]).start()
    pltpu.make_async_copy(ob, out, osem.at[0]).wait()


def on_device(nx, ny, volume):
    cx, cy, cz = volume.shape
    hx, hy, qx, qy = cx // 2, cy // 2, cx // 4, cy // 4
    n3, h3 = qx // 2 + 2, qy // 2 + PAD
    f32 = jnp.float32
    count = cx * nx * cy * ny * cz // 8
    weights = [
        halves(forward_matrix(cz), cz), folded(forward_matrix(cz // 2)),
        folded(forward_matrix(cz // 4)), half_product(inverse_matrix(cz), 0),
        folded(inverse_matrix(cz // 2)), folded(inverse_matrix(cz // 4)),
        half_product(inverse_matrix(cz), 1),
    ]
    vmem = lambda *s: pltpu.VMEM(s, f32)
    ey, ey2, ey3 = cy + 2 * PAD, hy + 2 * PAD, qy + 2 * PAD
    wide = lambda *s: pltpu.VMEM(s, jnp.bfloat16)
    pair = (2 * LANES, 2 * LANES)
    made = (
        vmem(hx + 1, 2, hy + PAD, LANES), vmem(cx, hy + PAD, LANES), vmem(cx, cy, cz), *[vmem(qx + 2, ey3, LANES) for _ in range(3)],
        vmem(qx + 4, ey3, LANES), vmem(4, n3, h3, LANES), vmem(PAD, LANES),
        wide(3 * LANES, cz), wide(*pair), wide(*pair),
    )
    rows = 4 * cy + 4 * cx + 10 + 6 * (hy + 2 * PAD) + 2 * hx * PAD + nx * ny
    scratch = [
        wide(2, cz, cz), wide(*pair), wide(*pair), wide(3 * LANES, cz),
        vmem(cx, hy + PAD, LANES), vmem(cx, hy + PAD, LANES), vmem(cx, cy, LANES),
        *[vmem(hx + 1, 2, hy + PAD, LANES) for _ in range(3)],
        vmem(cx, 2, ey, LANES), vmem(2, 2, hy, LANES), vmem(2, 2, hy, LANES),
        vmem(2, 1, LANES), vmem(2, ey2, LANES),
        vmem(2, 2, ey, LANES), vmem(2, 2, cy, LANES),
        vmem(2, cx, 2, 1, LANES), vmem(2, cx, 2, 1, LANES),
        vmem(2, 2, 2, 1, LANES), vmem(2, 2, 2, 1, LANES),
        vmem(hx + 1, 2, ey, LANES), vmem(hx + 1, 2, ey, LANES),
        vmem(hx, ey2, LANES), vmem(4, hy, LANES), vmem(2, hy, LANES),
        vmem(4, ey2, LANES), vmem(2, ey2, LANES),
        vmem(qx + 2, ey2, LANES), vmem(qx + 4, ey2, LANES),
        vmem(n3, ey3, LANES), vmem(n3, ey3, LANES),
        vmem(1, LANES), vmem(nx * ny - 1, 1, LANES), vmem(max(rows, cz * cz // 32), 1, LANES),
        pltpu.SemaphoreType.DMA((1,)), pltpu.SemaphoreType.DMA((5,)),
        pltpu.SemaphoreType.DMA((2,)), pltpu.SemaphoreType.DMA((2,)),
    ]
    near = pl.BlockSpec(memory_space=pltpu.VMEM)
    passed = pl.pallas_call(
        functools.partial(kernel, (cx, cy, cz), count, nx, ny),
        out_shape=made,
        in_specs=[pl.BlockSpec(memory_space=pltpu.HBM)] * 8,
        out_specs=(near,) * len(made),
        scratch_shapes=scratch,
        compiler_params=pltpu.CompilerParams(
            collective_id=0, has_side_effects=True, vmem_limit_bytes=56 * 1024 * 1024),
    )(volume, *[jnp.asarray(w) for w in weights])
    return pl.pallas_call(
        functools.partial(finish, (cx, cy, cz)),
        out_shape=jax.ShapeDtypeStruct(volume.shape, f32),
        in_specs=[near] * len(made),
        out_specs=pl.BlockSpec(memory_space=pltpu.HBM),
        scratch_shapes=[
            vmem(qx + 2, ey3, LANES), vmem(qx + 2, ey3, LANES), vmem(hx + 2, 2 * ey3, LANES),
            vmem(hx + 1, hy + PAD, LANES),
            vmem(cx, hy + PAD, LANES), vmem(cx, cy, LANES), vmem(cx, cy, cz), pltpu.SemaphoreType.DMA((1,)),
        ],
        compiler_params=pltpu.CompilerParams(vmem_limit_bytes=24 * 1024 * 1024),
    )(*passed)


def solution(mesh):
    spec = P("gx", "gy", None)
    body = functools.partial(on_device, mesh.shape["gx"], mesh.shape["gy"])
    return jax.shard_map(body, mesh=mesh, in_specs=(spec,), out_specs=spec, check_vma=False)
```

```python
import functools
import math

import jax
import jax.numpy as jnp
import numpy as np
from jax import lax
from jax.experimental import pallas as pl
from jax.experimental.pallas import tpu as pltpu
from jax.sharding import PartitionSpec as P

ROOT3 = math.sqrt(3.0)
NEAR = math.sqrt(3.0) / 4.0
FAR = (math.sqrt(3.0) - 2.0) / 4.0
LOW = (math.sqrt(3.0) - 1.0) / math.sqrt(2.0)
HIGH = (math.sqrt(3.0) + 1.0) / math.sqrt(2.0)
LANES = 128
PAD = 8


def forward_matrix(size):
    lines = np.eye(size)
    even, odd = lines[:, 0::2], lines[:, 1::2]
    smooth = even + ROOT3 * odd
    detail = odd - NEAR * smooth - FAR * np.roll(smooth, 1, 1)
    smooth = smooth - np.roll(detail, -1, 1)
    return np.concatenate([LOW * smooth, HIGH * detail], 1)


def inverse_matrix(size):
    lines = np.eye(size)
    smooth, detail = lines[:, : size // 2] / LOW, lines[:, size // 2 :] / HIGH
    first = smooth + np.roll(detail, -1, 1)
    odd = detail + NEAR * first + FAR * np.roll(first, 1, 1)
    even = first - ROOT3 * odd
    return np.stack([even, odd], 2).reshape(size, size)


def halves(matrix, size):
    full = np.zeros((size, size))
    full[: matrix.shape[0], : matrix.shape[1]] = matrix
    high = full.astype(jnp.bfloat16)
    low = (full - high.astype(np.float64)).astype(jnp.bfloat16)
    return np.stack([high, low])


def times(values, w_ref):
    high = values.astype(jnp.bfloat16)
    low = (values - high.astype(jnp.float32)).astype(jnp.bfloat16)
    dot = functools.partial(jnp.dot, preferred_element_type=jnp.float32)
    return dot(high, w_ref[0]) + (dot(low, w_ref[0]) + dot(high, w_ref[1]))


def folded(matrix):
    high, low = halves(matrix, LANES)
    return np.block([[high, low], [high, np.zeros_like(low)]])


def times_folded(values, w_ref):
    high = values.astype(jnp.bfloat16)
    low = (values - high.astype(jnp.float32)).astype(jnp.bfloat16)
    both = jnp.dot(jnp.concatenate([high, low], axis=1), w_ref[...],
                   preferred_element_type=jnp.float32)
    return both[:, :LANES] + both[:, LANES:]


def half_product(matrix, h):
    high, low = halves(matrix, len(matrix))
    mine = slice(h * LANES, (h + 1) * LANES)
    return np.concatenate([high[mine], high[mine], low[mine]], axis=0)


def times_half(values, w_ref):
    high = values.astype(jnp.bfloat16)
    low = (values - high.astype(jnp.float32)).astype(jnp.bfloat16)
    dot = functools.partial(jnp.dot, preferred_element_type=jnp.float32)
    return (dot(jnp.concatenate([high, low], axis=1), w_ref[: 2 * LANES])
            + dot(high, w_ref[2 * LANES :]))


def shrink(values, noise):
    return values - jnp.clip(values, -noise, noise)


def sums(even, odd):
    smooth = even + ROOT3 * odd
    return smooth, odd - NEAR * smooth


def undo(detail, first, before):
    odd = detail + NEAR * first + FAR * before
    return first - ROOT3 * odd, odd


def weave(even, odd):
    both = jnp.stack([even, odd], axis=1)
    return both.reshape((2 * even.shape[0],) + even.shape[1:])


def forward_rows(even, odd):
    axis = even.ndim - 2
    smooth, part = sums(even, odd)
    detail = part - FAR * pltpu.roll(smooth, 1, axis)
    return detail, smooth - pltpu.roll(detail, even.shape[axis] - 1, axis)


def limits(noise, level):
    base = noise * (1.0 / LOW ** (2 * (level - 1)))
    return base * (1.0 / (HIGH * HIGH)), base * (1.0 / (HIGH * LOW)), base * (1.0 / (LOW * LOW))


def spread(total, count_all):
    return jnp.sum(total, axis=(0, 1), keepdims=True) * (
        HIGH * HIGH * math.sqrt(math.pi / 2.0) / count_all)


def inverse1(hx, one_x, put, unroll=4):
    def step(n, carry):
        d, before = carry
        after, one = one_x(n + 1)
        even, odd = undo(d, one, before)
        put(2 * n, even)
        put(2 * n + 1, odd)
        return after, one

    lax.fori_loop(0, hx, step, one_x(0), unroll=unroll)


def inverse1_y(hy, det, smo, n, dst):
    y_d, y_n = det[n, 0:hy], det[n, 1 : hy + 1]
    even, odd = undo(
        y_d, smo[n, PAD : PAD + hy] + y_n, smo[n, PAD - 1 : PAD - 1 + hy] + y_d)
    dst[n, pl.ds(0, hy, stride=2), :] = even
    dst[n, pl.ds(1, hy, stride=2), :] = odd


def kernel(shape, count_all, nx, ny, vol, g1, g2, g3, g4, g5, g6, g7,
           d1s, p1d0, known1, dd, ds, sd, ep3, b3, noise, v1, v2, v3,
           w1, w2, w3, v4, p1d1, p1s1, o1, d1d, s1d, s1s,
           e1, lx, rx, tc, fix, hx1, sx1, hy1, sy1, hc1, sc1, xd1, xs1,
           e2, xl, xh, xlow, xhigh, xd2, xs2, t3d, t3s,
           mine, rows_in, dummy, send, recv, lsem, wsem):
    cx, cy, cz = shape
    hx, hy, qx, qy = cx // 2, cy // 2, cx // 4, cy // 4
    ix, iy = lax.axis_index("gx"), lax.axis_index("gy")

    def device(dx, dy):
        return (lax.rem(ix + dx + nx, nx), lax.rem(iy + dy + ny, ny))

    near = [(dx, dy) for dx in (-1, 0, 1) for dy in (-1, 0, 1) if dx or dy]
    peers = [(dx, dy) for dx in range(nx) for dy in range(ny) if dx or dy]
    peers.sort(key=lambda d: (d[0] % 2 == 0, d[0], min(d[1], ny - d[1])))
    taken = {(dx % nx, dy % ny) for dx, dy in near}
    barrier = pltpu.get_barrier_semaphore()

    def greet(dx, dy):
        pl.semaphore_signal(barrier, inc=1, device_id=device(dx, dy),
                            device_id_type=pl.DeviceIdType.MESH)

    for d in sorted(taken):
        greet(*d)
    loads = [
        pltpu.make_async_copy(
            vol.at[:, :, pl.ds(h * LANES, LANES)],
            e1.at[:, h, pl.ds(PAD, cy), :], lsem.at[h])
        for h in range(2)
    ]
    for c in loads:
        c.start()
    for d in peers:
        if d not in taken:
            greet(*d)
    first_weight = pltpu.make_async_copy(g1, w1, wsem.at[0])
    first_weight.start()
    more = list(zip((g2, g3, g4, g5, g6, g7), (w2, w3, v1, v2, v3, v4)))
    for src, dst in more:
        pltpu.make_async_copy(src, dst, wsem.at[1]).start()

    sent = [0]

    def post(src, dst, dx, dy, group):
        sent[0] += math.prod(src.shape) // LANES
        pltpu.make_async_remote_copy(
            src_ref=src, dst_ref=dst, send_sem=send.at[0], recv_sem=recv.at[group],
            device_id=device(dx, dy), device_id_type=pl.DeviceIdType.MESH).start()
        return math.prod(src.shape) // LANES

    def land(sem, rows):
        part = dummy.at[pl.ds(0, rows)]
        pltpu.make_async_copy(part, part, sem).wait()

    ep3[:, 0 : PAD // 2] = jnp.zeros((qx + 4, PAD // 2, LANES), jnp.float32)
    ep3[:, PAD // 2 + hy // 2 + PAD :] = jnp.zeros((qx + 4, PAD // 2, LANES), jnp.float32)
    fix[...] = jnp.zeros((2, hy + 2 * PAD, LANES), jnp.float32)
    for ref in (dd, ds, sd):
        ref[:, 0 : PAD // 2] = jnp.zeros((qx + 2, PAD // 2, LANES), jnp.float32)
        ref[:, PAD // 2 + hy // 2 + PAD :] = jnp.zeros((qx + 2, PAD // 2, LANES), jnp.float32)

    top = PAD + cy
    own1, own = slice(PAD, top), slice(PAD, PAD + hy)
    for c in loads:
        c.wait()
    first_weight.wait()

    def depth(xs, ys):
        shape = (xs.stop - xs.start, ys.stop - ys.start, LANES)
        rows = jnp.concatenate(
            [e1[xs, h, ys].reshape(shape[0] * shape[1], LANES) for h in range(2)], axis=1)
        got = times(rows, w1)
        for h in range(2):
            e1[xs, h, ys] = got[:, h * LANES : (h + 1) * LANES].reshape(shape)

    inner = slice(2 * PAD, top - PAD)
    depth(slice(0, cx), slice(PAD, 2 * PAD))
    depth(slice(0, cx), slice(top - PAD, top))
    depth(slice(0, 2), inner)
    depth(slice(cx - 2, cx), inner)
    sx1[1] = sums(e1[0, :, own1], e1[1, :, own1])[1]
    sx1[0] = sums(e1[cx - 2, :, own1], e1[cx - 1, :, own1])[0]
    sy1[1] = sums(e1[:, :, PAD : PAD + 1], e1[:, :, PAD + 1 : PAD + 2])[1]
    sy1[0] = sums(e1[:, :, top - 2 : top - 1], e1[:, :, top - 1 : top])[0]
    for x in range(2):
        sc1[x, 1] = sums(sx1[x, :, 0:1], sx1[x, :, 1:2])[1]
        sc1[x, 0] = sums(sx1[x, :, cy - 2 : cy - 1], sx1[x, :, cy - 1 : cy])[0]
    line = lax.broadcasted_iota(jnp.int32, (hy, LANES), 0)
    for x in range(2):
        load = lambda start: sx1[x, 1 - x, pl.ds(start, hy, stride=2), :]
        smooth, part = sums(load(0), load(1))
        detail = part - jnp.where(line > 0, FAR * pltpu.roll(smooth, 1, 0), 0.0)
        lx[x, 0] = detail
        lx[x, 1] = smooth - jnp.where(line < hy - 1, pltpu.roll(detail, hy - 1, 0), 0.0)
    pl.semaphore_wait(barrier, len(peers))
    step = (1, -1)
    post_x = lambda x, h, g: post(
        sx1.at[x, h], hx1.at[x, h, pl.ds(PAD, cy), :], step[x], 0, g)
    post_y = lambda y, h, g: post(sy1.at[y, :, h], hy1.at[y, :, h], 0, step[y], g)
    post_c = lambda x, y, h, g: post(
        sc1.at[x, y, h], hc1.at[x, y, h], step[x], step[y], g)
    post_l = lambda x, k, g: post(lx.at[x, k], rx.at[x, k], step[x], 0, g)
    noise1 = post_c(0, 0, 1, 0)
    coarse1 = post_l(1, 1, 1)
    noise1 += post_l(0, 0, 0) + post_y(0, 1, 0)
    coarse1 += post_y(1, 0, 1)
    later1 = (post_c(1, 1, 0, 2) + post(sc1.at[1, 1, 0], tc.at[0], 0, -1, 2)
              + post(sc1.at[1, 1, 0], tc.at[1], -1, 0, 2) + post_c(0, 0, 0, 2) + post_c(1, 1, 1, 2) + post_x(0, 0, 2) + post_x(1, 1, 2)
              + post_l(0, 1, 2) + post_l(1, 0, 2)
              + post_y(0, 0, 2) + post_y(1, 1, 2))
    for h in range(2):
        later1 += post_c(0, 1, h, 2) + post_c(1, 0, h, 2)

    slab = 4
    for lo in range(2, cx - 2, slab):
        depth(slice(lo, min(lo + slab, cx - 2)), inner)

    def pair1(n, rows=slice(None)):
        return sums(e1[2 * n, :, rows], e1[2 * n + 1, :, rows])

    def lift1(rows):
        def step(n, carry):
            _, part_n = pair1(n, rows)
            before, _ = pair1(n - 1, rows)
            detail = part_n - FAR * before
            xd1[n, :, rows] = detail
            xs1[n, :, rows] = before - detail
            return carry

        lax.fori_loop(1, hx, step, 0)

    def shrunk(n):
        load = lambda start: xs1[n, 0, pl.ds(start, hy, stride=2), :]
        s0, _ = sums(load(PAD), load(PAD + 1))
        _, tp = sums(load(PAD + 2), load(PAD + 3))
        s1s[n, 0, own] = s0 - (tp - FAR * s0)

    def finest(n):
        load = lambda start: xd1[n, 1, pl.ds(start, hy, stride=2), :]
        _, t0 = sums(load(PAD), load(PAD + 1))
        sm, _ = sums(load(PAD - 2), load(PAD - 1))
        return t0 - FAR * sm

    def fold(values):
        return jnp.sum(values.reshape(hy // PAD, PAD, LANES), axis=0)

    known = line > 0

    def inside(n, magnitude):
        shrunk(n)
        return magnitude + fold(jnp.where(known, jnp.abs(finest(n)), 0.0))

    lift1(own1)
    magnitude = lax.fori_loop(1, hx, inside, jnp.zeros((PAD, LANES), jnp.float32))
    land(wsem.at[1], sum(2 * math.prod(dst.shape) // (4 * LANES) for _, dst in more))
    done = hy - PAD
    rows = s1s[1:hx, 0, PAD : PAD + done].reshape((hx - 1) * done, LANES)
    e2[0 : hx - 1, PAD : PAD + done] = times_folded(rows, w2).reshape(hx - 1, done, LANES)

    land(recv.at[0], noise1)
    edge = hy1[0, :, 1].reshape(hx, 2, 1, LANES)
    edge_s, edge_t = sums(edge[:, 0], edge[:, 1])
    edge_d = edge_t - FAR * jnp.concatenate([hc1[0, 0, 1][None], edge_s[:-1]], axis=0)
    xd1[0, 1, own1] = sums(e1[0, 1, own1], e1[1, 1, own1])[1]
    xd1[0, 1, PAD - 2 : PAD - 1] = edge_d[0]
    xd1[0, 1, PAD - 1 : PAD] = jnp.zeros((1, LANES), jnp.float32)
    _, edge_t = sums(xd1[1:hx, 1, PAD : PAD + 1], xd1[1:hx, 1, PAD + 1 : PAD + 2])
    row = jnp.sum(jnp.abs(edge_t - FAR * edge_d[1:]), axis=0)
    mine[...] = row + jnp.sum(magnitude + fold(jnp.abs(finest(0) - FAR * rx[0, 0])), axis=0, keepdims=True)
    landed = 0
    for k, d in enumerate(peers):
        landed += post(mine, rows_in.at[k], d[0], d[1], 4)

    land(recv.at[1], coarse1)
    edge, _ = sums(e1[cx - 2, 0, own1], e1[cx - 1, 0, own1])
    xs1[hx, 0, own1] = edge * (1.0 + FAR)
    shrunk(hx)
    s1s[hx, 0, own] = s1s[hx, 0, own] - rx[1, 1]
    edge = hy1[1, :, 0].reshape(hx, 2, 1, LANES)
    edge_s, edge_t = sums(edge[:, 0], edge[:, 1])
    after = jnp.concatenate([edge_t[1:], jnp.zeros_like(edge_t[:1])], axis=0)
    last_t = edge_s - (after - FAR * edge_s)
    last_s, _ = sums(xs1[1 : hx + 1, 0, top - 2 : top - 1], xs1[1 : hx + 1, 0, top - 1 : top])
    last_s = jnp.concatenate([last_s[:-1], last_s[-1:] - rx[1, 1, hy - 1 : hy][None]], axis=0)
    s1s[1 : hx + 1, 0, PAD + hy - 1 : PAD + hy] = last_s - (last_t - FAR * last_s)
    rows = jnp.concatenate(
        [s1s[1:hx, 0, PAD + done : PAD + hy].reshape((hx - 1) * PAD, LANES), s1s[hx, 0, own]],
        axis=0)
    got = times_folded(rows, w2)
    e2[0 : hx - 1, PAD + done : PAD + hy] = got[: (hx - 1) * PAD].reshape(hx - 1, PAD, LANES)
    e2[hx - 1, own] = got[(hx - 1) * PAD :]

    def pair2(m, rows):
        return sums(e2[2 * m, rows], e2[2 * m + 1, rows])

    def coarse2(m, rows):
        return pair2(m, rows)[0] * (1.0 + FAR) - pair2(m + 1, rows)[1]

    xl[0] = pair2(qx - 2, own)[0]
    xl[1] = e2[hx - 2, own]
    xl[2] = e2[hx - 1, own]
    xl[3] = sums(coarse2(qx - 4, own), coarse2(qx - 3, own))[0]
    xh[0] = pair2(0, own)[1]
    xh[1] = sums(coarse2(0, own), coarse2(1, own))[1]
    y_own, y_low, y_high = pl.ds(PAD, hy), pl.ds(0, PAD), pl.ds(PAD + hy, PAD)
    s_own, s_first, s_last = pl.ds(0, hy), pl.ds(0, PAD), pl.ds(hy - PAD, PAD)
    round2 = 0
    for rows_s, rows_d, dy in ((s_own, y_own, 0), (s_last, y_low, 1), (s_first, y_high, -1)):
        round2 += post(xl.at[:, rows_s, :], xlow.at[:, rows_d, :], 1, dy, 3)
        round2 += post(xh.at[:, rows_s, :], xhigh.at[:, rows_d, :], -1, dy, 3)
    round2 += post(e2.at[:, pl.ds(PAD, PAD), :], e2.at[:, y_high, :], 0, -1, 3)
    round2 += post(e2.at[:, pl.ds(hy, PAD), :], e2.at[:, y_low, :], 0, 1, 3)

    land(recv.at[2], later1)

    def place(ref, rows, side):
        if side == 0:
            ref[..., PAD - 2 : PAD - 1, :] = rows
            ref[..., PAD - 1 : PAD, :] = jnp.zeros_like(rows)
        else:
            ref[..., top : top + 1, :] = -ROOT3 * rows
            ref[..., top + 1 : top + 2, :] = rows

    corners = jnp.concatenate(
        [sc1[1, 1, 0], tc[0], tc[1], hc1[1, 1, 0], jnp.zeros((PAD - 4, LANES), jnp.float32)], axis=0)
    corners = times_folded(corners, w2)
    for i in range(4):
        at = PAD - 1 + hy * (i % 2)
        fix[i // 2, at : at + 1] = corners[i : i + 1]
    for x in range(2):
        detail, smooth = rx[x, 0], rx[x, 1]
        smooth = smooth + jnp.where(line < hy - 1, pltpu.roll(detail, hy - 1, 0), 0.0)
        part = detail + jnp.where(line > 0, FAR * pltpu.roll(smooth, 1, 0), 0.0)
        odd = part + NEAR * smooth
        hx1[x, 1 - x, pl.ds(PAD, hy, stride=2), :] = smooth - ROOT3 * odd
        hx1[x, 1 - x, pl.ds(PAD + 1, hy, stride=2), :] = odd
    for side in range(2):
        place(e1, hy1[side], side)
        for x in range(2):
            place(hx1.at[x], hc1[x, side], side)
    lift1(slice(PAD - 2, PAD))
    lift1(slice(top, top + 2))
    wide = slice(PAD - 2, top + 2)
    _, edge = pair1(0, wide)
    detail = edge - FAR * hx1[0, :, wide]
    xd1[0, :, wide] = detail
    xs1[0, :, wide] = hx1[0, :, wide] - detail
    edge, _ = pair1(hx - 1, wide)
    detail = hx1[1, :, wide] - FAR * edge
    xd1[hx, :, wide] = detail
    xs1[hx, :, wide] = edge - detail

    def cols1(src, det, smo):
        def step(n, carry):
            for h in range(2):
                load = lambda start: src[n, h, pl.ds(start, hy + 1, stride=2), :]
                s0, t0 = sums(load(PAD), load(PAD + 1))
                sm, _ = sums(load(PAD - 2), load(PAD - 1))
                d = t0 - FAR * sm
                det[n, h, 0 : hy + 1] = d
                smo[n, h, PAD - 1 : PAD + hy] = sm - d
            return carry

        lax.fori_loop(0, hx + 1, step, 0)

    cols1(xd1, d1d, d1s)
    cols1(xs1, s1d, s1s)

    land(recv.at[4], landed)
    acc = mine[...]
    for k in range(len(peers)):
        acc = acc + rows_in[k]
    level = spread(acc, count_all)
    noise[...] = jnp.broadcast_to(level, (PAD, LANES))
    far1, mid1, near1 = limits(level, 1)

    def put_into(dst):
        def put(n, rows):
            dst[n] = rows
        return put

    def bands1(det, smo, h, limit_d, limit_s):
        def one_x(n):
            d = shrink(det[n, h], limit_d)
            return d, shrink(smo[n, h], limit_s) + d
        return one_x

    inverse1(hx, bands1(d1d, s1d, 1, far1, mid1), put_into(p1d1))
    inverse1(hx, bands1(d1s, s1s, 1, mid1, near1), put_into(p1s1))
    layers = 2
    detail_x = bands1(d1d, s1d, 0, far1, mid1)
    carry = detail_x(0)
    for n in range(layers):
        inverse1_y(hy, p1d1, p1s1, n, o1)
    for lo in range(0, cx, layers):
        for n in range(lo + layers, min(lo + 2 * layers, cx)):
            inverse1_y(hy, p1d1, p1s1, n, o1)
        for n in range(lo // 2, (lo + layers) // 2):
            d, before = carry
            carry = detail_x(n + 1)
            p1d0[2 * n], p1d0[2 * n + 1] = undo(d, carry[1], before)
        rows = o1[lo : lo + layers].reshape(layers * cy, LANES)
        known1[lo : lo + layers] = times_half(rows, v4).reshape(layers, cy, cz)

    land(recv.at[3], round2)
    every = slice(0, hy + 2 * PAD)
    before = xlow[0]
    xs2[0] = xlow[3]
    for m in range(-1, qx + 1):
        if m == qx:
            smooth, part = None, xhigh[0]
        elif m == -1:
            smooth, part = sums(xlow[1], xlow[2] + fix[0])
        elif m == qx - 1:
            smooth, part = sums(e2[hx - 2, every], e2[hx - 1, every] + fix[1])
        else:
            smooth, part = pair2(m, every)
        detail = part - FAR * before
        xd2[m + 1] = detail
        xs2[m + 2] = before - detail
        before = smooth
    xs2[qx + 3] = xhigh[1]
    pairs = hy // 2 + PAD

    def rows2(src):
        return forward_rows(src[:, pl.ds(0, pairs, stride=2), :],
                            src[:, pl.ds(1, pairs, stride=2), :])

    mid = slice(PAD // 2, PAD // 2 + pairs)
    dd[:, mid], ds[:, mid] = rows2(xd2)
    det, smo = rows2(xs2)
    sd[:, mid] = det[1 : qx + 3]
    ep3[:, mid] = smo

    n_own, n3, h3 = qx // 2, qx // 2 + 2, qy // 2 + PAD
    low_s, low_t = [ep3[0]], [None]
    for n in range(n_own + 1):
        s, t = sums(ep3[1 + 2 * n], ep3[2 + 2 * n])
        low_s.append(s)
        low_t.append(t)
    low_t.append(ep3[qx + 3])
    for n in range(n3):
        detail = low_t[n + 1] - FAR * low_s[n]
        t3d[n] = detail
        t3s[n] = low_s[n] - detail
    bands = []
    for src in (t3d, t3s):
        bands += forward_rows(src[:, pl.ds(0, h3, stride=2), :], src[:, pl.ds(1, h3, stride=2), :])
    rows = jnp.concatenate([band.reshape(n3 * h3, LANES) for band in bands], axis=0)
    b3[...] = times_folded(rows, w3).reshape(len(bands), n3, h3, LANES)

    land(send.at[0], sent[0])


def finish(shape, d1s, p1d0, known1, dd, ds, sd, ep3, b3, total, v1, v2, v3, out,
           ss, r2, r1, s0, p1s0, o1, ob, osem):
    cx, cy, cz = shape
    hx, hy, qx, qy = cx // 2, cy // 2, cx // 4, cy // 4
    n3, h3, x2, yrows = qx // 2 + 2, qy // 2 + PAD, qx + 2, qy + 2 * PAD
    noise = total[0:1]


    far3, mid3, near3 = (v[None] for v in limits(noise, 3))
    lane3 = lax.broadcasted_iota(jnp.int32, (n3, h3, LANES), 2)
    b_dd, b_ds, b_sd = shrink(b3[0], far3), shrink(b3[1], mid3), shrink(b3[2], mid3)
    b_ss = jnp.where(lane3 < cz // 8, b3[3], shrink(b3[3], near3))

    def inverse_x(det, smo):
        one = smo + det
        even, odd = undo(det[:-1], one[1:], one[:-1])
        return weave(even, odd)

    y_d = inverse_x(b_dd, b_sd)
    y_s = inverse_x(b_ds, b_ss)
    one = y_s + pltpu.roll(y_d, h3 - 1, 1)
    even, odd = undo(y_d, one, pltpu.roll(one, 1, 1))
    r2[:, pl.ds(0, h3, stride=2), :] = even
    r2[:, pl.ds(1, h3, stride=2), :] = odd
    back = times_folded(r2[...].reshape(x2 * yrows, LANES), v3).reshape(x2, yrows, LANES)

    far2, mid2, near2 = limits(noise, 2)
    lane2 = lax.broadcasted_iota(jnp.int32, (x2, yrows, LANES), 2)
    ss[...] = jnp.where(lane2 < cz // 4, back, shrink(ep3[1 : qx + 3], near2[None]))

    def one_x(n):
        d_d = shrink(dd[n], far2)
        d_s = shrink(ds[n], mid2)
        s_d = shrink(sd[n], mid2)
        return d_d, d_s, s_d + d_d, ss[n] + d_s

    def inv2(n, carry):
        d_d, d_s, b_d, b_s = carry
        after = one_x(n + 1)
        pair_d = undo(d_d, after[2], b_d)
        pair_s = undo(d_s, after[3], b_s)
        for i in range(2):
            y_d, y_s = pair_d[i], pair_s[i]
            one = y_s + pltpu.roll(y_d, yrows - 1, 0)
            even, odd = undo(y_d, one, pltpu.roll(one, 1, 0))
            r1[2 * n + i, pl.ds(0, yrows, stride=2), :] = even
            r1[2 * n + i, pl.ds(1, yrows, stride=2), :] = odd
        return after

    y1, group = hy + PAD, 3
    carry = one_x(0)
    for n in range(qx + 1):
        carry = inv2(n, carry)
        if (n + 1) % group == 0 or n == qx:
            lo, hi = 2 * (n // group * group), 2 * n + 2
            back = times_folded(r1[lo:hi, PAD : PAD + y1].reshape((hi - lo) * y1, LANES), v2)
            back = back.reshape(hi - lo, y1, LANES)
            s0[max(lo - 1, 0) : hi - 1] = back[1:] if lo == 0 else back
    _, mid1, _ = limits(noise, 1)

    def low_x(n):
        d = shrink(d1s[n, 0], mid1)
        return d, s0[n] + d

    def put_low(n, rows):
        p1s0[n] = rows

    inverse1(hx, low_x, put_low, True)

    layers = 2
    for n in range(layers):
        inverse1_y(hy, p1d0, p1s0, n, o1)
    for i in range(cx // layers):
        for n in range((i + 1) * layers, min((i + 2) * layers, cx)):
            inverse1_y(hy, p1d0, p1s0, n, o1)
        xs = slice(i * layers, (i + 1) * layers)
        rows = o1[xs].reshape(layers * cy, LANES)
        ob[xs] = known1[xs] + times_half(rows, v1).reshape(layers, cy, cz)
        for n in range(i * layers, (i + 1) * layers):
            pltpu.make_async_copy(ob.at[n], out.at[n], osem.at[0]).start()
    pltpu.make_async_copy(ob, out, osem.at[0]).wait()


def on_device(nx, ny, volume):
    cx, cy, cz = volume.shape
    hx, hy, qx, qy = cx // 2, cy // 2, cx // 4, cy // 4
    n3, h3 = qx // 2 + 2, qy // 2 + PAD
    f32 = jnp.float32
    count = cx * nx * cy * ny * cz // 8
    weights = [
        halves(forward_matrix(cz), cz), folded(forward_matrix(cz // 2)),
        folded(forward_matrix(cz // 4)), half_product(inverse_matrix(cz), 0),
        folded(inverse_matrix(cz // 2)), folded(inverse_matrix(cz // 4)),
        half_product(inverse_matrix(cz), 1),
    ]
    vmem = lambda *s: pltpu.VMEM(s, f32)
    ey, ey2, ey3 = cy + 2 * PAD, hy + 2 * PAD, qy + 2 * PAD
    wide = lambda *s: pltpu.VMEM(s, jnp.bfloat16)
    pair = (2 * LANES, 2 * LANES)
    made = (
        vmem(hx + 1, 2, hy + PAD, LANES), vmem(cx, hy + PAD, LANES), vmem(cx, cy, cz), *[vmem(qx + 2, ey3, LANES) for _ in range(3)],
        vmem(qx + 4, ey3, LANES), vmem(4, n3, h3, LANES), vmem(PAD, LANES),
        wide(3 * LANES, cz), wide(*pair), wide(*pair),
    )
    rows = 4 * cy + 4 * cx + 10 + 6 * (hy + 2 * PAD) + 2 * hx * PAD + nx * ny
    scratch = [
        wide(2, cz, cz), wide(*pair), wide(*pair), wide(3 * LANES, cz),
        vmem(cx, hy + PAD, LANES), vmem(cx, hy + PAD, LANES), vmem(cx, cy, LANES),
        *[vmem(hx + 1, 2, hy + PAD, LANES) for _ in range(3)],
        vmem(cx, 2, ey, LANES), vmem(2, 2, hy, LANES), vmem(2, 2, hy, LANES),
        vmem(2, 1, LANES), vmem(2, ey2, LANES),
        vmem(2, 2, ey, LANES), vmem(2, 2, cy, LANES),
        vmem(2, cx, 2, 1, LANES), vmem(2, cx, 2, 1, LANES),
        vmem(2, 2, 2, 1, LANES), vmem(2, 2, 2, 1, LANES),
        vmem(hx + 1, 2, ey, LANES), vmem(hx + 1, 2, ey, LANES),
        vmem(hx, ey2, LANES), vmem(4, hy, LANES), vmem(2, hy, LANES),
        vmem(4, ey2, LANES), vmem(2, ey2, LANES),
        vmem(qx + 2, ey2, LANES), vmem(qx + 4, ey2, LANES),
        vmem(n3, ey3, LANES), vmem(n3, ey3, LANES),
        vmem(1, LANES), vmem(nx * ny - 1, 1, LANES), vmem(max(rows, cz * cz // 32), 1, LANES),
        pltpu.SemaphoreType.DMA((1,)), pltpu.SemaphoreType.DMA((5,)),
        pltpu.SemaphoreType.DMA((2,)), pltpu.SemaphoreType.DMA((2,)),
    ]
    near = pl.BlockSpec(memory_space=pltpu.VMEM)
    passed = pl.pallas_call(
        functools.partial(kernel, (cx, cy, cz), count, nx, ny),
        out_shape=made,
        in_specs=[pl.BlockSpec(memory_space=pltpu.HBM)] * 8,
        out_specs=(near,) * len(made),
        scratch_shapes=scratch,
        compiler_params=pltpu.CompilerParams(
            collective_id=0, has_side_effects=True, vmem_limit_bytes=56 * 1024 * 1024),
    )(volume, *[jnp.asarray(w) for w in weights])
    return pl.pallas_call(
        functools.partial(finish, (cx, cy, cz)),
        out_shape=jax.ShapeDtypeStruct(volume.shape, f32),
        in_specs=[near] * len(made),
        out_specs=pl.BlockSpec(memory_space=pltpu.HBM),
        scratch_shapes=[
            vmem(qx + 2, ey3, LANES), vmem(qx + 2, ey3, LANES), vmem(hx + 2, 2 * ey3, LANES),
            vmem(hx + 1, hy + PAD, LANES),
            vmem(cx, hy + PAD, LANES), vmem(cx, cy, LANES), vmem(cx, cy, cz), pltpu.SemaphoreType.DMA((1,)),
        ],
        compiler_params=pltpu.CompilerParams(vmem_limit_bytes=24 * 1024 * 1024),
    )(*passed)


def solution(mesh):
    spec = P("gx", "gy", None)
    body = functools.partial(on_device, mesh.shape["gx"], mesh.shape["gy"])
    return jax.shard_map(body, mesh=mesh, in_specs=(spec,), out_specs=spec, check_vma=False)
```

```python
import functools
import math

import jax
import jax.numpy as jnp
import numpy as np
from jax import lax
from jax.experimental import pallas as pl
from jax.experimental.pallas import tpu as pltpu
from jax.sharding import PartitionSpec as P

ROOT3 = math.sqrt(3.0)
NEAR = math.sqrt(3.0) / 4.0
FAR = (math.sqrt(3.0) - 2.0) / 4.0
LOW = (math.sqrt(3.0) - 1.0) / math.sqrt(2.0)
HIGH = (math.sqrt(3.0) + 1.0) / math.sqrt(2.0)
LANES = 128
PAD = 8


def forward_matrix(size):
    lines = np.eye(size)
    even, odd = lines[:, 0::2], lines[:, 1::2]
    smooth = even + ROOT3 * odd
    detail = odd - NEAR * smooth - FAR * np.roll(smooth, 1, 1)
    smooth = smooth - np.roll(detail, -1, 1)
    return np.concatenate([LOW * smooth, HIGH * detail], 1)


def inverse_matrix(size):
    lines = np.eye(size)
    smooth, detail = lines[:, : size // 2] / LOW, lines[:, size // 2 :] / HIGH
    first = smooth + np.roll(detail, -1, 1)
    odd = detail + NEAR * first + FAR * np.roll(first, 1, 1)
    even = first - ROOT3 * odd
    return np.stack([even, odd], 2).reshape(size, size)


def halves(matrix, size):
    full = np.zeros((size, size))
    full[: matrix.shape[0], : matrix.shape[1]] = matrix
    high = full.astype(jnp.bfloat16)
    low = (full - high.astype(np.float64)).astype(jnp.bfloat16)
    return np.stack([high, low])


def times(values, w_ref):
    high = values.astype(jnp.bfloat16)
    low = (values - high.astype(jnp.float32)).astype(jnp.bfloat16)
    dot = functools.partial(jnp.dot, preferred_element_type=jnp.float32)
    return dot(high, w_ref[0]) + (dot(low, w_ref[0]) + dot(high, w_ref[1]))


def folded(matrix):
    high, low = halves(matrix, LANES)
    return np.block([[high, low], [high, np.zeros_like(low)]])


def times_folded(values, w_ref):
    high = values.astype(jnp.bfloat16)
    low = (values - high.astype(jnp.float32)).astype(jnp.bfloat16)
    both = jnp.dot(jnp.concatenate([high, low], axis=1), w_ref[...],
                   preferred_element_type=jnp.float32)
    return both[:, :LANES] + both[:, LANES:]


def half_product(matrix, h):
    high, low = halves(matrix, len(matrix))
    mine = slice(h * LANES, (h + 1) * LANES)
    return np.concatenate([high[mine], high[mine], low[mine]], axis=0)


def times_half(values, w_ref):
    high = values.astype(jnp.bfloat16)
    low = (values - high.astype(jnp.float32)).astype(jnp.bfloat16)
    dot = functools.partial(jnp.dot, preferred_element_type=jnp.float32)
    return (dot(jnp.concatenate([high, low], axis=1), w_ref[: 2 * LANES])
            + dot(high, w_ref[2 * LANES :]))


def shrink(values, noise):
    return values - jnp.clip(values, -noise, noise)


def sums(even, odd):
    smooth = even + ROOT3 * odd
    return smooth, odd - NEAR * smooth


def undo(detail, first, before):
    odd = detail + NEAR * first + FAR * before
    return first - ROOT3 * odd, odd


def weave(even, odd):
    both = jnp.stack([even, odd], axis=1)
    return both.reshape((2 * even.shape[0],) + even.shape[1:])


def forward_rows(even, odd):
    axis = even.ndim - 2
    smooth, part = sums(even, odd)
    detail = part - FAR * pltpu.roll(smooth, 1, axis)
    return detail, smooth - pltpu.roll(detail, even.shape[axis] - 1, axis)


def limits(noise, level):
    base = noise * (1.0 / LOW ** (2 * (level - 1)))
    return base * (1.0 / (HIGH * HIGH)), base * (1.0 / (HIGH * LOW)), base * (1.0 / (LOW * LOW))


def spread(total, count_all):
    return jnp.sum(total, axis=(0, 1), keepdims=True) * (
        HIGH * HIGH * math.sqrt(math.pi / 2.0) / count_all)


def inverse1(hx, one_x, put, unroll=4):
    def step(n, carry):
        d, before = carry
        after, one = one_x(n + 1)
        even, odd = undo(d, one, before)
        put(2 * n, even)
        put(2 * n + 1, odd)
        return after, one

    lax.fori_loop(0, hx, step, one_x(0), unroll=unroll)


def inverse1_y(hy, det, smo, n, dst):
    y_d, y_n = det[n, 0:hy], det[n, 1 : hy + 1]
    even, odd = undo(
        y_d, smo[n, PAD : PAD + hy] + y_n, smo[n, PAD - 1 : PAD - 1 + hy] + y_d)
    dst[n, pl.ds(0, hy, stride=2), :] = even
    dst[n, pl.ds(1, hy, stride=2), :] = odd


def kernel(shape, count_all, nx, ny, vol, g1, g2, g3, g4, g5, g6, g7,
           d1s, p1d0, known1, dd, ds, sd, ep3, b3, noise, v1, v2, v3,
           w1, w2, w3, v4, p1d1, p1s1, o1, d1d, s1d, s1s,
           e1, lx, rx, tc, fix, hx1, sx1, hy1, sy1, hc1, sc1, xd1, xs1,
           e2, xl, xh, xlow, xhigh, xd2, xs2, t3d, t3s,
           mine, rows_in, dummy, send, recv, lsem, wsem):
    cx, cy, cz = shape
    hx, hy, qx, qy = cx // 2, cy // 2, cx // 4, cy // 4
    ix, iy = lax.axis_index("gx"), lax.axis_index("gy")

    def device(dx, dy):
        return (lax.rem(ix + dx + nx, nx), lax.rem(iy + dy + ny, ny))

    near = [(dx, dy) for dx in (-1, 0, 1) for dy in (-1, 0, 1) if dx or dy]
    peers = [(dx, dy) for dx in range(nx) for dy in range(ny) if dx or dy]
    peers.sort(key=lambda d: (d[0] % 2 == 0, d[0], min(d[1], ny - d[1])))
    taken = {(dx % nx, dy % ny) for dx, dy in near}
    barrier = pltpu.get_barrier_semaphore()

    def greet(dx, dy):
        pl.semaphore_signal(barrier, inc=1, device_id=device(dx, dy),
                            device_id_type=pl.DeviceIdType.MESH)

    for d in sorted(taken):
        greet(*d)
    loads = [
        pltpu.make_async_copy(
            vol.at[:, :, pl.ds(h * LANES, LANES)],
            e1.at[:, h, pl.ds(PAD, cy), :], lsem.at[h])
        for h in range(2)
    ]
    for c in loads:
        c.start()
    for d in peers:
        if d not in taken:
            greet(*d)
    first_weight = pltpu.make_async_copy(g1, w1, wsem.at[0])
    first_weight.start()
    more = list(zip((g2, g3, g4, g5, g6, g7), (w2, w3, v1, v2, v3, v4)))
    for src, dst in more:
        pltpu.make_async_copy(src, dst, wsem.at[1]).start()

    sent = [0]

    def post(src, dst, dx, dy, group):
        sent[0] += math.prod(src.shape) // LANES
        pltpu.make_async_remote_copy(
            src_ref=src, dst_ref=dst, send_sem=send.at[0], recv_sem=recv.at[group],
            device_id=device(dx, dy), device_id_type=pl.DeviceIdType.MESH).start()
        return math.prod(src.shape) // LANES

    def land(sem, rows):
        part = dummy.at[pl.ds(0, rows)]
        pltpu.make_async_copy(part, part, sem).wait()

    ep3[:, 0 : PAD // 2] = jnp.zeros((qx + 4, PAD // 2, LANES), jnp.float32)
    ep3[:, PAD // 2 + hy // 2 + PAD :] = jnp.zeros((qx + 4, PAD // 2, LANES), jnp.float32)
    fix[...] = jnp.zeros((2, hy + 2 * PAD, LANES), jnp.float32)
    for ref in (dd, ds, sd):
        ref[:, 0 : PAD // 2] = jnp.zeros((qx + 2, PAD // 2, LANES), jnp.float32)
        ref[:, PAD // 2 + hy // 2 + PAD :] = jnp.zeros((qx + 2, PAD // 2, LANES), jnp.float32)

    top = PAD + cy
    own1, own = slice(PAD, top), slice(PAD, PAD + hy)
    for c in loads:
        c.wait()
    first_weight.wait()

    def depth(xs, ys):
        shape = (xs.stop - xs.start, ys.stop - ys.start, LANES)
        rows = jnp.concatenate(
            [e1[xs, h, ys].reshape(shape[0] * shape[1], LANES) for h in range(2)], axis=1)
        got = times(rows, w1)
        for h in range(2):
            e1[xs, h, ys] = got[:, h * LANES : (h + 1) * LANES].reshape(shape)

    inner = slice(2 * PAD, top - PAD)
    depth(slice(0, cx), slice(PAD, 2 * PAD))
    depth(slice(0, cx), slice(top - PAD, top))
    depth(slice(0, 2), inner)
    depth(slice(cx - 2, cx), inner)
    sx1[1] = sums(e1[0, :, own1], e1[1, :, own1])[1]
    sx1[0] = sums(e1[cx - 2, :, own1], e1[cx - 1, :, own1])[0]
    sy1[1] = sums(e1[:, :, PAD : PAD + 1], e1[:, :, PAD + 1 : PAD + 2])[1]
    sy1[0] = sums(e1[:, :, top - 2 : top - 1], e1[:, :, top - 1 : top])[0]
    for x in range(2):
        sc1[x, 1] = sums(sx1[x, :, 0:1], sx1[x, :, 1:2])[1]
        sc1[x, 0] = sums(sx1[x, :, cy - 2 : cy - 1], sx1[x, :, cy - 1 : cy])[0]
    line = lax.broadcasted_iota(jnp.int32, (hy, LANES), 0)
    for x in range(2):
        load = lambda start: sx1[x, 1 - x, pl.ds(start, hy, stride=2), :]
        smooth, part = sums(load(0), load(1))
        detail = part - jnp.where(line > 0, FAR * pltpu.roll(smooth, 1, 0), 0.0)
        lx[x, 0] = detail
        lx[x, 1] = smooth - jnp.where(line < hy - 1, pltpu.roll(detail, hy - 1, 0), 0.0)
    pl.semaphore_wait(barrier, len(peers))
    step = (1, -1)
    post_x = lambda x, h, g: post(
        sx1.at[x, h], hx1.at[x, h, pl.ds(PAD, cy), :], step[x], 0, g)
    post_y = lambda y, h, g: post(sy1.at[y, :, h], hy1.at[y, :, h], 0, step[y], g)
    post_c = lambda x, y, h, g: post(
        sc1.at[x, y, h], hc1.at[x, y, h], step[x], step[y], g)
    post_l = lambda x, k, g: post(lx.at[x, k], rx.at[x, k], step[x], 0, g)
    noise1 = post_c(0, 0, 1, 0)
    coarse1 = post_l(1, 1, 1)
    noise1 += post_l(0, 0, 0) + post_y(0, 1, 0)
    coarse1 += post_y(1, 0, 1)
    later1 = (post_c(1, 1, 0, 2) + post(sc1.at[1, 1, 0], tc.at[0], 0, -1, 2)
              + post(sc1.at[1, 1, 0], tc.at[1], -1, 0, 2) + post_c(0, 0, 0, 2) + post_c(1, 1, 1, 2) + post_x(0, 0, 2) + post_x(1, 1, 2)
              + post_l(0, 1, 2) + post_l(1, 0, 2)
              + post_y(0, 0, 2) + post_y(1, 1, 2))
    for h in range(2):
        later1 += post_c(0, 1, h, 2) + post_c(1, 0, h, 2)

    slab = 4
    for lo in range(2, cx - 2, slab):
        depth(slice(lo, min(lo + slab, cx - 2)), inner)

    def pair1(n, rows=slice(None)):
        return sums(e1[2 * n, :, rows], e1[2 * n + 1, :, rows])

    def lift1(rows):
        def step(n, carry):
            _, part_n = pair1(n, rows)
            before, _ = pair1(n - 1, rows)
            detail = part_n - FAR * before
            xd1[n, :, rows] = detail
            xs1[n, :, rows] = before - detail
            return carry

        lax.fori_loop(1, hx, step, 0)

    def shrunk(n):
        load = lambda start: xs1[n, 0, pl.ds(start, hy, stride=2), :]
        s0, _ = sums(load(PAD), load(PAD + 1))
        _, tp = sums(load(PAD + 2), load(PAD + 3))
        s1s[n, 0, own] = s0 - (tp - FAR * s0)

    def finest(n):
        load = lambda start: xd1[n, 1, pl.ds(start, hy, stride=2), :]
        _, t0 = sums(load(PAD), load(PAD + 1))
        sm, _ = sums(load(PAD - 2), load(PAD - 1))
        return t0 - FAR * sm

    def fold(values):
        return jnp.sum(values.reshape(hy // PAD, PAD, LANES), axis=0)

    known = line > 0

    def inside(n, magnitude):
        shrunk(n)
        return magnitude + fold(jnp.where(known, jnp.abs(finest(n)), 0.0))

    lift1(own1)
    magnitude = lax.fori_loop(1, hx, inside, jnp.zeros((PAD, LANES), jnp.float32))
    land(wsem.at[1], sum(2 * math.prod(dst.shape) // (4 * LANES) for _, dst in more))
    done = hy - PAD
    rows = s1s[1:hx, 0, PAD : PAD + done].reshape((hx - 1) * done, LANES)
    e2[0 : hx - 1, PAD : PAD + done] = times_folded(rows, w2).reshape(hx - 1, done, LANES)

    land(recv.at[0], noise1)
    edge = hy1[0, :, 1].reshape(hx, 2, 1, LANES)
    edge_s, edge_t = sums(edge[:, 0], edge[:, 1])
    edge_d = edge_t - FAR * jnp.concatenate([hc1[0, 0, 1][None], edge_s[:-1]], axis=0)
    xd1[0, 1, own1] = sums(e1[0, 1, own1], e1[1, 1, own1])[1]
    xd1[0, 1, PAD - 2 : PAD - 1] = edge_d[0]
    xd1[0, 1, PAD - 1 : PAD] = jnp.zeros((1, LANES), jnp.float32)
    _, edge_t = sums(xd1[1:hx, 1, PAD : PAD + 1], xd1[1:hx, 1, PAD + 1 : PAD + 2])
    row = jnp.sum(jnp.abs(edge_t - FAR * edge_d[1:]), axis=0)
    mine[...] = row + jnp.sum(magnitude + fold(jnp.abs(finest(0) - FAR * rx[0, 0])), axis=0, keepdims=True)
    landed = 0
    for k, d in enumerate(peers):
        landed += post(mine, rows_in.at[k], d[0], d[1], 4)

    land(recv.at[1], coarse1)
    edge, _ = sums(e1[cx - 2, 0, own1], e1[cx - 1, 0, own1])
    xs1[hx, 0, own1] = edge * (1.0 + FAR)
    shrunk(hx)
    s1s[hx, 0, own] = s1s[hx, 0, own] - rx[1, 1]
    edge = hy1[1, :, 0].reshape(hx, 2, 1, LANES)
    edge_s, edge_t = sums(edge[:, 0], edge[:, 1])
    after = jnp.concatenate([edge_t[1:], jnp.zeros_like(edge_t[:1])], axis=0)
    last_t = edge_s - (after - FAR * edge_s)
    last_s, _ = sums(xs1[1 : hx + 1, 0, top - 2 : top - 1], xs1[1 : hx + 1, 0, top - 1 : top])
    last_s = jnp.concatenate([last_s[:-1], last_s[-1:] - rx[1, 1, hy - 1 : hy][None]], axis=0)
    s1s[1 : hx + 1, 0, PAD + hy - 1 : PAD + hy] = last_s - (last_t - FAR * last_s)
    rows = jnp.concatenate(
        [s1s[1:hx, 0, PAD + done : PAD + hy].reshape((hx - 1) * PAD, LANES), s1s[hx, 0, own]],
        axis=0)
    got = times_folded(rows, w2)
    e2[0 : hx - 1, PAD + done : PAD + hy] = got[: (hx - 1) * PAD].reshape(hx - 1, PAD, LANES)
    e2[hx - 1, own] = got[(hx - 1) * PAD :]

    def pair2(m, rows):
        return sums(e2[2 * m, rows], e2[2 * m + 1, rows])

    def coarse2(m, rows):
        return pair2(m, rows)[0] * (1.0 + FAR) - pair2(m + 1, rows)[1]

    xl[0] = pair2(qx - 2, own)[0]
    xl[1] = e2[hx - 2, own]
    xl[2] = e2[hx - 1, own]
    xl[3] = sums(coarse2(qx - 4, own), coarse2(qx - 3, own))[0]
    xh[0] = pair2(0, own)[1]
    xh[1] = sums(coarse2(0, own), coarse2(1, own))[1]
    y_own, y_low, y_high = pl.ds(PAD, hy), pl.ds(0, PAD), pl.ds(PAD + hy, PAD)
    s_own, s_first, s_last = pl.ds(0, hy), pl.ds(0, PAD), pl.ds(hy - PAD, PAD)
    round2 = 0
    for rows_s, rows_d, dy in ((s_own, y_own, 0), (s_last, y_low, 1), (s_first, y_high, -1)):
        round2 += post(xl.at[:, rows_s, :], xlow.at[:, rows_d, :], 1, dy, 3)
        round2 += post(xh.at[:, rows_s, :], xhigh.at[:, rows_d, :], -1, dy, 3)
    round2 += post(e2.at[:, pl.ds(PAD, PAD), :], e2.at[:, y_high, :], 0, -1, 3)
    round2 += post(e2.at[:, pl.ds(hy, PAD), :], e2.at[:, y_low, :], 0, 1, 3)

    land(recv.at[2], later1)

    def place(ref, rows, side):
        if side == 0:
            ref[..., PAD - 2 : PAD - 1, :] = rows
            ref[..., PAD - 1 : PAD, :] = jnp.zeros_like(rows)
        else:
            ref[..., top : top + 1, :] = -ROOT3 * rows
            ref[..., top + 1 : top + 2, :] = rows

    corners = jnp.concatenate(
        [sc1[1, 1, 0], tc[0], tc[1], hc1[1, 1, 0], jnp.zeros((PAD - 4, LANES), jnp.float32)], axis=0)
    corners = times_folded(corners, w2)
    for i in range(4):
        at = PAD - 1 + hy * (i % 2)
        fix[i // 2, at : at + 1] = corners[i : i + 1]
    for x in range(2):
        detail, smooth = rx[x, 0], rx[x, 1]
        smooth = smooth + jnp.where(line < hy - 1, pltpu.roll(detail, hy - 1, 0), 0.0)
        part = detail + jnp.where(line > 0, FAR * pltpu.roll(smooth, 1, 0), 0.0)
        odd = part + NEAR * smooth
        hx1[x, 1 - x, pl.ds(PAD, hy, stride=2), :] = smooth - ROOT3 * odd
        hx1[x, 1 - x, pl.ds(PAD + 1, hy, stride=2), :] = odd
    for side in range(2):
        place(e1, hy1[side], side)
        for x in range(2):
            place(hx1.at[x], hc1[x, side], side)
    lift1(slice(PAD - 2, PAD))
    lift1(slice(top, top + 2))
    wide = slice(PAD - 2, top + 2)
    _, edge = pair1(0, wide)
    detail = edge - FAR * hx1[0, :, wide]
    xd1[0, :, wide] = detail
    xs1[0, :, wide] = hx1[0, :, wide] - detail
    edge, _ = pair1(hx - 1, wide)
    detail = hx1[1, :, wide] - FAR * edge
    xd1[hx, :, wide] = detail
    xs1[hx, :, wide] = edge - detail

    def cols1(src, det, smo):
        def step(n, carry):
            for h in range(2):
                load = lambda start: src[n, h, pl.ds(start, hy + 1, stride=2), :]
                s0, t0 = sums(load(PAD), load(PAD + 1))
                sm, _ = sums(load(PAD - 2), load(PAD - 1))
                d = t0 - FAR * sm
                det[n, h, 0 : hy + 1] = d
                smo[n, h, PAD - 1 : PAD + hy] = sm - d
            return carry

        lax.fori_loop(0, hx + 1, step, 0)

    cols1(xd1, d1d, d1s)
    cols1(xs1, s1d, s1s)

    land(recv.at[4], landed)
    acc = mine[...]
    for k in range(len(peers)):
        acc = acc + rows_in[k]
    level = spread(acc, count_all)
    noise[...] = jnp.broadcast_to(level, (PAD, LANES))
    far1, mid1, near1 = limits(level, 1)

    def put_into(dst):
        def put(n, rows):
            dst[n] = rows
        return put

    def bands1(det, smo, h, limit_d, limit_s):
        def one_x(n):
            d = shrink(det[n, h], limit_d)
            return d, shrink(smo[n, h], limit_s) + d
        return one_x

    high_d, high_s = bands1(d1d, s1d, 1, far1, mid1), bands1(d1s, s1s, 1, mid1, near1)

    def high_x(n, carry):
        new = high_d(n + 1) + high_s(n + 1)
        p1d1[2 * n], p1d1[2 * n + 1] = undo(carry[0], new[1], carry[1])
        p1s1[2 * n], p1s1[2 * n + 1] = undo(carry[2], new[3], carry[3])
        return new

    lax.fori_loop(0, hx, high_x, high_d(0) + high_s(0), unroll=4)
    layers = 2
    detail_x = bands1(d1d, s1d, 0, far1, mid1)
    carry = detail_x(0)
    for n in range(layers):
        inverse1_y(hy, p1d1, p1s1, n, o1)
    for lo in range(0, cx, layers):
        for n in range(lo + layers, min(lo + 2 * layers, cx)):
            inverse1_y(hy, p1d1, p1s1, n, o1)
        for n in range(lo // 2, (lo + layers) // 2):
            d, before = carry
            carry = detail_x(n + 1)
            p1d0[2 * n], p1d0[2 * n + 1] = undo(d, carry[1], before)
        rows = o1[lo : lo + layers].reshape(layers * cy, LANES)
        known1[lo : lo + layers] = times_half(rows, v4).reshape(layers, cy, cz)

    land(recv.at[3], round2)
    every = slice(0, hy + 2 * PAD)
    before = xlow[0]
    xs2[0] = xlow[3]
    for m in range(-1, qx + 1):
        if m == qx:
            smooth, part = None, xhigh[0]
        elif m == -1:
            smooth, part = sums(xlow[1], xlow[2] + fix[0])
        elif m == qx - 1:
            smooth, part = sums(e2[hx - 2, every], e2[hx - 1, every] + fix[1])
        else:
            smooth, part = pair2(m, every)
        detail = part - FAR * before
        xd2[m + 1] = detail
        xs2[m + 2] = before - detail
        before = smooth
    xs2[qx + 3] = xhigh[1]
    pairs = hy // 2 + PAD

    def rows2(src):
        return forward_rows(src[:, pl.ds(0, pairs, stride=2), :],
                            src[:, pl.ds(1, pairs, stride=2), :])

    mid = slice(PAD // 2, PAD // 2 + pairs)
    dd[:, mid], ds[:, mid] = rows2(xd2)
    det, smo = rows2(xs2)
    sd[:, mid] = det[1 : qx + 3]
    ep3[:, mid] = smo

    n_own, n3, h3 = qx // 2, qx // 2 + 2, qy // 2 + PAD
    low_s, low_t = [ep3[0]], [None]
    for n in range(n_own + 1):
        s, t = sums(ep3[1 + 2 * n], ep3[2 + 2 * n])
        low_s.append(s)
        low_t.append(t)
    low_t.append(ep3[qx + 3])
    for n in range(n3):
        detail = low_t[n + 1] - FAR * low_s[n]
        t3d[n] = detail
        t3s[n] = low_s[n] - detail
    bands = []
    for src in (t3d, t3s):
        bands += forward_rows(src[:, pl.ds(0, h3, stride=2), :], src[:, pl.ds(1, h3, stride=2), :])
    rows = jnp.concatenate([band.reshape(n3 * h3, LANES) for band in bands], axis=0)
    b3[...] = times_folded(rows, w3).reshape(len(bands), n3, h3, LANES)

    land(send.at[0], sent[0])


def finish(shape, d1s, p1d0, known1, dd, ds, sd, ep3, b3, total, v1, v2, v3, out,
           ss, r2, r1, s0, p1s0, o1, ob, osem):
    cx, cy, cz = shape
    hx, hy, qx, qy = cx // 2, cy // 2, cx // 4, cy // 4
    n3, h3, x2, yrows = qx // 2 + 2, qy // 2 + PAD, qx + 2, qy + 2 * PAD
    noise = total[0:1]


    far3, mid3, near3 = (v[None] for v in limits(noise, 3))
    lane3 = lax.broadcasted_iota(jnp.int32, (n3, h3, LANES), 2)
    b_dd, b_ds, b_sd = shrink(b3[0], far3), shrink(b3[1], mid3), shrink(b3[2], mid3)
    b_ss = jnp.where(lane3 < cz // 8, b3[3], shrink(b3[3], near3))

    def inverse_x(det, smo):
        one = smo + det
        even, odd = undo(det[:-1], one[1:], one[:-1])
        return weave(even, odd)

    y_d = inverse_x(b_dd, b_sd)
    y_s = inverse_x(b_ds, b_ss)
    one = y_s + pltpu.roll(y_d, h3 - 1, 1)
    even, odd = undo(y_d, one, pltpu.roll(one, 1, 1))
    r2[:, pl.ds(0, h3, stride=2), :] = even
    r2[:, pl.ds(1, h3, stride=2), :] = odd
    back = times_folded(r2[...].reshape(x2 * yrows, LANES), v3).reshape(x2, yrows, LANES)

    far2, mid2, near2 = limits(noise, 2)
    lane2 = lax.broadcasted_iota(jnp.int32, (x2, yrows, LANES), 2)
    ss[...] = jnp.where(lane2 < cz // 4, back, shrink(ep3[1 : qx + 3], near2[None]))

    def one_x(n):
        d_d = shrink(dd[n], far2)
        d_s = shrink(ds[n], mid2)
        s_d = shrink(sd[n], mid2)
        return d_d, d_s, s_d + d_d, ss[n] + d_s

    def inv2(n, carry):
        d_d, d_s, b_d, b_s = carry
        after = one_x(n + 1)
        pair_d = undo(d_d, after[2], b_d)
        pair_s = undo(d_s, after[3], b_s)
        for i in range(2):
            y_d, y_s = pair_d[i], pair_s[i]
            one = y_s + pltpu.roll(y_d, yrows - 1, 0)
            even, odd = undo(y_d, one, pltpu.roll(one, 1, 0))
            r1[2 * n + i, pl.ds(0, yrows, stride=2), :] = even
            r1[2 * n + i, pl.ds(1, yrows, stride=2), :] = odd
        return after

    y1, group = hy + PAD, 3
    carry = one_x(0)
    for n in range(qx + 1):
        carry = inv2(n, carry)
        if (n + 1) % group == 0 or n == qx:
            lo, hi = 2 * (n // group * group), 2 * n + 2
            back = times_folded(r1[lo:hi, PAD : PAD + y1].reshape((hi - lo) * y1, LANES), v2)
            back = back.reshape(hi - lo, y1, LANES)
            s0[max(lo - 1, 0) : hi - 1] = back[1:] if lo == 0 else back
    _, mid1, _ = limits(noise, 1)

    def low_x(n):
        d = shrink(d1s[n, 0], mid1)
        return d, s0[n] + d

    def put_low(n, rows):
        p1s0[n] = rows

    inverse1(hx, low_x, put_low, True)

    layers = 2
    for n in range(layers):
        inverse1_y(hy, p1d0, p1s0, n, o1)
    for i in range(cx // layers):
        for n in range((i + 1) * layers, min((i + 2) * layers, cx)):
            inverse1_y(hy, p1d0, p1s0, n, o1)
        xs = slice(i * layers, (i + 1) * layers)
        rows = o1[xs].reshape(layers * cy, LANES)
        ob[xs] = known1[xs] + times_half(rows, v1).reshape(layers, cy, cz)
        for n in range(i * layers, (i + 1) * layers):
            pltpu.make_async_copy(ob.at[n], out.at[n], osem.at[0]).start()
    pltpu.make_async_copy(ob, out, osem.at[0]).wait()


def on_device(nx, ny, volume):
    cx, cy, cz = volume.shape
    hx, hy, qx, qy = cx // 2, cy // 2, cx // 4, cy // 4
    n3, h3 = qx // 2 + 2, qy // 2 + PAD
    f32 = jnp.float32
    count = cx * nx * cy * ny * cz // 8
    weights = [
        halves(forward_matrix(cz), cz), folded(forward_matrix(cz // 2)),
        folded(forward_matrix(cz // 4)), half_product(inverse_matrix(cz), 0),
        folded(inverse_matrix(cz // 2)), folded(inverse_matrix(cz // 4)),
        half_product(inverse_matrix(cz), 1),
    ]
    vmem = lambda *s: pltpu.VMEM(s, f32)
    ey, ey2, ey3 = cy + 2 * PAD, hy + 2 * PAD, qy + 2 * PAD
    wide = lambda *s: pltpu.VMEM(s, jnp.bfloat16)
    pair = (2 * LANES, 2 * LANES)
    made = (
        vmem(hx + 1, 2, hy + PAD, LANES), vmem(cx, hy + PAD, LANES), vmem(cx, cy, cz), *[vmem(qx + 2, ey3, LANES) for _ in range(3)],
        vmem(qx + 4, ey3, LANES), vmem(4, n3, h3, LANES), vmem(PAD, LANES),
        wide(3 * LANES, cz), wide(*pair), wide(*pair),
    )
    rows = 4 * cy + 4 * cx + 10 + 6 * (hy + 2 * PAD) + 2 * hx * PAD + nx * ny
    scratch = [
        wide(2, cz, cz), wide(*pair), wide(*pair), wide(3 * LANES, cz),
        vmem(cx, hy + PAD, LANES), vmem(cx, hy + PAD, LANES), vmem(cx, cy, LANES),
        *[vmem(hx + 1, 2, hy + PAD, LANES) for _ in range(3)],
        vmem(cx, 2, ey, LANES), vmem(2, 2, hy, LANES), vmem(2, 2, hy, LANES),
        vmem(2, 1, LANES), vmem(2, ey2, LANES),
        vmem(2, 2, ey, LANES), vmem(2, 2, cy, LANES),
        vmem(2, cx, 2, 1, LANES), vmem(2, cx, 2, 1, LANES),
        vmem(2, 2, 2, 1, LANES), vmem(2, 2, 2, 1, LANES),
        vmem(hx + 1, 2, ey, LANES), vmem(hx + 1, 2, ey, LANES),
        vmem(hx, ey2, LANES), vmem(4, hy, LANES), vmem(2, hy, LANES),
        vmem(4, ey2, LANES), vmem(2, ey2, LANES),
        vmem(qx + 2, ey2, LANES), vmem(qx + 4, ey2, LANES),
        vmem(n3, ey3, LANES), vmem(n3, ey3, LANES),
        vmem(1, LANES), vmem(nx * ny - 1, 1, LANES), vmem(max(rows, cz * cz // 32), 1, LANES),
        pltpu.SemaphoreType.DMA((1,)), pltpu.SemaphoreType.DMA((5,)),
        pltpu.SemaphoreType.DMA((2,)), pltpu.SemaphoreType.DMA((2,)),
    ]
    near = pl.BlockSpec(memory_space=pltpu.VMEM)
    passed = pl.pallas_call(
        functools.partial(kernel, (cx, cy, cz), count, nx, ny),
        out_shape=made,
        in_specs=[pl.BlockSpec(memory_space=pltpu.HBM)] * 8,
        out_specs=(near,) * len(made),
        scratch_shapes=scratch,
        compiler_params=pltpu.CompilerParams(
            collective_id=0, has_side_effects=True, vmem_limit_bytes=56 * 1024 * 1024),
    )(volume, *[jnp.asarray(w) for w in weights])
    return pl.pallas_call(
        functools.partial(finish, (cx, cy, cz)),
        out_shape=jax.ShapeDtypeStruct(volume.shape, f32),
        in_specs=[near] * len(made),
        out_specs=pl.BlockSpec(memory_space=pltpu.HBM),
        scratch_shapes=[
            vmem(qx + 2, ey3, LANES), vmem(qx + 2, ey3, LANES), vmem(hx + 2, 2 * ey3, LANES),
            vmem(hx + 1, hy + PAD, LANES),
            vmem(cx, hy + PAD, LANES), vmem(cx, cy, LANES), vmem(cx, cy, cz), pltpu.SemaphoreType.DMA((1,)),
        ],
        compiler_params=pltpu.CompilerParams(vmem_limit_bytes=24 * 1024 * 1024),
    )(*passed)


def solution(mesh):
    spec = P("gx", "gy", None)
    body = functools.partial(on_device, mesh.shape["gx"], mesh.shape["gy"])
    return jax.shard_map(body, mesh=mesh, in_specs=(spec,), out_specs=spec, check_vma=False)
```
